64 devices in a mesh: dp: 4 (over x, y), ep: 16 (over z, core).
Axes of the slice: x: 2, y: 2, z: 8, core: 2. Of those that a mesh axis runs over, the one named last changes fastest.
The devices are a block of a 4x4x8 slice.
Arguments:
- tokens: bfloat16 [65536, 1024], P(('dp', 'ep')), parts along dimension 0
- route_idx: int32 [65536, 8], P(('dp', 'ep')), parts along dimension 0
- gate_vals: float32 [65536, 8], P(('dp', 'ep')), parts along dimension 0
- w_gate: bfloat16 [32, 1024, 512], P('ep')
- w_up: bfloat16 [32, 1024, 512], P('ep')
- w_down: bfloat16 [32, 512, 1024], P('ep')
Outputs:
- output: bfloat16 [65536, 1024], P(('dp', 'ep')), parts along dimension 0
There are 4 independent parts. The reference program is written for one: setup_inputs(seed, part) draws one part's arguments, and reference() takes and returns one part's arrays. A program takes and returns all parts, laid end to end along the dimension named above; an argument that names none is the same for every part.
All inputs are finite; a program needn't handle non-finite values.
Results may differ from the reference program's by a relative error of at most 0.00782001.
Values are sent between devices in bfloat16 or wider.
A program may use at most 768 MiB of HBM per device.

```python
import functools
import jax
import jax.numpy as jnp
from jax import lax

TOKENS_DEV = 1024
GROUP_SIZE = 16
D_MODEL = 1024
D_FF = 512
EXPERTS = 32
TOP_K = 8
CAPACITY = 512
TOKENS = TOKENS_DEV * GROUP_SIZE


def device_routing(expert_order, hot_counts, dev_key):
    key_jitter, key_perm, key_tokens = jax.random.split(dev_key, 3)
    cold_n = EXPERTS - TOP_K
    half_n = cold_n // 2
    rest_slots = TOKENS_DEV * TOP_K - jnp.sum(hot_counts)
    base_count = rest_slots // cold_n
    extra_count = rest_slots - base_count * cold_n
    cold_counts = base_count + (jnp.arange(cold_n) < extra_count).astype(jnp.int32)
    jitter_up = jax.random.randint(key_jitter, (half_n,), 0, (base_count - 1) // 2 + 1)
    jitter = jnp.stack([jitter_up, -jitter_up], axis=1).reshape(-1)
    jitter = jnp.pad(jitter, (0, cold_n - 2 * half_n))
    cold_counts = cold_counts + jax.random.permutation(key_perm, jitter)
    all_counts = jnp.concatenate([hot_counts, cold_counts])
    run_ends = jnp.cumsum(all_counts)
    rank_ids = jnp.searchsorted(run_ends, jnp.arange(TOKENS_DEV * TOP_K), side="right")
    flat_ids = expert_order[rank_ids]
    slot_grid = flat_ids.reshape(TOP_K, TOKENS_DEV).T
    return jax.random.permutation(key_tokens, slot_grid, axis=0)


def draw_routing(route_key):
    key_order, key_hot, key_pick, key_dev = jax.random.split(route_key, 4)
    expert_order = jax.random.permutation(key_order, EXPERTS)
    hot_counts = CAPACITY - jax.random.randint(key_hot, (GROUP_SIZE, TOP_K), 0, CAPACITY // 4 + 1)
    full_dev = jax.random.randint(key_pick, (), 0, GROUP_SIZE)
    at_full = (jnp.arange(GROUP_SIZE)[:, None] == full_dev) & (jnp.arange(TOP_K)[None, :] == 0)
    hot_counts = jnp.where(at_full, CAPACITY, hot_counts)
    dev_keys = jax.random.split(key_dev, GROUP_SIZE)
    per_device = jax.vmap(functools.partial(device_routing, expert_order))(hot_counts, dev_keys)
    return per_device.reshape(TOKENS, TOP_K).astype(jnp.int32)


def draw_weight(weight_key, fan_in, fan_out):
    expert_keys = jax.random.split(weight_key, EXPERTS)
    return lax.map(lambda one_key: (jax.random.normal(one_key, (fan_in, fan_out), jnp.float32) * fan_in ** -0.5).astype(jnp.bfloat16), expert_keys)


def setup_inputs(seed: int = 0, part: int = 0) -> dict:
    root_key = jax.random.key(seed)
    part_key = jax.random.fold_in(root_key, part)
    key_tok, key_route, key_gate = jax.random.split(part_key, 3)
    key_wg, key_wu, key_wd = jax.random.split(jax.random.key(seed + 1), 3)
    tokens = jax.random.normal(key_tok, (TOKENS, D_MODEL), jnp.float32).astype(jnp.bfloat16)
    route_idx = draw_routing(key_route)
    gate_vals = jax.random.uniform(key_gate, (TOKENS, TOP_K), jnp.float32, 0.5, 1.5) * TOP_K ** -0.5
    return {"tokens": tokens, "route_idx": route_idx, "gate_vals": gate_vals, "w_gate": draw_weight(key_wg, D_MODEL, D_FF), "w_up": draw_weight(key_wu, D_MODEL, D_FF), "w_down": draw_weight(key_wd, D_FF, D_MODEL)}


def reference(tokens, route_idx, gate_vals, w_gate, w_up, w_down):
    row_cap = GROUP_SIZE * CAPACITY
    targets = jnp.arange(row_cap) + 1

    def expert_step(y_acc, expert_args):
        expert_id, wg_one, wu_one, wd_one = expert_args
        hit_mask = route_idx == expert_id
        member = jnp.sum(hit_mask, axis=1, dtype=jnp.int32)
        row_weight = jnp.sum(jnp.where(hit_mask, gate_vals, 0.0), axis=1)
        row_ids = jnp.searchsorted(jnp.cumsum(member), targets, side="left")
        picked = jnp.take(tokens, row_ids, axis=0, mode="fill", fill_value=0)
        pre_gate = jnp.dot(picked, wg_one, preferred_element_type=jnp.float32)
        pre_up = jnp.dot(picked, wu_one, preferred_element_type=jnp.float32)
        hidden = (jax.nn.silu(pre_gate) * pre_up).astype(jnp.bfloat16)
        expert_out = jnp.dot(hidden, wd_one, preferred_element_type=jnp.float32).astype(jnp.bfloat16)
        row_gate = jnp.take(row_weight, row_ids, mode="fill", fill_value=0.0)
        y_acc = y_acc.at[row_ids].add(row_gate[:, None] * expert_out.astype(jnp.float32), mode="drop")
        return y_acc, None

    y_init = jnp.zeros((TOKENS, D_MODEL), jnp.float32)
    y_sum, unused = lax.scan(expert_step, y_init, (jnp.arange(EXPERTS), w_gate, w_up, w_down))
    return y_sum.astype(jnp.bfloat16)
```

```python
import functools
import math

import jax
import jax.numpy as jnp
from jax import lax
from jax.experimental import pallas as pl
from jax.experimental.pallas import tpu as pltpu
from jax.sharding import PartitionSpec as P

CORES = 2
CHUNKS = 4
TILE = 256


def kernel(side, planes, x_ref, route_ref, gate_ref, wg_ref, wu_ref, wd_ref,
           y_ref, gs_ref, us_ref, ds_ref,
           x_all, route_all, gate_all, y_acc, y_peer, y_out, g_buf, u_buf, d_buf,
           zsend, zrecv, hsend, hrecv, load_sem, tok_sem, tok_send, tok_recv, part_send, part_recv, out_sem):
    half = planes // 2
    tok_n = x_ref.shape[0]
    rows_all = x_all.shape[0]
    tile = min(TILE, tok_n)
    tiles_half = tok_n // tile
    tiles = rows_all // tile
    col = lax.axis_index("dp")
    pos = lax.axis_index("ep")
    core = pos % CORES
    plane = pos // CORES
    cx, cy = col // side, col % side
    parity = (cx + cy) % 2
    other = 1 - parity
    col_x = col + side * (1 - 2 * (cx % 2))
    col_y = col + 1 - 2 * (cy % 2)
    up = (pos + CORES) % (planes * CORES)
    down = (pos + (planes - 1) * CORES) % (planes * CORES)
    peer = pos + 1 - 2 * core
    ring = ({"ep": up}, {"ep": down})
    side_dev = ({"dp": col_x}, {"dp": col_y})
    own = (wg_ref, wu_ref, wd_ref)
    slots = (gs_ref, us_ref, ds_ref)
    bufs = (g_buf, u_buf, d_buf)
    rows = tuple(w.shape[1] // CHUNKS for w in own)

    barrier = pltpu.get_barrier_semaphore()
    for dev in (*ring, *side_dev, {"ep": peer}):
        pl.semaphore_signal(barrier, inc=1, device_id=dev)
    pl.semaphore_wait(barrier, 5)

    def piece(which, ref, idx, i):
        return ref.at[idx, pl.ds(i * rows[which], rows[which])]

    def first_hop(way, which, i):
        return pltpu.make_async_remote_copy(
            piece(which, own[which], parity, i), piece(which, slots[which], way, i),
            zsend.at[way, 0, which, i], zrecv.at[way, 0, which, i], device_id=ring[way])

    def next_hop(way, h, which, i):
        return pltpu.make_async_remote_copy(
            piece(which, slots[which], (h - 1) * 4 + way, i), piece(which, slots[which], h * 4 + way, i),
            zsend.at[way, h, which, i], zrecv.at[way, h, which, i], device_id=ring[way])

    def side_hop(way, h, which, i):
        return pltpu.make_async_remote_copy(
            piece(which, slots[which], (h - 1) * 4 + way, i), piece(which, slots[which], (h - 1) * 4 + 2 + way, i),
            hsend.at[way, h - 1, which, i], hrecv.at[way, h - 1, which, i], device_id=side_dev[way])

    def wait_ring(way, h, which, i):
        there = piece(which, slots[which], (h - 1) * 4 + way, i)
        pltpu.make_async_remote_copy(
            there, there, zsend.at[way, h - 1, which, i], zrecv.at[way, h - 1, which, i], device_id=ring[way]).wait_recv()

    lo = half_pieces(0)
    hi = half_pieces(1)

    def halves(way):
        return lo if way == 0 else hi

    def goes_far(way, which):
        return [i for i in range(CHUNKS) if (which, i) in halves(way)]

    mine = pl.ds(core * tok_n, tok_n)
    tok = ((x_ref, x_all), (route_ref, route_all), (gate_ref, gate_all))
    for k, (src, dst) in enumerate(tok):
        pltpu.make_async_remote_copy(src, dst.at[mine], tok_send.at[k], tok_recv.at[k], device_id={"ep": peer}).start()
        pltpu.make_async_copy(src, dst.at[mine], tok_sem.at[k]).start()
    for which in range(3):
        for i in range(CHUNKS):
            for way in range(2):
                first_hop(way, which, i).start()

    def load_own(e, buf):
        for which in range(3):
            pltpu.make_async_copy(own[which].at[e], bufs[which].at[buf], load_sem.at[buf, which]).start()

    def load_slot(s, buf):
        for which in range(3):
            pltpu.make_async_copy(slots[which].at[s], bufs[which].at[buf], load_sem.at[buf, which]).start()

    def load_last(s, buf):
        for which in range(3):
            for way in range(2):
                ids = goes_far(way, which)
                if ids:
                    part = pl.ds(ids[0] * rows[which], len(ids) * rows[which])
                    pltpu.make_async_copy(slots[which].at[s + way, part], bufs[which].at[buf, part], load_sem.at[buf, which]).start()

    def wait_load(buf):
        for which in range(3):
            pltpu.make_async_copy(own[which].at[0], bufs[which].at[buf], load_sem.at[buf, which]).wait()

    def expert_id(h, q):
        src = (plane + planes + (2 * (q % 2) - 1) * h) % planes
        sub = parity + (q // 2) * (1 - 2 * parity)
        return (src * CORES + core) * 2 + sub

    def compute(row0, buf, expert):
        part = pl.ds(row0, tile)
        x_tile = x_all[part]
        a = jnp.dot(x_tile, g_buf[buf], preferred_element_type=jnp.float32)
        b = jnp.dot(x_tile, u_buf[buf], preferred_element_type=jnp.float32)
        hidden = (jax.nn.silu(a) * b).astype(jnp.bfloat16)
        out = jnp.dot(hidden, d_buf[buf], preferred_element_type=jnp.float32).astype(jnp.bfloat16)
        gate = jnp.sum(jnp.where(route_all[part] == expert, gate_all[part], 0.0), axis=1, keepdims=True)
        y_acc[part] += jnp.where(gate > 0.0, gate * out.astype(jnp.float32), 0.0)

    load_own(0, 0)
    y_acc[...] = jnp.zeros_like(y_acc)
    for k, (src, dst) in enumerate(tok):
        pltpu.make_async_copy(src, dst.at[mine], tok_sem.at[k]).wait()
        pltpu.make_async_remote_copy(src, dst.at[mine], tok_send.at[k], tok_recv.at[k], device_id={"ep": peer}).wait()

    def wait_side(way, h, ids):
        for which, i in ids:
            side_hop(way, h, which, i).wait_recv()

    every = [(which, i) for which in range(3) for i in range(CHUNKS)]

    def step_tile(h, t):
        q = t // tiles
        buf = q % 2

        @pl.when(t % tiles == 0)
        def _():
            wait_load(buf)

            @pl.when(h == 1)
            def _():
                @pl.when(q == 0)
                def _():
                    load_own(1, 1)

            @pl.when(h > 1)
            def _():
                @pl.when(q < 3)
                def _():
                    @pl.when(q == 1)
                    def _():
                        wait_side(0, h - 1, every)

                    @pl.when(q == 2)
                    def _():
                        wait_side(1, h - 1, every)

                    load_slot((h - 2) * 4 + q + 1, 1 - buf)

        first = (plane * CORES + core) * 2 + q
        expert = jnp.where(h == 1, first, expert_id(h - 1, q))
        compute((t % tiles) * tile, buf, expert)

    per_set = -(-4 * tiles // (3 * CHUNKS))

    def stage(h, carry):
        @pl.when(h > 1)
        def _():
            load_slot((h - 2) * 4, 0)

        count = jnp.where(h == 1, 2, 4) * tiles
        for which in range(3):
            def one(i, c, which=which):
                for way in range(2):
                    far = goes_far(way, which)
                    wait_ring(way, h, which, i)
                    if len(far) == CHUNKS:
                        next_hop(way, h, which, i).start()
                    else:
                        ok = h < half - 1
                        if far:
                            ok = ok | ((i >= far[0]) & (i <= far[-1]))

                        @pl.when(ok)
                        def _():
                            next_hop(way, h, which, i).start()
                    side_hop(way, h, which, i).start()

                def tile_step(k, c2):
                    t = (which * CHUNKS + i) * per_set + k

                    @pl.when(t < count)
                    def _():
                        step_tile(h, t)
                    return c2

                return lax.fori_loop(0, per_set, tile_step, c)

            lax.fori_loop(0, CHUNKS, one, 0)
        return carry

    lax.fori_loop(1, half, stage, 0)

    load_slot((half - 2) * 4, 0)
    sets = len(lo)
    per_last = -(-4 * tiles // sets)
    for k in range(sets):
        for way in range(2):
            which, i = halves(way)[k]
            wait_ring(way, half, which, i)
            side_hop(way, half, which, i).start()

        def tile_step(n, c, k=k):
            t = k * per_last + n

            @pl.when(t < 4 * tiles)
            def _():
                step_tile(half, t)
            return c

        lax.fori_loop(0, per_last, tile_step, 0)

    far_slot = (half - 1) * 4
    load_last(far_slot, 0)
    for way in range(2):
        wait_side(way, half, halves(way))
    load_last(far_slot + 2, 1)
    wait_load(0)

    def far_own(t, c):
        compute(t * tile, 0, expert_id(half, 0))
        return c

    lax.fori_loop(0, tiles, far_own, 0)
    wait_load(1)

    def part_copy(t):
        src = y_acc.at[pl.ds((1 - core) * tok_n + t * tile, tile)]
        return pltpu.make_async_remote_copy(src, y_peer.at[pl.ds(t * tile, tile)], part_send.at[t], part_recv.at[t], device_id={"ep": peer})

    def far_side(t, c):
        which_half = (1 - core) + (t // tiles_half) * (2 * core - 1)
        compute(which_half * tok_n + (t % tiles_half) * tile, 1, expert_id(half, 2))

        @pl.when((t >= 1) & (t <= tiles_half))
        def _():
            part_copy(t - 1).start()
        return c

    lax.fori_loop(0, tiles, far_side, 0)

    def finish(t, c):
        part_copy(t).wait()
        part = pl.ds(t * tile, tile)
        y_out[part] = (y_acc[pl.ds(core * tok_n + t * tile, tile)] + y_peer[part]).astype(y_out.dtype)
        pltpu.make_async_copy(y_out.at[part], y_ref.at[part], out_sem.at[t]).start()
        return c

    lax.fori_loop(0, tiles_half, finish, 0)

    def drain_out(t, c):
        part = pl.ds(t * tile, tile)
        pltpu.make_async_copy(y_out.at[part], y_ref.at[part], out_sem.at[t]).wait()
        return c

    lax.fori_loop(0, tiles_half, drain_out, 0)

    for which in range(3):
        def drain(i, c, which=which):
            for way in range(2):
                first_hop(way, which, i).wait_send()

                def per_stage(h, c2):
                    side_hop(way, h, which, i).wait_send()
                    return c2

                lax.fori_loop(1, half, per_stage, 0)

                def per_hop(h, c2):
                    next_hop(way, h, which, i).wait_send()
                    return c2

                lax.fori_loop(1, half - 1, per_hop, 0)
            return c

        lax.fori_loop(0, CHUNKS, drain, 0)
    for way in range(2):
        for which, i in halves(way):
            next_hop(way, half - 1, which, i).wait_send()
            side_hop(way, half, which, i).wait_send()


def half_pieces(way):
    mid = CHUNKS // 2
    return [(way, i) for i in range(CHUNKS)] + [(2, way * mid + i) for i in range(mid)]


def moe(side, planes, x, route, gate, wg, wu, wd):
    tok_n, d_model = x.shape
    d_ff = wg.shape[2]
    half = planes // 2
    slots = half * 4
    tile = min(TILE, tok_n)
    parts = tok_n // tile
    bf = jnp.bfloat16
    any_spec = pl.BlockSpec(memory_space=pl.ANY)
    dma = pltpu.SemaphoreType.DMA
    rows = CORES * tok_n
    out = pl.pallas_call(
        functools.partial(kernel, side, planes),
        out_shape=(
            jax.ShapeDtypeStruct((tok_n, d_model), bf),
            jax.ShapeDtypeStruct((slots, d_model, d_ff), bf),
            jax.ShapeDtypeStruct((slots, d_model, d_ff), bf),
            jax.ShapeDtypeStruct((slots, d_ff, d_model), bf),
        ),
        in_specs=[any_spec] * 6,
        out_specs=(any_spec,) * 4,
        scratch_shapes=[
            pltpu.VMEM((rows, d_model), bf),
            pltpu.VMEM((rows, route.shape[1]), jnp.int32),
            pltpu.VMEM((rows, route.shape[1]), jnp.float32),
            pltpu.VMEM((rows, d_model), jnp.float32),
            pltpu.VMEM((tok_n, d_model), jnp.float32),
            pltpu.VMEM((tok_n, d_model), bf),
            pltpu.VMEM((2, d_model, d_ff), bf),
            pltpu.VMEM((2, d_model, d_ff), bf),
            pltpu.VMEM((2, d_ff, d_model), bf),
            dma((2, half, 3, CHUNKS)),
            dma((2, half, 3, CHUNKS)),
            dma((2, half, 3, CHUNKS)),
            dma((2, half, 3, CHUNKS)),
            dma((2, 3)),
            dma((3,)),
            dma((3,)),
            dma((3,)),
            dma((parts,)),
            dma((parts,)),
            dma((parts,)),
        ],
        compiler_params=pltpu.CompilerParams(
            collective_id=0, has_side_effects=True, vmem_limit_bytes=60 * 1024 * 1024),
        name="stream_experts",
    )(x, route, gate, wg, wu, wd)
    return out[0]


def solution(mesh):
    planes = mesh.shape["ep"] // CORES
    side = math.isqrt(mesh.shape["dp"])
    row_spec = P(("dp", "ep"))
    expert_spec = P("ep")

    def local_step(tok_loc, route_loc, gate_loc, wg_loc, wu_loc, wd_loc):
        return moe(side, planes, tok_loc, route_loc, gate_loc, wg_loc, wu_loc, wd_loc)

    return jax.shard_map(local_step, mesh=mesh, in_specs=(row_spec, row_spec, row_spec, expert_spec, expert_spec, expert_spec), out_specs=row_spec, check_vma=False)
```

```python
import functools
import math

import jax
import jax.numpy as jnp
from jax import lax
from jax.experimental import pallas as pl
from jax.experimental.pallas import tpu as pltpu
from jax.sharding import PartitionSpec as P

CORES = 2
CHUNKS = 8
TILE = 256
LANES = 128


def kernel(side, planes, x_ref, route_ref, gate_ref, wg_ref, wu_ref, wd_ref,
           y_ref, gs_ref, us_ref, ds_ref,
           x_all, route_all, gate_all, gate_rows, gate_cols, y_acc, y_peer, hidden,
           g_buf, u_buf, d_buf, g_far, u_far, d_far,
           zsend, zrecv, hsend, hrecv, psend, precv, gu_sem, d_sem, tok_sem, tok_send, tok_recv, part_send, part_recv):
    half = planes // 2
    tok_n = x_ref.shape[0]
    tile = min(TILE, tok_n)
    tiles_half = tok_n // tile
    tiles = CORES * tiles_half
    experts = planes * CORES * 2
    col = lax.axis_index("dp")
    pos = lax.axis_index("ep")
    core = pos % CORES
    plane = pos // CORES
    cx, cy = col // side, col % side
    parity = (cx + cy) % 2
    col_x = col + side * (1 - 2 * (cx % 2))
    col_y = col + 1 - 2 * (cy % 2)
    up = (pos + CORES) % (planes * CORES)
    down = (pos + (planes - 1) * CORES) % (planes * CORES)
    peer = {"ep": pos + 1 - 2 * core}
    ring = ({"ep": up}, {"ep": down})
    side_dev = ({"dp": col_x}, {"dp": col_y})
    own = (wg_ref, wu_ref, wd_ref)
    slots = (gs_ref, us_ref, ds_ref)
    far = (g_far, u_far, d_far)
    rows = tuple(w.shape[1] // CHUNKS for w in own)
    mid = CHUNKS // 2
    mine = core * tok_n
    theirs = (1 - core) * tok_n
    remote = pltpu.make_async_remote_copy

    barrier = pltpu.get_barrier_semaphore()
    for dev in (*ring, *side_dev, peer):
        pl.semaphore_signal(barrier, inc=1, device_id=dev)
    pl.semaphore_wait(barrier, 5)

    def piece(which, ref, idx, i):
        return ref.at[idx, pl.ds(i * rows[which], rows[which])]

    def first_hop(way, which, i):
        return remote(piece(which, own[which], parity, i), piece(which, slots[which], way, i),
                      zsend.at[way, 0, which, i], zrecv.at[way, 0, which, i], device_id=ring[way])

    def next_hop(way, h, which, i):
        return remote(piece(which, slots[which], (h - 1) * 4 + way, i), piece(which, slots[which], h * 4 + way, i),
                      zsend.at[way, h, which, i], zrecv.at[way, h, which, i], device_id=ring[way])

    def last_hop(way, which, i):
        return remote(piece(which, slots[which], (half - 2) * 4 + way, i), piece(which, far[which], 0, i),
                      zsend.at[way, half - 1, which, i], zrecv.at[way, half - 1, which, i], device_id=ring[way])

    def side_hop(way, h, which, i):
        return remote(piece(which, slots[which], (h - 1) * 4 + way, i), piece(which, slots[which], (h - 1) * 4 + 2 + way, i),
                      hsend.at[way, h - 1, which, i], hrecv.at[way, h - 1, which, i], device_id=side_dev[way])

    def far_side(way, which, i):
        return remote(piece(which, far[which], 0, i), piece(which, far[which], 2, i),
                      hsend.at[way, half - 1, which, i], hrecv.at[way, half - 1, which, i], device_id=side_dev[way])

    def to_peer(kind, which, i):
        return remote(piece(which, far[which], 2 * kind, i), piece(which, far[which], 2 * kind + 1, i),
                      psend.at[kind, which, i], precv.at[kind, which, i], device_id=peer)

    def wait_ring(way, h, which, i):
        there = piece(which, slots[which], (h - 1) * 4 + way, i)
        remote(there, there, zsend.at[way, h - 1, which, i], zrecv.at[way, h - 1, which, i], device_id=ring[way]).wait_recv()

    def wait_side(h, which):
        def one(i, c):
            for way in range(2):
                side_hop(way, h, which, i).wait_recv()
            return c

        lax.fori_loop(0, CHUNKS, one, 0)

    for which in range(3):
        def start(i, c, which=which):
            for way in range(2):
                first_hop(way, which, i).start()
            return c

        lax.fori_loop(0, CHUNKS, start, 0)

    def load_gu(refs, idx, b):
        for m, buf in enumerate((g_buf, u_buf)):
            pltpu.make_async_copy(refs[m].at[idx], buf.at[b], gu_sem.at[b, m]).start()

    def wait_gu(b):
        for m, buf in enumerate((g_buf, u_buf)):
            pltpu.make_async_copy(own[m].at[0], buf.at[b], gu_sem.at[b, m]).wait()

    def load_d(ref, idx, b):
        pltpu.make_async_copy(ref.at[idx], d_buf.at[b], d_sem.at[b]).start()

    def wait_d(b):
        pltpu.make_async_copy(wd_ref.at[0], d_buf.at[b], d_sem.at[b]).wait()

    load_gu(own, 0, 0)
    load_gu(own, 1, 1)
    my_rows = pl.ds(mine, tok_n)
    tok = ((x_ref, x_all.at[my_rows]), (route_ref, route_all.at[core]), (gate_ref, gate_all.at[core]))
    for k, (src, dst) in enumerate(tok):
        remote(src, dst, tok_send.at[k], tok_recv.at[k], device_id=peer).start()
        pltpu.make_async_copy(src, dst, tok_sem.at[k]).start()
    y_acc[...] = jnp.zeros_like(y_acc)
    gate_rows[...] = jnp.zeros_like(gate_rows)
    for k, (src, dst) in reversed(list(enumerate(tok))):
        pltpu.make_async_copy(src, dst, tok_sem.at[k]).wait()
        remote(src, dst, tok_send.at[k], tok_recv.at[k], device_id=peer).wait()

    def dense(c, carry):
        route, gate = route_all[c], gate_all[c]
        for e in range(experts):
            gate_rows[e:e + 1, :] = jnp.sum(jnp.where(route == e, gate, 0.0), axis=0, keepdims=True)
        for b in range(tok_n // LANES):
            gate_cols[pl.ds(c * tok_n + b * LANES, LANES), :] = gate_rows[:, b * LANES:(b + 1) * LANES].T
        return carry

    lax.fori_loop(0, CORES, dense, 0)

    def expert_id(h, q, ring_core):
        src = (plane + planes + (2 * (q % 2) - 1) * h) % planes
        sub = parity + (q // 2) * (1 - 2 * parity)
        return (src * CORES + ring_core) * 2 + sub

    def front(row0, g, u, q, out0):
        x_tile = x_all[pl.ds(row0, tile)]
        a = jnp.dot(x_tile, g, preferred_element_type=jnp.float32)
        b = jnp.dot(x_tile, u, preferred_element_type=jnp.float32)
        hidden[q, pl.ds(out0, tile)] = (jax.nn.silu(a) * b).astype(jnp.bfloat16)

    def back(q, h0, d, row0, expert):
        out = jnp.dot(hidden[q, pl.ds(h0, tile)], d, preferred_element_type=jnp.float32).astype(jnp.bfloat16)
        gates = gate_cols[pl.ds(row0, tile)]
        lane = lax.broadcasted_iota(jnp.int32, gates.shape, 1)
        gate = jnp.sum(jnp.where(lane == expert, gates, 0.0), axis=1, keepdims=True)
        return jnp.where(gate > 0.0, gate * out.astype(jnp.float32), 0.0)

    def front_tile(t, q0):
        e, r = t // tiles, t % tiles

        @pl.when(r == 0)
        def _():
            wait_gu(e)

        front(r * tile, g_buf[e], u_buf[e], q0 + e, r * tile)

    def back_tile(t, stage):
        q, r = t // tiles, t % tiles

        @pl.when(r == 0)
        def _():
            wait_d(q)

        expert = jnp.where(stage == 0, (plane * CORES + core) * 2 + q, expert_id(stage, q, core))
        y_acc[pl.ds(r * tile, tile)] += back(q, r * tile, d_buf[q], r * tile, expert)

    def run(tile_fn, first, count, arg):
        def one(k, c):
            tile_fn(first + k, arg)
            return c

        lax.fori_loop(0, count, one, 0)

    def late_pair(h):
        for which in range(2):
            wait_side(h, which)
        load_gu(slots, (h - 1) * 4 + 2, 0)
        load_gu(slots, (h - 1) * 4 + 3, 1)

    def downs(h):
        wait_side(h, 2)
        for q in range(4):
            load_d(ds_ref, (h - 1) * 4 + q, q)

    per_front = 2 * tiles // CHUNKS
    per_back = 4 * tiles // CHUNKS
    halves = ([(0, i) for i in range(CHUNKS)] + [(2, i) for i in range(mid)],
              [(1, i) for i in range(CHUNKS)] + [(2, mid + i) for i in range(mid)])

    def stage(h, carry):
        for which in range(3):
            if which == 0:
                @pl.when(h > 1)
                def _():
                    late_pair(h - 1)
            elif which == 1:
                @pl.when(h == 1)
                def _():
                    load_d(wd_ref, 0, 0)
                    load_d(wd_ref, 1, 1)

                @pl.when(h > 1)
                def _():
                    downs(h - 1)
            else:
                load_gu(slots, (h - 1) * 4, 0)
                load_gu(slots, (h - 1) * 4 + 1, 1)

            def one(i, c, which=which):
                for way in range(2):
                    wait_ring(way, h, which, i)
                    far_ids = [k for w, k in halves[way] if w == which]

                    @pl.when(h < half - 1)
                    def _():
                        next_hop(way, h, which, i).start()

                    if far_ids:
                        @pl.when((h == half - 1) & (i >= far_ids[0]) & (i <= far_ids[-1]))
                        def _():
                            last_hop(way, which, i).start()
                    side_hop(way, h, which, i).start()
                if which == 0:
                    run(front_tile, i * per_front, per_front, 2 - 2 * jnp.where(h == 1, 1, 0))
                elif which == 1:
                    n = jnp.where(h == 1, per_back // 2, per_back)
                    run(back_tile, i * n, n, h - 1)
                else:
                    run(front_tile, i * per_front, per_front, 0)
                return c

            lax.fori_loop(0, CHUNKS, one, 0)
        return carry

    lax.fori_loop(1, half, stage, 0)

    def far_ring(way, which, i):
        last_hop(way, which, i).wait_recv()
        far_side(way, which, i).start()
        to_peer(0, which, i).start()

    def far_cross(way, which, i):
        far_side(way, which, i).wait_recv()
        to_peer(1, which, i).start()

    late_pair(half - 1)

    def far_a(i, c):
        for way in range(2):
            far_ring(way, way, i)

        @pl.when(i >= 2)
        def _():
            for way in range(2):
                far_cross(way, way, i - 2)
        run(front_tile, i * 2 * per_front, 2 * per_front, 2)
        return c

    lax.fori_loop(0, mid, far_a, 0)
    downs(half - 1)

    def far_b(i, c):
        for way in range(2):
            far_ring(way, way, i)
            far_cross(way, way, i - 2)
        run(back_tile, (i - mid) * 2 * per_back, 2 * per_back, half - 1)
        return c

    lax.fori_loop(mid, CHUNKS, far_b, 0)

    def part_copy(t):
        src = y_acc.at[pl.ds(theirs + t * tile, tile)]
        return remote(src, y_peer.at[pl.ds(t * tile, tile)], part_send.at[t], part_recv.at[t], device_id=peer)

    def far_front(f):
        def one(t, c):
            front(mine + t * tile, g_far[f], u_far[f], f, t * tile)
            return c

        lax.fori_loop(0, tiles_half, one, 0)

    def wait_peer(kind, which):
        def one(i, c):
            to_peer(kind, which, i).wait_recv()
            return c

        lax.fori_loop(0, CHUNKS, one, 0)

    for n in range(mid):
        for way in range(2):
            far_ring(way, 2, way * mid + n)
            if n < 2:
                far_cross(way, way, CHUNKS - 2 + n)
            else:
                far_cross(way, 2, way * mid + n - 2)
        if n == 1:
            for t in range(tiles_half):
                part_copy(t).start()
        if n % 2 == 1:
            for which in range(2):
                wait_peer(n // 2, which)
        if n < 4:
            far_front(n)

    def far_back(f, expert):
        def one(t, c):
            y_acc[pl.ds(mine + t * tile, tile)] += back(f, t * tile, d_far[f], mine + t * tile, expert)
            return c

        lax.fori_loop(0, tiles_half, one, 0)

    far_back(0, expert_id(half, 0, core))
    for way in range(2):
        far_cross(way, 2, way * mid + mid - 2)
    wait_peer(0, 2)
    far_back(1, expert_id(half, 0, 1 - core))
    for way in range(2):
        far_cross(way, 2, way * mid + mid - 1)
    far_back(2, expert_id(half, 2, core))
    for t in range(tiles_half):
        part_copy(t).wait()
    wait_peer(1, 2)

    def finish(t, c):
        part = pl.ds(t * tile, tile)
        row0 = mine + t * tile
        total = y_acc[pl.ds(row0, tile)] + y_peer[part] + back(3, t * tile, d_far[3], row0, expert_id(half, 2, 1 - core))
        y_ref[part] = total.astype(y_ref.dtype)
        return c

    lax.fori_loop(0, tiles_half, finish, 0)

    for which in range(3):
        def drain(i, c, which=which):
            for way in range(2):
                first_hop(way, which, i).wait_send()

                def per_stage(h, c2):
                    side_hop(way, h, which, i).wait_send()
                    return c2

                lax.fori_loop(1, half, per_stage, 0)

                def per_hop(h, c2):
                    next_hop(way, h, which, i).wait_send()
                    return c2

                lax.fori_loop(1, half - 1, per_hop, 0)
            for kind in range(2):
                to_peer(kind, which, i).wait_send()
            return c

        lax.fori_loop(0, CHUNKS, drain, 0)
    for way in range(2):
        for which, i in halves[way]:
            last_hop(way, which, i).wait_send()
            far_side(way, which, i).wait_send()


def moe(side, planes, x, route, gate, wg, wu, wd):
    tok_n, d_model = x.shape
    d_ff = wg.shape[2]
    half = planes // 2
    slots = (half - 1) * 4
    parts = tok_n // min(TILE, tok_n)
    bf = jnp.bfloat16
    f32 = jnp.float32
    any_spec = pl.BlockSpec(memory_space=pl.ANY)
    dma = pltpu.SemaphoreType.DMA
    rows = CORES * tok_n
    top_k = route.shape[0]
    out = pl.pallas_call(
        functools.partial(kernel, side, planes),
        out_shape=(
            jax.ShapeDtypeStruct((tok_n, d_model), bf),
            jax.ShapeDtypeStruct((slots, d_model, d_ff), bf),
            jax.ShapeDtypeStruct((slots, d_model, d_ff), bf),
            jax.ShapeDtypeStruct((slots, d_ff, d_model), bf),
        ),
        in_specs=[any_spec] * 6,
        out_specs=(pl.BlockSpec(memory_space=pltpu.VMEM),) + (any_spec,) * 3,
        scratch_shapes=[
            pltpu.VMEM((rows, d_model), bf),
            pltpu.VMEM((CORES, top_k, tok_n), jnp.int32),
            pltpu.VMEM((CORES, top_k, tok_n), f32),
            pltpu.VMEM((LANES, tok_n), f32),
            pltpu.VMEM((rows, LANES), f32),
            pltpu.VMEM((rows, d_model), f32),
            pltpu.VMEM((tok_n, d_model), f32),
            pltpu.VMEM((4, rows, d_ff), bf),
            pltpu.VMEM((2, d_model, d_ff), bf),
            pltpu.VMEM((2, d_model, d_ff), bf),
            pltpu.VMEM((4, d_ff, d_model), bf),
            pltpu.VMEM((4, d_model, d_ff), bf),
            pltpu.VMEM((4, d_model, d_ff), bf),
            pltpu.VMEM((4, d_ff, d_model), bf),
            dma((2, half, 3, CHUNKS)),
            dma((2, half, 3, CHUNKS)),
            dma((2, half, 3, CHUNKS)),
            dma((2, half, 3, CHUNKS)),
            dma((2, 3, CHUNKS)),
            dma((2, 3, CHUNKS)),
            dma((2, 2)),
            dma((4,)),
            dma((3,)),
            dma((3,)),
            dma((3,)),
            dma((parts,)),
            dma((parts,)),
        ],
        compiler_params=pltpu.CompilerParams(
            collective_id=0, has_side_effects=True, vmem_limit_bytes=50 * 1024 * 1024),
        name="stream_experts",
    )(x, route, gate, wg, wu, wd)
    return out[0]


def solution(mesh):
    planes = mesh.shape["ep"] // CORES
    side = math.isqrt(mesh.shape["dp"])
    row_spec = P(("dp", "ep"))
    expert_spec = P("ep")

    def local_step(tok_loc, route_loc, gate_loc, wg_loc, wu_loc, wd_loc):
        return moe(side, planes, tok_loc, route_loc.T, gate_loc.T, wg_loc, wu_loc, wd_loc)

    return jax.shard_map(local_step, mesh=mesh, in_specs=(row_spec, row_spec, row_spec, expert_spec, expert_spec, expert_spec), out_specs=row_spec, check_vma=False)
```

```python
import functools
import math

import jax
import jax.numpy as jnp
from jax import lax
from jax.experimental import pallas as pl
from jax.experimental.pallas import tpu as pltpu
from jax.sharding import PartitionSpec as P

CORES = 2
CHUNKS = 4
TILE = 256
LANES = 128


def kernel(side, planes, x_ref, route_ref, gate_ref, wg_ref, wu_ref, wd_ref,
           y_ref, gs_ref, us_ref, ds_ref,
           x_all, route_all, gate_all, gate_rows, gate_cols, y_acc, y_peer, hidden,
           g_buf, u_buf, d_buf, g_far, u_far, d_far,
           zsend, zrecv, hsend, hrecv, psend, precv, gu_sem, d_sem, tok_sem, tok_send, tok_recv, part_send, part_recv):
    half = planes // 2
    tok_n = x_ref.shape[0]
    tile = min(TILE, tok_n)
    tiles_half = tok_n // tile
    tiles = CORES * tiles_half
    experts = planes * CORES * 2
    col = lax.axis_index("dp")
    pos = lax.axis_index("ep")
    core = pos % CORES
    plane = pos // CORES
    cx, cy = col // side, col % side
    parity = (cx + cy) % 2
    col_x = col + side * (1 - 2 * (cx % 2))
    col_y = col + 1 - 2 * (cy % 2)
    up = (pos + CORES) % (planes * CORES)
    down = (pos + (planes - 1) * CORES) % (planes * CORES)
    peer = {"ep": pos + 1 - 2 * core}
    ring = ({"ep": up}, {"ep": down})
    side_dev = ({"dp": col_x}, {"dp": col_y})
    own = (wg_ref, wu_ref, wd_ref)
    slots = (gs_ref, us_ref, ds_ref)
    far = (g_far, u_far, d_far)
    rows = tuple(w.shape[1] // CHUNKS for w in own)
    mid = CHUNKS // 2
    mine = core * tok_n
    theirs = (1 - core) * tok_n
    remote = pltpu.make_async_remote_copy

    barrier = pltpu.get_barrier_semaphore()
    for dev in (*ring, *side_dev, peer):
        pl.semaphore_signal(barrier, inc=1, device_id=dev)
    pl.semaphore_wait(barrier, 5)

    def piece(which, ref, idx, i):
        return ref.at[idx, pl.ds(i * rows[which], rows[which])]

    def first_hop(way, which, i):
        return remote(piece(which, own[which], parity, i), piece(which, slots[which], way, i),
                      zsend.at[way, 0, which, i], zrecv.at[way, 0, which, i], device_id=ring[way])

    def next_hop(way, h, which, i):
        return remote(piece(which, slots[which], (h - 1) * 4 + way, i), piece(which, slots[which], h * 4 + way, i),
                      zsend.at[way, h, which, i], zrecv.at[way, h, which, i], device_id=ring[way])

    def last_hop(way, which, i):
        return remote(piece(which, slots[which], (half - 2) * 4 + way, i), piece(which, far[which], 0, i),
                      zsend.at[way, half - 1, which, i], zrecv.at[way, half - 1, which, i], device_id=ring[way])

    def side_hop(way, h, which, i):
        return remote(piece(which, slots[which], (h - 1) * 4 + way, i), piece(which, slots[which], (h - 1) * 4 + 2 + way, i),
                      hsend.at[way, h - 1, which, i], hrecv.at[way, h - 1, which, i], device_id=side_dev[way])

    def far_side(way, which, i):
        return remote(piece(which, far[which], 0, i), piece(which, far[which], 2, i),
                      hsend.at[way, half - 1, which, i], hrecv.at[way, half - 1, which, i], device_id=side_dev[way])

    def to_peer(kind, which, i):
        return remote(piece(which, far[which], 2 * kind, i), piece(which, far[which], 2 * kind + 1, i),
                      psend.at[kind, which, i], precv.at[kind, which, i], device_id=peer)

    def wait_ring(way, h, which, i):
        there = piece(which, slots[which], (h - 1) * 4 + way, i)
        remote(there, there, zsend.at[way, h - 1, which, i], zrecv.at[way, h - 1, which, i], device_id=ring[way]).wait_recv()

    def wait_side(h, which):
        def one(i, c):
            for way in range(2):
                side_hop(way, h, which, i).wait_recv()
            return c

        lax.fori_loop(0, CHUNKS, one, 0)

    for which in range(3):
        def start(i, c, which=which):
            for way in range(2):
                first_hop(way, which, i).start()
            return c

        lax.fori_loop(0, CHUNKS, start, 0)

    def load_gu(refs, idx, b):
        for m, buf in enumerate((g_buf, u_buf)):
            pltpu.make_async_copy(refs[m].at[idx], buf.at[b], gu_sem.at[b, m]).start()

    def wait_gu(b):
        for m, buf in enumerate((g_buf, u_buf)):
            pltpu.make_async_copy(own[m].at[0], buf.at[b], gu_sem.at[b, m]).wait()

    def load_d(ref, idx, b):
        pltpu.make_async_copy(ref.at[idx], d_buf.at[b], d_sem.at[b]).start()

    def wait_d(b):
        pltpu.make_async_copy(wd_ref.at[0], d_buf.at[b], d_sem.at[b]).wait()

    load_gu(own, 0, 0)
    load_gu(own, 1, 1)
    my_rows = pl.ds(mine, tok_n)
    tok = ((x_ref, x_all.at[my_rows]), (route_ref, route_all.at[core]), (gate_ref, gate_all.at[core]))
    for k, (src, dst) in enumerate(tok):
        remote(src, dst, tok_send.at[k], tok_recv.at[k], device_id=peer).start()
        pltpu.make_async_copy(src, dst, tok_sem.at[k]).start()
    y_acc[...] = jnp.zeros_like(y_acc)
    gate_rows[...] = jnp.zeros_like(gate_rows)
    for k, (src, dst) in reversed(list(enumerate(tok))):
        pltpu.make_async_copy(src, dst, tok_sem.at[k]).wait()
        remote(src, dst, tok_send.at[k], tok_recv.at[k], device_id=peer).wait()

    def dense(c, carry):
        route, gate = route_all[c], gate_all[c]
        for e in range(experts):
            gate_rows[e:e + 1, :] = jnp.sum(jnp.where(route == e, gate, 0.0), axis=0, keepdims=True)
        for b in range(tok_n // LANES):
            gate_cols[pl.ds(c * tok_n + b * LANES, LANES), :] = gate_rows[:, b * LANES:(b + 1) * LANES].T
        return carry

    lax.fori_loop(0, CORES, dense, 0)

    def expert_id(h, q, ring_core):
        src = (plane + planes + (2 * (q % 2) - 1) * h) % planes
        sub = parity + (q // 2) * (1 - 2 * parity)
        return (src * CORES + ring_core) * 2 + sub

    def front(row0, g, u, q, out0):
        x_tile = x_all[pl.ds(row0, tile)]
        a = jnp.dot(x_tile, g, preferred_element_type=jnp.float32)
        b = jnp.dot(x_tile, u, preferred_element_type=jnp.float32)
        hidden[q, pl.ds(out0, tile)] = (jax.nn.silu(a) * b).astype(jnp.bfloat16)

    def back(q, h0, d, row0, expert):
        out = jnp.dot(hidden[q, pl.ds(h0, tile)], d, preferred_element_type=jnp.float32).astype(jnp.bfloat16)
        gates = gate_cols[pl.ds(row0, tile)]
        lane = lax.broadcasted_iota(jnp.int32, gates.shape, 1)
        gate = jnp.sum(jnp.where(lane == expert, gates, 0.0), axis=1, keepdims=True)
        return jnp.where(gate > 0.0, gate * out.astype(jnp.float32), 0.0)

    def front_tile(t, q0):
        e, r = t // tiles, t % tiles

        @pl.when(r == 0)
        def _():
            wait_gu(e)

        front(r * tile, g_buf[e], u_buf[e], q0 + e, r * tile)

    def back_tile(t, stage):
        q, r = t // tiles, t % tiles

        @pl.when(r == 0)
        def _():
            wait_d(q)

        expert = jnp.where(stage == 0, (plane * CORES + core) * 2 + q, expert_id(stage, q, core))
        y_acc[pl.ds(r * tile, tile)] += back(q, r * tile, d_buf[q], r * tile, expert)

    def run(tile_fn, first, count, arg):
        def one(k, c):
            tile_fn(first + k, arg)
            return c

        lax.fori_loop(0, count, one, 0)

    def late_pair(h):
        for which in range(2):
            wait_side(h, which)
        load_gu(slots, (h - 1) * 4 + 2, 0)
        load_gu(slots, (h - 1) * 4 + 3, 1)

    def downs(h):
        wait_side(h, 2)
        for q in range(4):
            load_d(ds_ref, (h - 1) * 4 + q, q)

    per_front = 2 * tiles // CHUNKS
    per_back = 4 * tiles // CHUNKS
    halves = ([(0, i) for i in range(CHUNKS)] + [(2, i) for i in range(mid)],
              [(1, i) for i in range(CHUNKS)] + [(2, mid + i) for i in range(mid)])

    def stage(h, carry):
        for which in range(3):
            if which == 0:
                @pl.when(h > 1)
                def _():
                    late_pair(h - 1)
            elif which == 1:
                @pl.when(h == 1)
                def _():
                    load_d(wd_ref, 0, 0)
                    load_d(wd_ref, 1, 1)

                @pl.when(h > 1)
                def _():
                    downs(h - 1)
            else:
                load_gu(slots, (h - 1) * 4, 0)
                load_gu(slots, (h - 1) * 4 + 1, 1)

            def one(i, c, which=which):
                for way in range(2):
                    wait_ring(way, h, which, i)
                    far_ids = [k for w, k in halves[way] if w == which]

                    @pl.when(h < half - 1)
                    def _():
                        next_hop(way, h, which, i).start()

                    if far_ids:
                        @pl.when((h == half - 1) & (i >= far_ids[0]) & (i <= far_ids[-1]))
                        def _():
                            last_hop(way, which, i).start()
                    side_hop(way, h, which, i).start()
                if which == 0:
                    run(front_tile, i * per_front, per_front, 2 - 2 * jnp.where(h == 1, 1, 0))
                elif which == 1:
                    n = jnp.where(h == 1, per_back // 2, per_back)
                    run(back_tile, i * n, n, h - 1)
                else:
                    run(front_tile, i * per_front, per_front, 0)
                return c

            lax.fori_loop(0, CHUNKS, one, 0)
        return carry

    lax.fori_loop(1, half, stage, 0)

    def far_ring(way, which, i):
        last_hop(way, which, i).wait_recv()
        far_side(way, which, i).start()
        to_peer(0, which, i).start()

    def far_cross(way, which, i):
        far_side(way, which, i).wait_recv()
        to_peer(1, which, i).start()

    late_pair(half - 1)

    def far_a(i, c):
        for way in range(2):
            far_ring(way, way, i)

        @pl.when(i >= 2)
        def _():
            for way in range(2):
                far_cross(way, way, i - 2)
        run(front_tile, i * 2 * per_front, 2 * per_front, 2)
        return c

    lax.fori_loop(0, mid, far_a, 0)
    downs(half - 1)

    def far_b(i, c):
        for way in range(2):
            far_ring(way, way, i)
            far_cross(way, way, i - 2)
        run(back_tile, (i - mid) * 2 * per_back, 2 * per_back, half - 1)
        return c

    lax.fori_loop(mid, CHUNKS, far_b, 0)

    def part_copy(t):
        src = y_acc.at[pl.ds(theirs + t * tile, tile)]
        return remote(src, y_peer.at[pl.ds(t * tile, tile)], part_send.at[t], part_recv.at[t], device_id=peer)

    def far_front(f):
        def one(t, c):
            front(mine + t * tile, g_far[f], u_far[f], f, t * tile)
            return c

        lax.fori_loop(0, tiles_half, one, 0)

    def wait_peer(kind, which):
        def one(i, c):
            to_peer(kind, which, i).wait_recv()
            return c

        lax.fori_loop(0, CHUNKS, one, 0)

    for n in range(mid):
        for way in range(2):
            far_ring(way, 2, way * mid + n)
            if n < 2:
                far_cross(way, way, CHUNKS - 2 + n)
            else:
                far_cross(way, 2, way * mid + n - 2)
        if n == mid // 2:
            for t in range(tiles_half):
                part_copy(t).start()
        for f in range(n * 4 // mid, (n + 1) * 4 // mid):
            if f % 2 == 1:
                for which in range(2):
                    wait_peer(f // 2, which)
            far_front(f)

    def far_back(f, expert):
        def one(t, c):
            y_acc[pl.ds(mine + t * tile, tile)] += back(f, t * tile, d_far[f], mine + t * tile, expert)
            return c

        lax.fori_loop(0, tiles_half, one, 0)

    far_back(0, expert_id(half, 0, core))
    for way in range(2):
        far_cross(way, 2, way * mid + mid - 2)
    wait_peer(0, 2)
    far_back(1, expert_id(half, 0, 1 - core))
    for way in range(2):
        far_cross(way, 2, way * mid + mid - 1)
    far_back(2, expert_id(half, 2, core))
    for t in range(tiles_half):
        part_copy(t).wait()
    wait_peer(1, 2)

    def finish(t, c):
        part = pl.ds(t * tile, tile)
        row0 = mine + t * tile
        total = y_acc[pl.ds(row0, tile)] + y_peer[part] + back(3, t * tile, d_far[3], row0, expert_id(half, 2, 1 - core))
        y_ref[part] = total.astype(y_ref.dtype)
        return c

    lax.fori_loop(0, tiles_half, finish, 0)

    for which in range(3):
        def drain(i, c, which=which):
            for way in range(2):
                first_hop(way, which, i).wait_send()

                def per_stage(h, c2):
                    side_hop(way, h, which, i).wait_send()
                    return c2

                lax.fori_loop(1, half, per_stage, 0)

                def per_hop(h, c2):
                    next_hop(way, h, which, i).wait_send()
                    return c2

                lax.fori_loop(1, half - 1, per_hop, 0)
            for kind in range(2):
                to_peer(kind, which, i).wait_send()
            return c

        lax.fori_loop(0, CHUNKS, drain, 0)
    for way in range(2):
        for which, i in halves[way]:
            last_hop(way, which, i).wait_send()
            far_side(way, which, i).wait_send()


def moe(side, planes, x, route, gate, wg, wu, wd):
    tok_n, d_model = x.shape
    d_ff = wg.shape[2]
    half = planes // 2
    slots = (half - 1) * 4
    parts = tok_n // min(TILE, tok_n)
    bf = jnp.bfloat16
    f32 = jnp.float32
    any_spec = pl.BlockSpec(memory_space=pl.ANY)
    dma = pltpu.SemaphoreType.DMA
    rows = CORES * tok_n
    top_k = route.shape[0]
    out = pl.pallas_call(
        functools.partial(kernel, side, planes),
        out_shape=(
            jax.ShapeDtypeStruct((tok_n, d_model), bf),
            jax.ShapeDtypeStruct((slots, d_model, d_ff), bf),
            jax.ShapeDtypeStruct((slots, d_model, d_ff), bf),
            jax.ShapeDtypeStruct((slots, d_ff, d_model), bf),
        ),
        in_specs=[pl.BlockSpec(memory_space=pltpu.HBM)] * 6,
        out_specs=(pl.BlockSpec(memory_space=pltpu.VMEM),) + (any_spec,) * 3,
        scratch_shapes=[
            pltpu.VMEM((rows, d_model), bf),
            pltpu.VMEM((CORES, top_k, tok_n), jnp.int32),
            pltpu.VMEM((CORES, top_k, tok_n), f32),
            pltpu.VMEM((LANES, tok_n), f32),
            pltpu.VMEM((rows, LANES), f32),
            pltpu.VMEM((rows, d_model), f32),
            pltpu.VMEM((tok_n, d_model), f32),
            pltpu.VMEM((4, rows, d_ff), bf),
            pltpu.VMEM((2, d_model, d_ff), bf),
            pltpu.VMEM((2, d_model, d_ff), bf),
            pltpu.VMEM((4, d_ff, d_model), bf),
            pltpu.VMEM((4, d_model, d_ff), bf),
            pltpu.VMEM((4, d_model, d_ff), bf),
            pltpu.VMEM((4, d_ff, d_model), bf),
            dma((2, half, 3, CHUNKS)),
            dma((2, half, 3, CHUNKS)),
            dma((2, half, 3, CHUNKS)),
            dma((2, half, 3, CHUNKS)),
            dma((2, 3, CHUNKS)),
            dma((2, 3, CHUNKS)),
            dma((2, 2)),
            dma((4,)),
            dma((3,)),
            dma((3,)),
            dma((3,)),
            dma((parts,)),
            dma((parts,)),
        ],
        compiler_params=pltpu.CompilerParams(
            collective_id=0, has_side_effects=True, vmem_limit_bytes=50 * 1024 * 1024),
        name="stream_experts",
    )(x, route, gate, wg, wu, wd)
    return out[0]


def solution(mesh):
    planes = mesh.shape["ep"] // CORES
    side = math.isqrt(mesh.shape["dp"])
    row_spec = P(("dp", "ep"))
    expert_spec = P("ep")

    def local_step(tok_loc, route_loc, gate_loc, wg_loc, wu_loc, wd_loc):
        return moe(side, planes, tok_loc, route_loc.T, gate_loc.T, wg_loc, wu_loc, wd_loc)

    return jax.shard_map(local_step, mesh=mesh, in_specs=(row_spec, row_spec, row_spec, expert_spec, expert_spec, expert_spec), out_specs=row_spec, check_vma=False)
```

```python
import functools
import math

import jax
import jax.numpy as jnp
from jax import lax
from jax.experimental import pallas as pl
from jax.experimental.pallas import tpu as pltpu
from jax.sharding import PartitionSpec as P

CORES = 2
CHUNKS = 4
TILE = 512
SUBS = 4
LANES = 128


def kernel(side, planes, x_ref, route_ref, gate_ref, wg_ref, wu_ref, wd_ref,
           y_ref, gs_ref, us_ref, ds_ref,
           x_all, route_all, gate_all, gate_rows, gate_cols, y_acc, y_peer, hidden,
           g_buf, u_buf, d_buf, g_far, u_far, d_far,
           zsend, zrecv, hsend, hrecv, psend, precv, far_recv, first_recv, last_recv, cross_recv,
           gu_sem, d_sem, tok_sem, tok_send, tok_recv, part_send, part_recv):
    half = planes // 2
    tok_n = x_ref.shape[0]
    tile = min(TILE, tok_n)
    tiles_half = tok_n // tile
    tiles = CORES * tiles_half
    experts = planes * CORES * 2
    col = lax.axis_index("dp")
    pos = lax.axis_index("ep")
    core = pos % CORES
    plane = pos // CORES
    cx, cy = col // side, col % side
    parity = (cx + cy) % 2
    col_x = col + side * (1 - 2 * (cx % 2))
    col_y = col + 1 - 2 * (cy % 2)
    up = (pos + CORES) % (planes * CORES)
    down = (pos + (planes - 1) * CORES) % (planes * CORES)
    peer = {"ep": pos + 1 - 2 * core}
    ring = ({"ep": up}, {"ep": down})
    side_dev = ({"dp": col_x}, {"dp": col_y})
    own = (wg_ref, wu_ref, wd_ref)
    slots = (gs_ref, us_ref, ds_ref)
    far = (g_far, u_far, d_far)
    rows = tuple(w.shape[1] // CHUNKS for w in own)
    mid = CHUNKS // 2
    mine = core * tok_n
    theirs = (1 - core) * tok_n
    remote = pltpu.make_async_remote_copy

    barrier = pltpu.get_barrier_semaphore()
    for dev in (*ring, *side_dev, peer):
        pl.semaphore_signal(barrier, inc=1, device_id=dev)
    with jax.named_scope("entry"):
        pl.semaphore_wait(barrier, 5)

    def piece(which, ref, idx, i):
        return ref.at[idx, pl.ds(i * rows[which], rows[which])]

    def first_hop(way, which, i):
        return remote(piece(which, own[which], parity, i), piece(which, slots[which], way, i),
                      zsend.at[way, which], zrecv.at[way, 0, which, i], device_id=ring[way])

    def next_hop(way, h, which, i):
        return remote(piece(which, slots[which], (h - 1) * 4 + way, i), piece(which, slots[which], h * 4 + way, i),
                      zsend.at[way, which], zrecv.at[way, h, which, i], device_id=ring[way])

    def last_hop(way, which, i):
        return remote(piece(which, slots[which], (half - 2) * 4 + way, i), piece(which, far[which], 0, i),
                      zsend.at[way, which], zrecv.at[way, half - 1, which, i], device_id=ring[way])

    def side_hop(way, h, which, i):
        return remote(piece(which, slots[which], (h - 1) * 4 + way, i), piece(which, slots[which], (h - 1) * 4 + 2 + way, i),
                      hsend.at[way, which], hrecv.at[way, h - 1, which], device_id=side_dev[way])

    def far_side(way, which, i):
        return remote(piece(which, far[which], 0, i), piece(which, far[which], 2, i),
                      hsend.at[way, which], far_recv.at[way, which, i], device_id=side_dev[way])

    def to_peer(kind, which, i):
        return remote(piece(which, far[which], 2 * kind, i), piece(which, far[which], 2 * kind + 1, i),
                      psend.at[kind, which], precv.at[kind, which], device_id=peer)

    def cut(ref, idx, which, i, n):
        size = rows[which] // SUBS
        return ref.at[idx, pl.ds(i * rows[which] + n * size, size)]

    def first_cut(way, n):
        return remote(cut(wg_ref, parity, 0, 0, n), cut(gs_ref, way, 0, 0, n),
                      zsend.at[way, 0], first_recv.at[way, n], device_id=ring[way])

    def side_cut(way, n):
        return remote(cut(gs_ref, way, 0, 0, n), cut(gs_ref, 2 + way, 0, 0, n),
                      hsend.at[way, 0], hrecv.at[way, 0, 0], device_id=side_dev[way])

    def last_piece(way):
        return way * mid + mid - 1

    def last_cut(way, n):
        return remote(cut(ds_ref, (half - 2) * 4 + way, 2, last_piece(way), n), cut(d_far, 0, 2, last_piece(way), n),
                      zsend.at[way, 2], last_recv.at[way, n], device_id=ring[way])

    def last_side_cut(way, n):
        return remote(cut(d_far, 0, 2, last_piece(way), n), cut(d_far, 2, 2, last_piece(way), n),
                      hsend.at[way, 2], cross_recv.at[way, n], device_id=side_dev[way])

    def peer_cut(kind, way, n):
        return remote(cut(d_far, 2 * kind, 2, last_piece(way), n), cut(d_far, 2 * kind + 1, 2, last_piece(way), n),
                      psend.at[kind, 2], precv.at[kind, 2], device_id=peer)

    def wait_ring(way, h, which, i):
        there = piece(which, slots[which], (h - 1) * 4 + way, i)
        remote(there, there, zsend.at[way, which], zrecv.at[way, h - 1, which, i], device_id=ring[way]).wait_recv()

    def wait_side(h, which):
        for way in range(2):
            there = slots[which].at[(h - 1) * 4 + 2 + way]
            with jax.named_scope(f"wait_s{which}"):
                remote(there, there, hsend.at[way, which], hrecv.at[way, h - 1, which], device_id=side_dev[way]).wait_recv()

    for n in range(SUBS):
        for way in range(2):
            first_cut(way, n).start()
    for which in range(3):
        def start(i, c, which=which):
            for way in range(2):
                first_hop(way, which, i).start()
            return c

        lax.fori_loop(1 if which == 0 else 0, CHUNKS, start, 0)

    def load_gu(refs, idx, b):
        for m, buf in enumerate((g_buf, u_buf)):
            pltpu.make_async_copy(refs[m].at[idx], buf.at[b], gu_sem.at[b, m]).start()

    def wait_gu(b):
        for m, buf in enumerate((g_buf, u_buf)):
            pltpu.make_async_copy(own[m].at[0], buf.at[b], gu_sem.at[b, m]).wait()

    def load_d(ref, idx, b):
        pltpu.make_async_copy(ref.at[idx], d_buf.at[b], d_sem.at[b]).start()

    def wait_d(b):
        pltpu.make_async_copy(wd_ref.at[0], d_buf.at[b], d_sem.at[b]).wait()

    load_gu(own, 0, 0)
    load_gu(own, 1, 1)
    my_rows = pl.ds(mine, tok_n)
    tok = ((x_ref, x_all.at[my_rows]), (route_ref, route_all.at[core]), (gate_ref, gate_all.at[core]))
    for k, (src, dst) in enumerate(tok):
        remote(src, dst, tok_send.at[k], tok_recv.at[k], device_id=peer).start()
        pltpu.make_async_copy(src, dst, tok_sem.at[k]).start()
    y_acc[...] = jnp.zeros_like(y_acc)
    gate_rows[...] = jnp.zeros_like(gate_rows)
    def first_forward(n):
        for way in range(2):
            with jax.named_scope("wait_first"):
                first_cut(way, n).wait_recv()
            side_cut(way, n).start()

    first_forward(0)
    for k, (src, dst) in reversed(list(enumerate(tok))):
        pltpu.make_async_copy(src, dst, tok_sem.at[k]).wait()
        remote(src, dst, tok_send.at[k], tok_recv.at[k], device_id=peer).wait()

    def dense(c, carry):
        route, gate = route_all[c], gate_all[c]
        for e in range(experts):
            gate_rows[e:e + 1, :] = jnp.sum(jnp.where(route == e, gate, 0.0), axis=0, keepdims=True)
        for b in range(tok_n // LANES):
            gate_cols[pl.ds(c * tok_n + b * LANES, LANES), :] = gate_rows[:, b * LANES:(b + 1) * LANES].T
        return carry

    for n in range(1, SUBS):
        first_forward(n)
        if n <= CORES:
            dense(n - 1, 0)

    def expert_id(h, q, ring_core):
        src = (plane + planes + (2 * (q % 2) - 1) * h) % planes
        sub = parity + (q // 2) * (1 - 2 * parity)
        return (src * CORES + ring_core) * 2 + sub

    def front(row0, g, u, q, out0):
        x_tile = x_all[pl.ds(row0, tile)]
        a = jnp.dot(x_tile, g, preferred_element_type=jnp.float32)
        b = jnp.dot(x_tile, u, preferred_element_type=jnp.float32)
        hidden[q, pl.ds(out0, tile)] = (jax.nn.silu(a) * b).astype(jnp.bfloat16)

    def back(q, h0, d, row0, expert):
        out = jnp.dot(hidden[q, pl.ds(h0, tile)], d, preferred_element_type=jnp.float32).astype(jnp.bfloat16)
        gates = gate_cols[pl.ds(row0, tile)]
        lane = lax.broadcasted_iota(jnp.int32, gates.shape, 1)
        gate = jnp.sum(jnp.where(lane == expert, gates, 0.0), axis=1, keepdims=True)
        return jnp.where(gate > 0.0, gate * out.astype(jnp.float32), 0.0)

    def front_tile(t, q0):
        e, r = t // tiles, t % tiles

        @pl.when(r == 0)
        def _():
            wait_gu(e)

        front(r * tile, g_buf[e], u_buf[e], q0 + e, r * tile)

    def back_tile(t, stage):
        q, r = t // tiles, t % tiles

        @pl.when(r == 0)
        def _():
            wait_d(q)

        expert = jnp.where(stage == 0, (plane * CORES + core) * 2 + q, expert_id(stage, q, core))
        y_acc[pl.ds(r * tile, tile)] += back(q, r * tile, d_buf[q], r * tile, expert)

    def run(tile_fn, first, count, arg):
        def one(k, c):
            tile_fn(first + k, arg)
            return c

        with jax.named_scope(tile_fn.__name__):
            lax.fori_loop(0, count, one, 0)

    def ups(h, first):
        if first:
            for which in range(2):
                wait_side(h, which)
        for e in range(2):
            load_gu(slots, (h - 1) * 4 + first + e, e)

    def downs(h):
        wait_side(h, 2)
        for q in range(4):
            load_d(ds_ref, (h - 1) * 4 + q, q)

    per_front = 4 * tiles // CHUNKS
    per_back = 4 * tiles // CHUNKS
    halves = ([(0, i) for i in range(CHUNKS)] + [(2, i) for i in range(mid)],
              [(1, i) for i in range(CHUNKS)] + [(2, mid + i) for i in range(mid)])

    def stage(h, carry):
        for which in range(3):
            if which == 0:
                @pl.when(h > 1)
                def _():
                    downs(h - 1)
            elif which == 1:
                @pl.when(h == 1)
                def _():
                    load_d(wd_ref, 0, 0)
                    load_d(wd_ref, 1, 1)
            else:
                ups(h, 0)

            def one(i, c, which=which):
                for way in range(2):
                    def take():
                        with jax.named_scope(f"wait_z{which}"):
                            wait_ring(way, h, which, i)
                        side_hop(way, h, which, i).start()

                    if which == 0:
                        pl.when((h > 1) | (i > 0))(take)
                    else:
                        take()
                    far_ids = [k for w, k in halves[way] if w == which]

                    @pl.when(h < half - 1)
                    def _():
                        next_hop(way, h, which, i).start()

                    if far_ids:
                        whole = far_ids[-1] - (which == 2)

                        @pl.when((h == half - 1) & (i >= far_ids[0]) & (i <= whole))
                        def _():
                            last_hop(way, which, i).start()

                    if which == 2:
                        @pl.when((h == half - 1) & (i == last_piece(way)))
                        def _():
                            for n in range(SUBS):
                                last_cut(way, n).start()
                if which == 0:
                    @pl.when(h == 1)
                    def _():
                        run(front_tile, i * (per_front // 2), per_front // 2, 0)

                    @pl.when(h > 1)
                    def _():
                        run(back_tile, i * per_back, per_back, h - 1)
                elif which == 1:
                    @pl.when(h == 1)
                    def _():
                        run(back_tile, i * (per_back // 2), per_back // 2, 0)
                else:
                    @pl.when(i == mid)
                    def _():
                        ups(h, 2)

                    @pl.when(i < mid)
                    def _():
                        run(front_tile, i * per_front, per_front, 0)

                    @pl.when(i >= mid)
                    def _():
                        run(front_tile, (i - mid) * per_front, per_front, 2)
                return c

            lax.fori_loop(0, CHUNKS, one, 0)
        return carry

    lax.fori_loop(1, half, stage, 0)

    def far_ring(way, which, i):
        with jax.named_scope("wait_zfar"):
            last_hop(way, which, i).wait_recv()
        far_side(way, which, i).start()
        to_peer(0, which, i).start()

    def far_cross(way, which, i):
        with jax.named_scope("wait_sfar"):
            far_side(way, which, i).wait_recv()
        to_peer(1, which, i).start()

    def whole(kind, which):
        there = far[which].at[2 * kind + 1]
        return remote(there, there, psend.at[kind, which], precv.at[kind, which], device_id=peer)

    downs(half - 1)

    def far_a(i, c):
        for way in range(2):
            far_ring(way, way, i)

        @pl.when(i >= 2)
        def _():
            for way in range(2):
                far_cross(way, way, i - 2)
        run(back_tile, i * per_back, per_back, half - 1)
        return c

    lax.fori_loop(0, CHUNKS, far_a, 0)

    def part_copy(t):
        src = y_acc.at[pl.ds(theirs + t * tile, tile)]
        return remote(src, y_peer.at[pl.ds(t * tile, tile)], part_send.at[t], part_recv.at[t], device_id=peer)

    def far_front(f, t):
        front(mine + t * tile, g_far[f], u_far[f], f, t * tile)

    for n in range(mid - 1):
        for way in range(2):
            far_ring(way, 2, way * mid + n)
            if n < 2:
                far_cross(way, way, CHUNKS - 2 + n)
            else:
                far_cross(way, 2, way * mid + n - 2)

    def front_pair(f0, inside):
        def one(t, c):
            inside(t)
            with jax.named_scope("far_front"):
                far_front(f0 + t // tiles_half, t % tiles_half)
            return c

        lax.fori_loop(0, 2 * tiles_half, one, 0)

    def late_peer(t):
        @pl.when(t == tiles_half)
        def _():
            for which in range(2):
                whole(0, which).wait_recv()

    front_pair(0, late_peer)
    for t in range(tiles_half):
        part_copy(t).start()
    for way in range(2):
        for n in range(max(mid - 3, -1), mid - 2):
            far_cross(way, 2, way * mid + n) if n >= 0 else far_cross(way, way, CHUNKS - 1)

    def last_forward(t):
        @pl.when(t == tiles_half)
        def _():
            for which in range(2):
                whole(1, which).wait_recv()
        for n in range(SUBS):
            @pl.when(t == n * 2 * tiles_half // SUBS)
            def _():
                for way in range(2):
                    with jax.named_scope("wait_zcut"):
                        last_cut(way, n).wait_recv()
                    last_side_cut(way, n).start()
                    peer_cut(0, way, n).start()

    front_pair(2, last_forward)

    def far_back(f, expert):
        def one(t, c):
            y_acc[pl.ds(mine + t * tile, tile)] += back(f, t * tile, d_far[f], mine + t * tile, expert)
            return c

        with jax.named_scope("far_back"):
            lax.fori_loop(0, tiles_half, one, 0)

    for way in range(2):
        for n in range(mid - 2, mid - 1):
            far_cross(way, 2, way * mid + n)
    far_back(0, expert_id(half, 0, core))
    whole(0, 2).wait_recv()

    def last_cross(n):
        for way in range(2):
            with jax.named_scope("wait_scut"):
                last_side_cut(way, n).wait_recv()
            peer_cut(1, way, n).start()

    for n in range(SUBS - 1):
        last_cross(n)
    far_back(1, expert_id(half, 0, 1 - core))
    last_cross(SUBS - 1)
    far_back(2, expert_id(half, 2, core))
    with jax.named_scope("wait_part"):
        for t in range(tiles_half):
            part_copy(t).wait()
    with jax.named_scope("wait_peer_last"):
        whole(1, 2).wait_recv()

    def finish(t, c):
        part = pl.ds(t * tile, tile)
        row0 = mine + t * tile
        total = y_acc[pl.ds(row0, tile)] + y_peer[part] + back(3, t * tile, d_far[3], row0, expert_id(half, 2, 1 - core))
        y_ref[part] = total.astype(y_ref.dtype)
        return c

    with jax.named_scope("finish"):
        lax.fori_loop(0, tiles_half, finish, 0)

    with jax.named_scope("drain"):
      for which in range(3):
        for way in range(2):
            if which == 2:
                there = ds_ref.at[pl.ds(0, 2 * half - 1), pl.ds(0, ds_ref.shape[1] // 2)]
            else:
                there = slots[which].at[pl.ds(0, half - (way != which))]
            remote(there, there, zsend.at[way, which], zrecv.at[way, 0, which, 0], device_id=ring[way]).wait_send()
            remote(there, there, hsend.at[way, which], hrecv.at[way, 0, which], device_id=side_dev[way]).wait_send()
        for kind in range(2):
            whole(kind, which).wait_send()


def moe(side, planes, x, route, gate, wg, wu, wd):
    tok_n, d_model = x.shape
    d_ff = wg.shape[2]
    half = planes // 2
    slots = (half - 1) * 4
    parts = tok_n // min(TILE, tok_n)
    bf = jnp.bfloat16
    f32 = jnp.float32
    any_spec = pl.BlockSpec(memory_space=pl.ANY)
    dma = pltpu.SemaphoreType.DMA
    rows = CORES * tok_n
    top_k = route.shape[0]
    out = pl.pallas_call(
        functools.partial(kernel, side, planes),
        out_shape=(
            jax.ShapeDtypeStruct((tok_n, d_model), bf),
            jax.ShapeDtypeStruct((slots, d_model, d_ff), bf),
            jax.ShapeDtypeStruct((slots, d_model, d_ff), bf),
            jax.ShapeDtypeStruct((slots, d_ff, d_model), bf),
        ),
        in_specs=[pl.BlockSpec(memory_space=pltpu.HBM)] * 6,
        out_specs=(pl.BlockSpec(memory_space=pltpu.VMEM),) + (any_spec,) * 3,
        scratch_shapes=[
            pltpu.VMEM((rows, d_model), bf),
            pltpu.VMEM((CORES, top_k, tok_n), jnp.int32),
            pltpu.VMEM((CORES, top_k, tok_n), f32),
            pltpu.VMEM((LANES, tok_n), f32),
            pltpu.VMEM((rows, LANES), f32),
            pltpu.VMEM((rows, d_model), f32),
            pltpu.VMEM((tok_n, d_model), f32),
            pltpu.VMEM((4, rows, d_ff), bf),
            pltpu.VMEM((2, d_model, d_ff), bf),
            pltpu.VMEM((2, d_model, d_ff), bf),
            pltpu.VMEM((4, d_ff, d_model), bf),
            pltpu.VMEM((4, d_model, d_ff), bf),
            pltpu.VMEM((4, d_model, d_ff), bf),
            pltpu.VMEM((4, d_ff, d_model), bf),
            dma((2, 3)),
            dma((2, half, 3, CHUNKS)),
            dma((2, 3)),
            dma((2, half - 1, 3)),
            dma((2, 3)),
            dma((2, 3)),
            dma((2, 3, CHUNKS)),
            dma((2, SUBS)),
            dma((2, SUBS)),
            dma((2, SUBS)),
            dma((2, 2)),
            dma((4,)),
            dma((3,)),
            dma((3,)),
            dma((3,)),
            dma((parts,)),
            dma((parts,)),
        ],
        compiler_params=pltpu.CompilerParams(
            collective_id=0, has_side_effects=True, vmem_limit_bytes=50 * 1024 * 1024),
        name="stream_experts",
    )(x, route, gate, wg, wu, wd)
    return out[0]


def solution(mesh):
    planes = mesh.shape["ep"] // CORES
    side = math.isqrt(mesh.shape["dp"])
    row_spec = P(("dp", "ep"))
    expert_spec = P("ep")

    def local_step(tok_loc, route_loc, gate_loc, wg_loc, wu_loc, wd_loc):
        return moe(side, planes, tok_loc, route_loc.T, gate_loc.T, wg_loc, wu_loc, wd_loc)

    return jax.shard_map(local_step, mesh=mesh, in_specs=(row_spec, row_spec, row_spec, expert_spec, expert_spec, expert_spec), out_specs=row_spec, check_vma=False)
```

```python
import functools
import math

import jax
import jax.numpy as jnp
from jax import lax
from jax.experimental import pallas as pl
from jax.experimental.pallas import tpu as pltpu
from jax.sharding import PartitionSpec as P

CORES = 2
CHUNKS = 4
TILE = 512
SUBS = 4
LANES = 128


def kernel(side, planes, x_ref, route_ref, gate_ref, wg_ref, wu_ref, wd_ref,
           y_ref, gs_ref, us_ref, ds_ref,
           x_all, route_all, gate_all, gate_rows, gate_cols, y_acc, y_peer, hidden,
           g_buf, u_buf, d_buf, g_far, u_far, d_far,
           zsend, zrecv, hsend, hrecv, psend, precv, far_recv, first_recv, last_recv, cross_recv,
           gu_sem, d_sem, tok_sem, tok_send, tok_recv, part_send, part_recv):
    half = planes // 2
    tok_n = x_ref.shape[0]
    tile = min(TILE, tok_n)
    tiles_half = tok_n // tile
    tiles = CORES * tiles_half
    experts = planes * CORES * 2
    col = lax.axis_index("dp")
    pos = lax.axis_index("ep")
    core = pos % CORES
    plane = pos // CORES
    cx, cy = col // side, col % side
    parity = (cx + cy) % 2
    col_x = col + side * (1 - 2 * (cx % 2))
    col_y = col + 1 - 2 * (cy % 2)
    up = (pos + CORES) % (planes * CORES)
    down = (pos + (planes - 1) * CORES) % (planes * CORES)
    peer = {"ep": pos + 1 - 2 * core}
    ring = ({"ep": up}, {"ep": down})
    side_dev = ({"dp": col_x}, {"dp": col_y})
    own = (wg_ref, wu_ref, wd_ref)
    slots = (gs_ref, us_ref, ds_ref)
    far = (g_far, u_far, d_far)
    rows = tuple(w.shape[1] // CHUNKS for w in own)
    mid = CHUNKS // 2
    mine = core * tok_n
    theirs = (1 - core) * tok_n
    remote = pltpu.make_async_remote_copy

    barrier = pltpu.get_barrier_semaphore()
    for dev in (*ring, *side_dev, peer):
        pl.semaphore_signal(barrier, inc=1, device_id=dev)
    with jax.named_scope("entry"):
        pl.semaphore_wait(barrier, 5)

    def piece(which, ref, idx, i):
        return ref.at[idx, pl.ds(i * rows[which], rows[which])]

    def first_hop(way, which, i):
        return remote(piece(which, own[which], parity, i), piece(which, slots[which], way, i),
                      zsend.at[way, which], zrecv.at[way, 0, which, i], device_id=ring[way])

    def next_hop(way, h, which, i):
        return remote(piece(which, slots[which], (h - 1) * 4 + way, i), piece(which, slots[which], h * 4 + way, i),
                      zsend.at[way, which], zrecv.at[way, h, which, i], device_id=ring[way])

    def last_hop(way, which, i):
        return remote(piece(which, slots[which], (half - 2) * 4 + way, i), piece(which, far[which], 0, i),
                      zsend.at[way, which], zrecv.at[way, half - 1, which, i], device_id=ring[way])

    def side_hop(way, h, which, i):
        return remote(piece(which, slots[which], (h - 1) * 4 + way, i), piece(which, slots[which], (h - 1) * 4 + 2 + way, i),
                      hsend.at[way, which], hrecv.at[way, h - 1, which], device_id=side_dev[way])

    def far_side(way, which, i):
        return remote(piece(which, far[which], 0, i), piece(which, far[which], 2, i),
                      hsend.at[way, which], far_recv.at[way, which, i], device_id=side_dev[way])

    def to_peer(kind, which, i):
        return remote(piece(which, far[which], 2 * kind, i), piece(which, far[which], 2 * kind + 1, i),
                      psend.at[kind, which], precv.at[kind, which], device_id=peer)

    def cut(ref, idx, which, i, n):
        size = rows[which] // SUBS
        return ref.at[idx, pl.ds(i * rows[which] + n * size, size)]

    def first_cut(way, n):
        return remote(cut(wg_ref, parity, 0, 0, n), cut(gs_ref, way, 0, 0, n),
                      zsend.at[way, 0], first_recv.at[way, n], device_id=ring[way])

    def side_cut(way, n):
        return remote(cut(gs_ref, way, 0, 0, n), cut(gs_ref, 2 + way, 0, 0, n),
                      hsend.at[way, 0], hrecv.at[way, 0, 0], device_id=side_dev[way])

    def last_piece(way):
        return way * mid + mid - 1

    def last_cut(way, n):
        return remote(cut(ds_ref, (half - 2) * 4 + way, 2, last_piece(way), n), cut(d_far, 0, 2, last_piece(way), n),
                      zsend.at[way, 2], last_recv.at[way, n], device_id=ring[way])

    def last_side_cut(way, n):
        return remote(cut(d_far, 0, 2, last_piece(way), n), cut(d_far, 2, 2, last_piece(way), n),
                      hsend.at[way, 2], cross_recv.at[way, n], device_id=side_dev[way])

    def peer_cut(kind, way, n):
        return remote(cut(d_far, 2 * kind, 2, last_piece(way), n), cut(d_far, 2 * kind + 1, 2, last_piece(way), n),
                      psend.at[kind, 2], precv.at[kind, 2], device_id=peer)

    def wait_ring(way, h, which, i):
        there = piece(which, slots[which], (h - 1) * 4 + way, i)
        remote(there, there, zsend.at[way, which], zrecv.at[way, h - 1, which, i], device_id=ring[way]).wait_recv()

    def wait_side(h, which):
        for way in range(2):
            there = slots[which].at[(h - 1) * 4 + 2 + way]
            with jax.named_scope(f"wait_s{which}"):
                remote(there, there, hsend.at[way, which], hrecv.at[way, h - 1, which], device_id=side_dev[way]).wait_recv()

    for n in range(SUBS):
        for way in range(2):
            first_cut(way, n).start()
    for which in range(3):
        def start(i, c, which=which):
            for way in range(2):
                first_hop(way, which, i).start()
            return c

        lax.fori_loop(1 if which == 0 else 0, CHUNKS, start, 0)

    def load_gu(refs, idx, b):
        for m, buf in enumerate((g_buf, u_buf)):
            pltpu.make_async_copy(refs[m].at[idx], buf.at[b], gu_sem.at[b, m]).start()

    def wait_gu(b):
        for m, buf in enumerate((g_buf, u_buf)):
            pltpu.make_async_copy(own[m].at[0], buf.at[b], gu_sem.at[b, m]).wait()

    def load_d(ref, idx, b):
        pltpu.make_async_copy(ref.at[idx], d_buf.at[b], d_sem.at[b]).start()

    def wait_d(b):
        pltpu.make_async_copy(wd_ref.at[0], d_buf.at[b], d_sem.at[b]).wait()

    load_gu(own, 0, 0)
    load_gu(own, 1, 1)
    my_rows = pl.ds(mine, tok_n)
    tok = ((x_ref, x_all.at[my_rows]), (route_ref, route_all.at[core]), (gate_ref, gate_all.at[core]))
    for k, (src, dst) in enumerate(tok):
        remote(src, dst, tok_send.at[k], tok_recv.at[k], device_id=peer).start()
        pltpu.make_async_copy(src, dst, tok_sem.at[k]).start()
    y_acc[...] = jnp.zeros_like(y_acc)
    gate_rows[...] = jnp.zeros_like(gate_rows)
    def first_forward(n):
        for way in range(2):
            with jax.named_scope("wait_first"):
                first_cut(way, n).wait_recv()
            side_cut(way, n).start()

    first_forward(0)
    for k, (src, dst) in reversed(list(enumerate(tok))):
        pltpu.make_async_copy(src, dst, tok_sem.at[k]).wait()
        remote(src, dst, tok_send.at[k], tok_recv.at[k], device_id=peer).wait()

    def dense(c, carry):
        route, gate = route_all[c], gate_all[c]
        for e in range(experts):
            gate_rows[e:e + 1, :] = jnp.sum(jnp.where(route == e, gate, 0.0), axis=0, keepdims=True)
        for b in range(tok_n // LANES):
            gate_cols[pl.ds(c * tok_n + b * LANES, LANES), :] = gate_rows[:, b * LANES:(b + 1) * LANES].T
        return carry

    for n in range(1, SUBS):
        first_forward(n)
        if n <= CORES:
            dense(n - 1, 0)

    def expert_id(h, q, ring_core):
        src = (plane + planes + (2 * (q % 2) - 1) * h) % planes
        sub = parity + (q // 2) * (1 - 2 * parity)
        return (src * CORES + ring_core) * 2 + sub

    def front(row0, g, u, q, out0):
        x_tile = x_all[pl.ds(row0, tile)]
        a = jnp.dot(x_tile, g, preferred_element_type=jnp.float32)
        b = jnp.dot(x_tile, u, preferred_element_type=jnp.float32)
        hidden[q, pl.ds(out0, tile)] = (jax.nn.silu(a) * b).astype(jnp.bfloat16)

    def back(q, h0, d, row0, expert):
        out = jnp.dot(hidden[q, pl.ds(h0, tile)], d, preferred_element_type=jnp.float32).astype(jnp.bfloat16)
        gates = gate_cols[pl.ds(row0, tile)]
        lane = lax.broadcasted_iota(jnp.int32, gates.shape, 1)
        gate = jnp.sum(jnp.where(lane == expert, gates, 0.0), axis=1, keepdims=True)
        return jnp.where(gate > 0.0, gate * out.astype(jnp.float32), 0.0)

    def front_tile(t, q0):
        e, r = t // tiles, t % tiles

        @pl.when(r == 0)
        def _():
            wait_gu(e)

        front(r * tile, g_buf[e], u_buf[e], q0 + e, r * tile)

    def back_tile(t, stage):
        q, r = t // tiles, t % tiles

        @pl.when(r == 0)
        def _():
            wait_d(q)

        expert = jnp.where(stage == 0, (plane * CORES + core) * 2 + q, expert_id(stage, q, core))
        y_acc[pl.ds(r * tile, tile)] += back(q, r * tile, d_buf[q], r * tile, expert)

    def run(tile_fn, first, count, arg):
        def one(k, c):
            tile_fn(first + k, arg)
            return c

        with jax.named_scope(tile_fn.__name__):
            lax.fori_loop(0, count, one, 0)

    def ups(h, first):
        if first:
            for which in range(2):
                wait_side(h, which)
        for e in range(2):
            load_gu(slots, (h - 1) * 4 + first + e, e)

    def downs(h, first):
        if first:
            wait_side(h, 2)
        for q in range(2):
            load_d(ds_ref, (h - 1) * 4 + first + q, first + q)

    per_front = 4 * tiles // CHUNKS
    per_back = 4 * tiles // CHUNKS
    halves = ([(0, i) for i in range(CHUNKS)] + [(2, i) for i in range(mid)],
              [(1, i) for i in range(CHUNKS)] + [(2, mid + i) for i in range(mid)])

    def stage(h, carry):
        for which in range(3):
            if which == 0:
                @pl.when(h > 1)
                def _():
                    downs(h - 1, 0)
            elif which == 1:
                @pl.when(h == 1)
                def _():
                    load_d(wd_ref, 0, 0)
                    load_d(wd_ref, 1, 1)
            else:
                ups(h, 0)

            def one(i, c, which=which):
                for way in range(2):
                    def take():
                        with jax.named_scope(f"wait_z{which}"):
                            wait_ring(way, h, which, i)
                        side_hop(way, h, which, i).start()

                    if which == 0:
                        pl.when((h > 1) | (i > 0))(take)
                    else:
                        take()
                    far_ids = [k for w, k in halves[way] if w == which]

                    @pl.when(h < half - 1)
                    def _():
                        next_hop(way, h, which, i).start()

                    if far_ids:
                        whole = far_ids[-1] - (which == 2)

                        @pl.when((h == half - 1) & (i >= far_ids[0]) & (i <= whole))
                        def _():
                            last_hop(way, which, i).start()

                    if which == 2:
                        @pl.when((h == half - 1) & (i == last_piece(way)))
                        def _():
                            for n in range(SUBS):
                                last_cut(way, n).start()
                if which == 0:
                    @pl.when(h == 1)
                    def _():
                        run(front_tile, i * (per_front // 2), per_front // 2, 0)

                    @pl.when(h > 1)
                    def _():
                        run(back_tile, i * per_back, per_back, h - 1)

                        @pl.when(i == 0)
                        def _():
                            downs(h - 1, 2)
                elif which == 1:
                    @pl.when(h == 1)
                    def _():
                        run(back_tile, i * (per_back // 2), per_back // 2, 0)
                else:
                    @pl.when(i < mid)
                    def _():
                        run(front_tile, i * per_front, per_front, 0)

                    @pl.when(i == mid - 1)
                    def _():
                        ups(h, 2)

                    @pl.when(i >= mid)
                    def _():
                        run(front_tile, (i - mid) * per_front, per_front, 2)
                return c

            lax.fori_loop(0, CHUNKS, one, 0)
        return carry

    lax.fori_loop(1, half, stage, 0)

    def far_ring(way, which, i):
        with jax.named_scope("wait_zfar"):
            last_hop(way, which, i).wait_recv()
        far_side(way, which, i).start()
        to_peer(0, which, i).start()

    def far_cross(way, which, i):
        with jax.named_scope("wait_sfar"):
            far_side(way, which, i).wait_recv()
        to_peer(1, which, i).start()

    def whole(kind, which):
        there = far[which].at[2 * kind + 1]
        return remote(there, there, psend.at[kind, which], precv.at[kind, which], device_id=peer)

    def far_front(f, t):
        front(mine + t * tile, g_far[f], u_far[f], f, t * tile)

    def part_copy(t):
        src = y_acc.at[pl.ds(theirs + t * tile, tile)]
        return remote(src, y_peer.at[pl.ds(t * tile, tile)], part_send.at[t], part_recv.at[t], device_id=peer)

    downs(half - 1, 0)
    third = (4 * tiles - per_back) // 2

    def far_a(i, c):
        for way in range(2):
            far_ring(way, way, i)

        @pl.when(i == 2)
        def _():
            for way in range(2):
                far_cross(way, way, 0)
        run(back_tile, jnp.where(i == 0, 0, per_back + (i - 1) * third), jnp.where(i == 0, per_back, third), half - 1)

        @pl.when(i == 0)
        def _():
            downs(half - 1, 2)
        return c

    lax.fori_loop(0, CHUNKS - 1, far_a, 0)
    for way in range(2):
        far_ring(way, way, CHUNKS - 1)
        far_cross(way, way, 1)
    for t in range(tiles_half):
        part_copy(t).start()

    def fronts(f, inside):
        def one(t, c):
            inside(t)
            far_front(f, t)
            return c

        lax.fori_loop(0, tiles_half, one, 0)

    def nothing(t):
        pass

    fronts(0, nothing)
    for way in range(2):
        far_ring(way, 2, way * mid)
        far_cross(way, way, 2)
    for which in range(2):
        whole(0, which).wait_recv()
    fronts(1, nothing)
    for way in range(2):
        far_cross(way, way, 3)

    def forward_01(t):
        for n in range(2):
            @pl.when(t == n * tiles_half // 2)
            def _():
                last_forward(n)

    def forward_23(t):
        for n in range(2):
            @pl.when(t == n * tiles_half // 2)
            def _():
                last_forward(2 + n)

    def last_forward(n):
        for way in range(2):
            last_cut(way, n).wait_recv()
            last_side_cut(way, n).start()
            peer_cut(0, way, n).start()

    fronts(2, forward_01)
    for which in range(2):
        whole(1, which).wait_recv()
    fronts(3, forward_23)

    def far_back(f, expert):
        def one(t, c):
            y_acc[pl.ds(mine + t * tile, tile)] += back(f, t * tile, d_far[f], mine + t * tile, expert)
            return c

        with jax.named_scope("far_back"):
            lax.fori_loop(0, tiles_half, one, 0)

    for way in range(2):
        far_cross(way, 2, way * mid)
    far_back(0, expert_id(half, 0, core))
    whole(0, 2).wait_recv()

    def last_cross(n):
        for way in range(2):
            with jax.named_scope("wait_scut"):
                last_side_cut(way, n).wait_recv()
            peer_cut(1, way, n).start()

    for n in range(SUBS - 1):
        last_cross(n)
    far_back(1, expert_id(half, 0, 1 - core))
    last_cross(SUBS - 1)
    far_back(2, expert_id(half, 2, core))
    with jax.named_scope("wait_part"):
        for t in range(tiles_half):
            part_copy(t).wait()
    with jax.named_scope("wait_peer_last"):
        whole(1, 2).wait_recv()

    def finish(t, c):
        part = pl.ds(t * tile, tile)
        row0 = mine + t * tile
        total = y_acc[pl.ds(row0, tile)] + y_peer[part] + back(3, t * tile, d_far[3], row0, expert_id(half, 2, 1 - core))
        y_ref[part] = total.astype(y_ref.dtype)
        return c

    with jax.named_scope("finish"):
        lax.fori_loop(0, tiles_half, finish, 0)

    with jax.named_scope("drain"):
      for which in range(3):
        for way in range(2):
            if which == 2:
                there = ds_ref.at[pl.ds(0, 2 * half - 1), pl.ds(0, ds_ref.shape[1] // 2)]
            else:
                there = slots[which].at[pl.ds(0, half - (way != which))]
            remote(there, there, zsend.at[way, which], zrecv.at[way, 0, which, 0], device_id=ring[way]).wait_send()
            remote(there, there, hsend.at[way, which], hrecv.at[way, 0, which], device_id=side_dev[way]).wait_send()
        for kind in range(2):
            whole(kind, which).wait_send()


def moe(side, planes, x, route, gate, wg, wu, wd):
    tok_n, d_model = x.shape
    d_ff = wg.shape[2]
    half = planes // 2
    slots = (half - 1) * 4
    parts = tok_n // min(TILE, tok_n)
    bf = jnp.bfloat16
    f32 = jnp.float32
    any_spec = pl.BlockSpec(memory_space=pl.ANY)
    dma = pltpu.SemaphoreType.DMA
    rows = CORES * tok_n
    top_k = route.shape[0]
    out = pl.pallas_call(
        functools.partial(kernel, side, planes),
        out_shape=(
            jax.ShapeDtypeStruct((tok_n, d_model), bf),
            jax.ShapeDtypeStruct((slots, d_model, d_ff), bf),
            jax.ShapeDtypeStruct((slots, d_model, d_ff), bf),
            jax.ShapeDtypeStruct((slots, d_ff, d_model), bf),
        ),
        in_specs=[pl.BlockSpec(memory_space=pltpu.HBM)] * 6,
        out_specs=(pl.BlockSpec(memory_space=pltpu.VMEM),) + (any_spec,) * 3,
        scratch_shapes=[
            pltpu.VMEM((rows, d_model), bf),
            pltpu.VMEM((CORES, top_k, tok_n), jnp.int32),
            pltpu.VMEM((CORES, top_k, tok_n), f32),
            pltpu.VMEM((LANES, tok_n), f32),
            pltpu.VMEM((rows, LANES), f32),
            pltpu.VMEM((rows, d_model), f32),
            pltpu.VMEM((tok_n, d_model), f32),
            pltpu.VMEM((4, rows, d_ff), bf),
            pltpu.VMEM((2, d_model, d_ff), bf),
            pltpu.VMEM((2, d_model, d_ff), bf),
            pltpu.VMEM((4, d_ff, d_model), bf),
            pltpu.VMEM((4, d_model, d_ff), bf),
            pltpu.VMEM((4, d_model, d_ff), bf),
            pltpu.VMEM((4, d_ff, d_model), bf),
            dma((2, 3)),
            dma((2, half, 3, CHUNKS)),
            dma((2, 3)),
            dma((2, half - 1, 3)),
            dma((2, 3)),
            dma((2, 3)),
            dma((2, 3, CHUNKS)),
            dma((2, SUBS)),
            dma((2, SUBS)),
            dma((2, SUBS)),
            dma((2, 2)),
            dma((4,)),
            dma((3,)),
            dma((3,)),
            dma((3,)),
            dma((parts,)),
            dma((parts,)),
        ],
        compiler_params=pltpu.CompilerParams(
            collective_id=0, has_side_effects=True, vmem_limit_bytes=50 * 1024 * 1024),
        name="stream_experts",
    )(x, route, gate, wg, wu, wd)
    return out[0]


def solution(mesh):
    planes = mesh.shape["ep"] // CORES
    side = math.isqrt(mesh.shape["dp"])
    row_spec = P(("dp", "ep"))
    expert_spec = P("ep")

    def local_step(tok_loc, route_loc, gate_loc, wg_loc, wu_loc, wd_loc):
        return moe(side, planes, tok_loc, route_loc.T, gate_loc.T, wg_loc, wu_loc, wd_loc)

    return jax.shard_map(local_step, mesh=mesh, in_specs=(row_spec, row_spec, row_spec, expert_spec, expert_spec, expert_spec), out_specs=row_spec, check_vma=False)
```

```python
import functools
import math

import jax
import jax.numpy as jnp
from jax import lax
from jax.experimental import pallas as pl
from jax.experimental.pallas import tpu as pltpu
from jax.sharding import PartitionSpec as P

CORES = 2
CHUNKS = 4
TILE = 512
BACK = 8
LANES = 128


def kernel(side, planes, x_ref, route_ref, gate_ref, wg_ref, wu_ref, wd_ref,
           y_ref, gu_ref, ds_ref, tr_ref,
           x_all, route_all, gate_all, gate_rows, gate_cols, y_acc, y_peer, b_peer, y_ret, hidden,
           gu_buf, d_buf, gu_far, d_far,
           zsend, zrecv, tsend, trecv, frecv, f3recv, farrecv, gu_sem, d_sem, own_sem, own_send, own_recv,
           near_send, near_recv, fwd_send, fwd_recv, bsend, brecv, rsend, rrecv, psend, precv):
    last = planes // 2 - 1
    tok_n, d_model = x_ref.shape
    part_n = tok_n // 2
    tile = min(TILE, tok_n // 2)
    per_block = tok_n // tile
    experts = planes * CORES * 2
    col = lax.axis_index("dp")
    pos = lax.axis_index("ep")
    core = pos % CORES
    plane = pos // CORES
    cx, cy = col // side, col % side
    parity = (cx + cy) % 2
    cls = cx % 2
    alt = 1 - cls
    col_x = col + side * (1 - 2 * (cx % 2))
    col_y = col + 1 - 2 * (cy % 2)
    up = (pos + CORES) % (planes * CORES)
    down = (pos + (planes - 1) * CORES) % (planes * CORES)
    peer = {"ep": pos + 1 - 2 * core}
    ring = ({"ep": up}, {"ep": down})
    side_dev = ({"dp": col_x}, {"dp": col_y})
    gu_rows = wg_ref.shape[1] // CHUNKS
    d_rows = wd_ref.shape[1] // CHUNKS
    mid = CHUNKS // 2
    remote = pltpu.make_async_remote_copy

    with jax.named_scope("entry"):
        barrier = pltpu.get_barrier_semaphore()
        for dev in (*ring, *side_dev, peer):
            pl.semaphore_signal(barrier, inc=1, device_id=dev)
        pl.semaphore_wait(barrier, 5)

    def gu_cut(i):
        return pl.ds(i * gu_rows, gu_rows)

    def d_cut(i):
        return pl.ds(i * d_rows, d_rows)

    def first_gu(way, i):
        for m, w in enumerate((wg_ref, wu_ref)):
            @pl.when(cls == m)
            def _(m=m, w=w):
                remote(w.at[parity, gu_cut(i)], gu_ref.at[way, m, gu_cut(i)],
                       zsend.at[way, 0], zrecv.at[way, 0, 0, i], device_id=ring[way]).start()

    def first_d(way, i):
        remote(wd_ref.at[parity, d_cut(i)], ds_ref.at[way, d_cut(i)],
               zsend.at[way, 1], zrecv.at[way, 0, 1, i], device_id=ring[way]).start()

    def next_gu(way, h, i):
        return remote(gu_ref.at[(h - 1) * 2 + way, cls, gu_cut(i)], gu_ref.at[h * 2 + way, cls, gu_cut(i)],
                      zsend.at[way, 0], zrecv.at[way, h, 0, i], device_id=ring[way])

    def next_d(way, h, i):
        return remote(ds_ref.at[(h - 1) * 2 + way, d_cut(i)], ds_ref.at[h * 2 + way, d_cut(i)],
                      zsend.at[way, 1], zrecv.at[way, h, 1, i], device_id=ring[way])

    def wait_ring(way, h, kind, i):
        there = ds_ref.at[(h - 1) * 2 + way, d_cut(i)] if kind else gu_ref.at[(h - 1) * 2 + way, cls, gu_cut(i)]
        remote(there, there, zsend.at[way, kind], zrecv.at[way, h - 1, kind, i], device_id=ring[way]).wait_recv()

    def far_gu(way, i):
        m = cls if way == 0 else alt
        return remote(gu_ref.at[(last - 1) * 2 + way, m, gu_cut(i)], gu_far.at[m, gu_cut(i)],
                      zsend.at[way, 0], farrecv.at[way, 0], device_id=ring[way])

    def far_d(way, i):
        return remote(ds_ref.at[(last - 1) * 2 + way, d_cut(i)], d_far.at[d_cut(i)],
                      zsend.at[way, 1], farrecv.at[way, 1], device_id=ring[way])

    def transit_out(way, h, i):
        slot = (h - 1) * 2 + way
        return remote(gu_ref.at[slot, cls, gu_cut(i)], tr_ref.at[slot, gu_cut(i)],
                      tsend.at[way, 0], trecv.at[way, h - 1, i], device_id=side_dev[way])

    def transit_on(way, h, i, sem):
        slot = (h - 1) * 2 + way
        m = alt if way == 0 else cls
        return remote(tr_ref.at[slot, gu_cut(i)], gu_ref.at[slot, m, gu_cut(i)],
                      tsend.at[way, 1], sem, device_id=side_dev[1 - way])

    def wait_final(way, h):
        there = gu_ref.at[(h - 1) * 2 + way, alt]
        remote(there, there, tsend.at[way, 1], frecv.at[way, h - 1], device_id=side_dev[1 - way]).wait_recv()

    for i in range(CHUNKS):
        for way in range(2):
            first_gu(way, i)
    for i in range(CHUNKS):
        for way in range(2):
            first_d(way, i)

    near_block = CORES + core

    def near(way):
        part = pl.ds(way * part_n, part_n)
        return [remote(src, dst, near_send.at[way, k], near_recv.at[way, k], device_id=side_dev[way]) for k, (src, dst) in enumerate((
            (route_ref.at[:, part], route_all.at[near_block, :, part]),
            (gate_ref.at[:, part], gate_all.at[near_block, :, part]),
            (x_ref.at[part], x_all.at[pl.ds(near_block * tok_n + way * part_n, part_n)])))]

    for way in range(2):
        for copy in near(way):
            copy.start()

    def load_own(e):
        for m, w in enumerate((wg_ref, wu_ref)):
            pltpu.make_async_copy(w.at[e], gu_buf.at[e, m], gu_sem.at[e]).start()
        pltpu.make_async_copy(wd_ref.at[e], d_buf.at[e], d_sem.at[e]).start()

    def load_slot(h, e):
        slot = (h - 1) * 2 + e
        pltpu.make_async_copy(gu_ref.at[slot], gu_buf.at[e], gu_sem.at[e]).start()
        pltpu.make_async_copy(ds_ref.at[slot], d_buf.at[e], d_sem.at[e]).start()

    def wait_gu(e):
        pltpu.make_async_copy(gu_ref.at[0], gu_buf.at[e], gu_sem.at[e]).wait()

    def wait_d(e):
        pltpu.make_async_copy(ds_ref.at[0], d_buf.at[e], d_sem.at[e]).wait()

    load_own(0)
    load_own(1)
    tok = ((route_ref, route_all.at[core]), (gate_ref, gate_all.at[core]), (x_ref, x_all.at[pl.ds(core * tok_n, tok_n)]))
    for k, (src, dst) in enumerate(tok):
        remote(src, dst, own_send.at[k], own_recv.at[k], device_id=peer).start()
        pltpu.make_async_copy(src, dst, own_sem.at[k]).start()
    y_acc[...] = jnp.zeros_like(y_acc)
    gate_rows[...] = jnp.zeros_like(gate_rows)
    for k, (src, dst) in enumerate(tok):
        pltpu.make_async_copy(src, dst, own_sem.at[k]).wait()
        remote(src, dst, own_send.at[k], own_recv.at[k], device_id=peer).wait()

    def dense(block):
        route, gate = route_all[block], gate_all[block]
        for e in range(experts):
            gate_rows[e:e + 1, :] = jnp.sum(jnp.where(route == e, gate, 0.0), axis=0, keepdims=True)
        for b in range(tok_n // LANES):
            gate_cols[pl.ds(block * tok_n + b * LANES, LANES), :] = gate_rows[:, b * LANES:(b + 1) * LANES].T

    def dense_pair(first):
        def one(c, carry):
            dense(first + c)
            return carry

        lax.fori_loop(0, CORES, one, 0)

    dense_pair(0)

    def forward():
        mine = pl.ds(near_block * tok_n, tok_n)
        return [remote(ref, ref, fwd_send.at[k], fwd_recv.at[k], device_id=peer) for k, ref in enumerate((
            route_all.at[near_block], gate_all.at[near_block], x_all.at[mine]))]

    def expert_id(h, way):
        src = (plane + planes + (2 * way - 1) * h) % planes
        return (src * CORES + core) * 2 + parity

    def front(row0, gu, q):
        x_tile = x_all[pl.ds(row0, tile)]
        a = jnp.dot(x_tile, gu[0], preferred_element_type=jnp.float32)
        b = jnp.dot(x_tile, gu[1], preferred_element_type=jnp.float32)
        hidden[q, pl.ds(row0, tile)] = (jax.nn.silu(a) * b).astype(jnp.bfloat16)

    def back(row0, d, q, expert):
        part = pl.ds(row0, tile)
        out = jnp.dot(hidden[q, part], d, preferred_element_type=jnp.float32).astype(jnp.bfloat16)
        gates = gate_cols[part]
        lane = lax.broadcasted_iota(jnp.int32, gates.shape, 1)
        gate = jnp.sum(jnp.where(lane == expert, gates, 0.0), axis=1, keepdims=True)
        y_acc[part] += jnp.where(gate > 0.0, gate * out.astype(jnp.float32), 0.0)

    def group(e, phase, block0, blocks, expert, fresh):
        first, count = block0 * per_block, blocks * per_block

        @pl.when(phase == 0)
        def _():
            @pl.when(fresh)
            def _():
                wait_gu(e)

            def one(t, c):
                front(t * tile, gu_buf.at[e], e)
                return c

            with jax.named_scope("front"):
                lax.fori_loop(first, first + count, one, 0)

        @pl.when(phase == 1)
        def _():
            @pl.when(fresh)
            def _():
                wait_d(e)

            def one(t, c):
                back(t * tile, d_buf[e], e, expert)
                return c

            with jax.named_scope("back"):
                lax.fori_loop(first, first + count, one, 0)

    def own_id(e):
        return (plane * CORES + core) * 2 + e

    def load_pair(h):
        for way in range(2):
            with jax.named_scope("wait_final"):
                wait_final(way, h)
            load_slot(h, way)

    def stage(h, carry):
        def gates_and_ups(i, c):
            for way in range(2):
                with jax.named_scope("wait_z0"):
                    wait_ring(way, h, 0, i)

                @pl.when(h < last)
                def _():
                    next_gu(way, h, i).start()

                if way == 0:
                    @pl.when(h == last)
                    def _():
                        far_gu(0, i).start()
                transit_out(way, h, i).start()

            @pl.when((h == 2) & (i == 0))
            def _():
                with jax.named_scope("wait_fwd"):
                    for copy in forward():
                        copy.wait()
                dense_pair(CORES)

            @pl.when((h >= 3) | ((h == 1) & (i >= 2)))
            def _():
                mine = h == 1
                group(jnp.where(mine, 0, 1), jnp.where(mine, i - 2, i // 2), jnp.where(mine, 0, 2 * (i % 2)), 2,
                      jnp.where(mine, own_id(0), expert_id(h - 2, 1)), mine | (i % 2 == 0))

            @pl.when((h >= 2) & (i == CHUNKS - 1))
            def _():
                load_pair(h - 1)
            return c

        lax.fori_loop(0, CHUNKS, gates_and_ups, 0)

        def downs(i, c):
            for way in range(2):
                with jax.named_scope("wait_z1"):
                    wait_ring(way, h, 1, i)

                @pl.when(h < last)
                def _():
                    next_d(way, h, i).start()

                @pl.when((h == last) & ((i < mid) if way == 0 else (i >= mid)))
                def _():
                    far_d(way, i).start()
            for way in range(2):
                with jax.named_scope("wait_t"):
                    transit_out(way, h, i).wait_recv()
                if way == 0:
                    transit_on(0, h, i, frecv.at[0, h - 1]).start()
                else:
                    @pl.when(h < last)
                    def _():
                        transit_on(1, h, i, frecv.at[1, h - 1]).start()

                    @pl.when(h == last)
                    def _():
                        transit_on(1, h, i, f3recv.at[i]).start()

            @pl.when((h == 1) & (i == 1))
            def _():
                with jax.named_scope("wait_near"):
                    for way in range(2):
                        for copy in near(way):
                            copy.wait()
                for copy in forward():
                    copy.start()

            @pl.when((h >= 2) | (i < 2))
            def _():
                mine = h == 1
                group(jnp.where(mine, 1, 0), jnp.where(mine, i, i // 2), jnp.where(mine, 0, 2 * (i % 2)), 2,
                      jnp.where(mine, own_id(1), expert_id(h - 1, 0)), mine | (i % 2 == 0))
            return c

        lax.fori_loop(0, CHUNKS, downs, 0)
        return carry

    lax.fori_loop(1, last + 1, stage, 0)

    def rest(i, c):
        group(1, i // 2, 2 * (i % 2), 2, expert_id(last - 1, 1), i % 2 == 0)
        with jax.named_scope("wait_f3"):
            transit_on(1, last, i, f3recv.at[i]).wait_recv()
        far_gu(1, i).start()
        return c

    lax.fori_loop(0, CHUNKS, rest, 0)
    with jax.named_scope("wait_final"):
        wait_final(0, last)
    for e in range(2):
        load_slot(last, e)

    def near_groups(g, c):
        e, phase = g // 2, g % 2
        group(e, phase, CORES, CORES, expert_id(last, e), g >= 0)
        return c

    lax.fori_loop(0, 4, near_groups, 0)

    def far_tiles(fn, block):
        def one(t, c):
            fn((block * per_block + t) * tile)
            return c

        lax.fori_loop(0, per_block, one, 0)

    def far_front(row0):
        front(row0, gu_far, 0)

    far_expert = expert_id(last + 1, 0)

    def far_back(row0):
        back(row0, d_far[...], 0, far_expert)

    with jax.named_scope("wait_far0"):
        for way in range(2):
            m = cls if way == 0 else alt
            remote(gu_far.at[m], gu_far.at[m], zsend.at[way, 0], farrecv.at[way, 0], device_id=ring[way]).wait_recv()
    theirs, ours = CORES + 1 - core, CORES + core
    with jax.named_scope("far_front"):
        far_tiles(far_front, theirs)
        far_tiles(far_front, ours)
    with jax.named_scope("wait_far1"):
        for way in range(2):
            there = d_far.at[pl.ds(0, mid * d_rows)]
            remote(there, there, zsend.at[way, 1], farrecv.at[way, 1], device_id=ring[way]).wait_recv()

    size = part_n // BACK

    def to_peer(way, k):
        off = way * part_n + k * size
        return remote(y_acc.at[pl.ds(theirs * tok_n + off, size)], b_peer.at[pl.ds(off, size)],
                      bsend, brecv.at[way, k], device_id=peer)

    def give_back(way, k):
        off = way * part_n + k * size
        return remote(y_acc.at[pl.ds(ours * tok_n + off, size)], y_ret.at[pl.ds(off, size)],
                      rsend.at[way], rrecv.at[way, k], device_id=side_dev[way])

    with jax.named_scope("far_back"):
        far_tiles(far_back, theirs)
        far_back(ours * tok_n)
    for k in range(BACK):
        for way in range(2):
            to_peer(way, k).start()
    with jax.named_scope("far_back"):
        def more(t, c):
            far_back(ours * tok_n + t * tile)
            return c

        lax.fori_loop(1, per_block, more, 0)

    def sums(k, c):
        @pl.when(k < BACK)
        def _():
            for way in range(2):
                with jax.named_scope("wait_b"):
                    to_peer(way, k).wait_recv()
                off = way * part_n + k * size
                y_acc[pl.ds(ours * tok_n + off, size)] += b_peer[pl.ds(off, size)]

        @pl.when(k > 0)
        def _():
            for way in range(2):
                give_back(way, k - 1).start()
        return c

    lax.fori_loop(0, BACK + 1, sums, 0)

    def own_block(block):
        def one(g, c):
            group(g // 2, g % 2, block, 1, expert_id(last, g // 2), g < 0)
            return c

        lax.fori_loop(0, 4, one, 0)
        with jax.named_scope("far_own"):
            far_tiles(far_front, block)
            far_tiles(far_back, block)

    def part_copy():
        return remote(y_acc.at[pl.ds((1 - core) * tok_n, tok_n)], y_peer, psend, precv, device_id=peer)

    def own_blocks(n, c):
        own_block(core + (1 - n) * (1 - 2 * core))

        @pl.when(n == 0)
        def _():
            part_copy().start()
        return c

    lax.fori_loop(0, CORES, own_blocks, 0)
    with jax.named_scope("wait_part"):
        part_copy().wait()

    def finish(k, c):
        for way in range(2):
            with jax.named_scope("wait_r"):
                give_back(way, k).wait_recv()
            part = pl.ds(way * part_n + k * size, size)
            mine = pl.ds(core * tok_n + way * part_n + k * size, size)
            y_ref[part] = (y_acc[mine] + y_peer[part] + y_ret[part]).astype(y_ref.dtype)
        return c

    lax.fori_loop(0, BACK, finish, 0)

    with jax.named_scope("drain"):
        for way in range(2):
            whole = gu_ref.at[pl.ds(0, (last + 1) // 2)]
            remote(whole, whole, zsend.at[way, 0], farrecv.at[way, 0], device_id=ring[way]).wait_send()
            whole = gu_ref.at[pl.ds(0, 2), pl.ds(0, 2), pl.ds(0, (2 * last + 1) * gu_rows // 2)]
            remote(whole, whole, zsend.at[way, 1], farrecv.at[way, 1], device_id=ring[way]).wait_send()
            whole = tr_ref.at[pl.ds(0, last)]
            for hop in range(2):
                remote(whole, whole, tsend.at[way, hop], frecv.at[way, 0], device_id=side_dev[way]).wait_send()
            whole = y_ret.at[pl.ds(0, part_n)]
            remote(whole, whole, rsend.at[way], rrecv.at[way, 0], device_id=side_dev[way]).wait_send()
        remote(b_peer, b_peer, bsend, brecv.at[0, 0], device_id=peer).wait_send()


def moe(side, planes, x, route, gate, wg, wu, wd):
    tok_n, d_model = x.shape
    d_ff = wg.shape[2]
    last = planes // 2 - 1
    bf = jnp.bfloat16
    f32 = jnp.float32
    any_spec = pl.BlockSpec(memory_space=pl.ANY)
    dma = pltpu.SemaphoreType.DMA
    blocks = 2 * CORES
    rows = blocks * tok_n
    top_k = route.shape[0]
    out = pl.pallas_call(
        functools.partial(kernel, side, planes),
        out_shape=(
            jax.ShapeDtypeStruct((tok_n, d_model), bf),
            jax.ShapeDtypeStruct((2 * last, 2, d_model, d_ff), bf),
            jax.ShapeDtypeStruct((2 * last, d_ff, d_model), bf),
            jax.ShapeDtypeStruct((2 * last, d_model, d_ff), bf),
        ),
        in_specs=[any_spec] * 6,
        out_specs=(pl.BlockSpec(memory_space=pltpu.VMEM),) + (any_spec,) * 3,
        scratch_shapes=[
            pltpu.VMEM((rows, d_model), bf),
            pltpu.VMEM((blocks, top_k, tok_n), jnp.int32),
            pltpu.VMEM((blocks, top_k, tok_n), f32),
            pltpu.VMEM((LANES, tok_n), f32),
            pltpu.VMEM((rows, LANES), f32),
            pltpu.VMEM((rows, d_model), f32),
            pltpu.VMEM((tok_n, d_model), f32),
            pltpu.VMEM((tok_n, d_model), f32),
            pltpu.VMEM((tok_n, d_model), f32),
            pltpu.VMEM((2, rows, d_ff), bf),
            pltpu.VMEM((2, 2, d_model, d_ff), bf),
            pltpu.VMEM((2, d_ff, d_model), bf),
            pltpu.VMEM((2, d_model, d_ff), bf),
            pltpu.VMEM((d_ff, d_model), bf),
            dma((2, 2)),
            dma((2, last, 2, CHUNKS)),
            dma((2, 2)),
            dma((2, last, CHUNKS)),
            dma((2, last)),
            dma((CHUNKS,)),
            dma((2, 2)),
            dma((2,)),
            dma((2,)),
            dma((3,)),
            dma((3,)),
            dma((3,)),
            dma((2, 3)),
            dma((2, 3)),
            dma((3,)),
            dma((3,)),
            dma(()),
            dma((2, BACK)),
            dma((2,)),
            dma((2, BACK)),
            dma(()),
            dma(()),
        ],
        compiler_params=pltpu.CompilerParams(
            collective_id=0, has_side_effects=True, vmem_limit_bytes=62 * 1024 * 1024),
        name="stream_experts",
    )(x, route, gate, wg, wu, wd)
    return out[0]


def solution(mesh):
    planes = mesh.shape["ep"] // CORES
    side = math.isqrt(mesh.shape["dp"])
    row_spec = P(("dp", "ep"))
    expert_spec = P("ep")

    def local_step(tok_loc, route_loc, gate_loc, wg_loc, wu_loc, wd_loc):
        return moe(side, planes, tok_loc, route_loc.T, gate_loc.T, wg_loc, wu_loc, wd_loc)

    return jax.shard_map(local_step, mesh=mesh, in_specs=(row_spec, row_spec, row_spec, expert_spec, expert_spec, expert_spec), out_specs=row_spec, check_vma=False)
```

```python
import functools
import math

import jax
import jax.numpy as jnp
from jax import lax
from jax.experimental import pallas as pl
from jax.experimental.pallas import tpu as pltpu
from jax.sharding import PartitionSpec as P

CORES = 2
CHUNKS = 4
TILE = 512
BACK = 4
WAVES = 2
LANES = 128


def kernel(side, planes, x_ref, route_ref, gate_ref, wg_ref, wu_ref, wd_ref,
           y_ref, gu_ref, ds_ref, tr_ref,
           x_all, route_all, gate_all, gate_cols, y_acc, b_peer, y_ret, hidden,
           gu_buf, d_buf, gu_far, d_far,
           zsend, zrecv, tsend, trecv, frecv, f3recv, farrecv, gu_sem, d_sem, own_sem, own_send, own_recv,
           near_send, near_recv, fwd_send, fwd_recv, bsend, brecv, rsend, rrecv, psend, precv, free_sem):
    last = planes // 2 - 1
    tok_n, d_model = x_ref.shape
    part_n = tok_n // 2
    tile = min(TILE, tok_n // 2)
    per_block = tok_n // tile
    experts = planes * CORES * 2
    col = lax.axis_index("dp")
    pos = lax.axis_index("ep")
    core = pos % CORES
    plane = pos // CORES
    cx, cy = col // side, col % side
    parity = (cx + cy) % 2
    cls = cx % 2
    alt = 1 - cls
    col_x = col + side * (1 - 2 * (cx % 2))
    col_y = col + 1 - 2 * (cy % 2)
    up = (pos + CORES) % (planes * CORES)
    down = (pos + (planes - 1) * CORES) % (planes * CORES)
    peer = {"ep": pos + 1 - 2 * core}
    ring = ({"ep": up}, {"ep": down})
    side_dev = ({"dp": col_x}, {"dp": col_y})
    gu_rows = wg_ref.shape[1] // CHUNKS
    d_rows = wd_ref.shape[1] // CHUNKS
    mid = CHUNKS // 2
    remote = pltpu.make_async_remote_copy

    with jax.named_scope("entry"):
        barrier = pltpu.get_barrier_semaphore()
        for dev in (*ring, *side_dev, peer):
            pl.semaphore_signal(barrier, inc=1, device_id=dev)
        pl.semaphore_wait(barrier, 5)

    def gu_cut(i):
        return pl.ds(i * gu_rows, gu_rows)

    def d_cut(i):
        return pl.ds(i * d_rows, d_rows)

    def first_gu(way, i):
        for m, w in enumerate((wg_ref, wu_ref)):
            @pl.when(cls == m)
            def _(m=m, w=w):
                remote(w.at[parity, gu_cut(i)], gu_ref.at[way, m, gu_cut(i)],
                       zsend.at[way, 0], zrecv.at[way, 0, 0, i], device_id=ring[way]).start()

    def first_d(way, i):
        remote(wd_ref.at[parity, d_cut(i)], ds_ref.at[way, d_cut(i)],
               zsend.at[way, 1], zrecv.at[way, 0, 1, i], device_id=ring[way]).start()

    def next_gu(way, h, i):
        return remote(gu_ref.at[(h - 1) * 2 + way, cls, gu_cut(i)], gu_ref.at[h * 2 + way, cls, gu_cut(i)],
                      zsend.at[way, 0], zrecv.at[way, h, 0, i], device_id=ring[way])

    def next_d(way, h, i):
        return remote(ds_ref.at[(h - 1) * 2 + way, d_cut(i)], ds_ref.at[h * 2 + way, d_cut(i)],
                      zsend.at[way, 1], zrecv.at[way, h, 1, i], device_id=ring[way])

    def wait_ring(way, h, kind, i):
        there = ds_ref.at[(h - 1) * 2 + way, d_cut(i)] if kind else gu_ref.at[(h - 1) * 2 + way, cls, gu_cut(i)]
        remote(there, there, zsend.at[way, kind], zrecv.at[way, h - 1, kind, i], device_id=ring[way]).wait_recv()

    def far_gu(way, i):
        m = cls if way == 0 else alt
        return remote(gu_ref.at[(last - 1) * 2 + way, m, gu_cut(i)], gu_far.at[m, gu_cut(i)],
                      zsend.at[way, 0], farrecv.at[way, 0], device_id=ring[way])

    def far_d(way, i):
        return remote(ds_ref.at[(last - 1) * 2 + way, d_cut(i)], d_far.at[d_cut(i)],
                      zsend.at[way, 1], farrecv.at[way, 1], device_id=ring[way])

    def transit_out(way, h, i):
        slot = (h - 1) * 2 + way
        return remote(gu_ref.at[slot, cls, gu_cut(i)], tr_ref.at[slot, gu_cut(i)],
                      tsend.at[way, 0], trecv.at[way, h - 1, i], device_id=side_dev[way])

    def transit_on(way, h, i, sem):
        slot = (h - 1) * 2 + way
        m = alt if way == 0 else cls
        return remote(tr_ref.at[slot, gu_cut(i)], gu_ref.at[slot, m, gu_cut(i)],
                      tsend.at[way, 1], sem, device_id=side_dev[1 - way])

    def wait_final(way, h):
        there = gu_ref.at[(h - 1) * 2 + way, alt]
        remote(there, there, tsend.at[way, 1], frecv.at[way, h - 1], device_id=side_dev[1 - way]).wait_recv()

    for i in range(CHUNKS):
        for way in range(2):
            first_gu(way, i)
    for i in range(CHUNKS):
        for way in range(2):
            first_d(way, i)

    near_block = CORES + core

    wave_n = part_n // WAVES

    def near(way):
        copies = []
        for w in range(WAVES):
            src = pl.ds(way * part_n + w * wave_n, wave_n)
            off = w * part_n + way * wave_n
            dst = pl.ds(off, wave_n)
            copies += [
                remote(route_ref.at[:, src], route_all.at[near_block, :, dst], near_send.at[way, 0], near_recv.at[way, 0], device_id=side_dev[way]),
                remote(gate_ref.at[:, src], gate_all.at[near_block, :, dst], near_send.at[way, 1], near_recv.at[way, 1], device_id=side_dev[way]),
                remote(x_ref.at[src], x_all.at[pl.ds(near_block * tok_n + off, wave_n)], near_send.at[way, 2], near_recv.at[way, 2], device_id=side_dev[way])]
        return copies

    def wait_near(way):
        part = pl.ds(0, part_n)
        for k, ref in enumerate((route_all.at[near_block, :, part], gate_all.at[near_block, :, part], x_all.at[pl.ds(near_block * tok_n, part_n)])):
            remote(ref, ref, near_send.at[way, k], near_recv.at[way, k], device_id=side_dev[way]).wait()

    for way in range(2):
        for copy in near(way):
            copy.start()

    def load_own(e):
        for m, w in enumerate((wg_ref, wu_ref)):
            pltpu.make_async_copy(w.at[e], gu_buf.at[e, m], gu_sem.at[e]).start()
        pltpu.make_async_copy(wd_ref.at[e], d_buf.at[e], d_sem.at[e]).start()

    def load_slot(h, e):
        slot = (h - 1) * 2 + e
        pltpu.make_async_copy(gu_ref.at[slot], gu_buf.at[e], gu_sem.at[e]).start()
        pltpu.make_async_copy(ds_ref.at[slot], d_buf.at[e], d_sem.at[e]).start()

    def load_early(e):
        slot = (last - 1) * 2 + e
        pltpu.make_async_copy(gu_ref.at[slot, cls], gu_buf.at[e, cls], gu_sem.at[e]).start()
        pltpu.make_async_copy(ds_ref.at[slot], d_buf.at[e], d_sem.at[e]).start()

    def load_late(e):
        slot = (last - 1) * 2 + e
        pltpu.make_async_copy(gu_ref.at[slot, alt], gu_buf.at[e, alt], gu_sem.at[e]).start()

    def wait_gu(e):
        pltpu.make_async_copy(gu_ref.at[0], gu_buf.at[e], gu_sem.at[e]).wait()

    def wait_d(e):
        pltpu.make_async_copy(ds_ref.at[0], d_buf.at[e], d_sem.at[e]).wait()

    load_own(0)
    load_own(1)
    tok = ((route_ref, route_all.at[core]), (gate_ref, gate_all.at[core]), (x_ref, x_all.at[pl.ds(core * tok_n, tok_n)]))
    for k, (src, dst) in enumerate(tok):
        remote(src, dst, own_send.at[k], own_recv.at[k], device_id=peer).start()
        pltpu.make_async_copy(src, dst, own_sem.at[k]).start()
    y_acc[...] = jnp.zeros_like(y_acc)
    y_ret[pl.ds(0, LANES), :] = jnp.zeros((LANES, d_model), jnp.float32)
    for k, (src, dst) in enumerate(tok):
        pltpu.make_async_copy(src, dst, own_sem.at[k]).wait()
        remote(src, dst, own_send.at[k], own_recv.at[k], device_id=peer).wait()

    def dense(block):
        route, gate = route_all[block], gate_all[block]
        for e in range(experts):
            y_ret[e:e + 1, pl.ds(0, tok_n)] = jnp.sum(jnp.where(route == e, gate, 0.0), axis=0, keepdims=True)
        for b in range(tok_n // LANES):
            gate_cols[pl.ds(block * tok_n + b * LANES, LANES), :] = y_ret[pl.ds(0, LANES), b * LANES:(b + 1) * LANES].T

    def dense_pair(first):
        def one(c, carry):
            dense(first + c)
            return carry

        lax.fori_loop(0, CORES, one, 0)

    dense_pair(0)

    def forward():
        mine = pl.ds(near_block * tok_n, tok_n)
        return [remote(ref, ref, fwd_send.at[k], fwd_recv.at[k], device_id=peer) for k, ref in enumerate((
            route_all.at[near_block], gate_all.at[near_block], x_all.at[mine]))]

    def expert_id(h, way):
        src = (plane + planes + (2 * way - 1) * h) % planes
        return (src * CORES + core) * 2 + parity

    def front(row0, gu):
        x_tile = x_all[pl.ds(row0, tile)]
        a = jnp.dot(x_tile, gu[0], preferred_element_type=jnp.float32)
        b = jnp.dot(x_tile, gu[1], preferred_element_type=jnp.float32)
        hidden[pl.ds(row0, tile)] = (jax.nn.silu(a) * b).astype(jnp.bfloat16)

    def back(row0, d, expert):
        part = pl.ds(row0, tile)
        out = jnp.dot(hidden[part], d, preferred_element_type=jnp.float32).astype(jnp.bfloat16)
        gates = gate_cols[part]
        lane = lax.broadcasted_iota(jnp.int32, gates.shape, 1)
        gate = jnp.sum(jnp.where(lane == expert, gates, 0.0), axis=1, keepdims=True)
        y_acc[part] += jnp.where(gate > 0.0, gate * out.astype(jnp.float32), 0.0)

    def group(e, phase, block0, blocks, expert, fresh):
        first, count = block0 * per_block, blocks * per_block

        @pl.when(phase == 0)
        def _():
            @pl.when(fresh)
            def _():
                wait_gu(e)

            def one(t, c):
                front(t * tile, gu_buf.at[e])
                return c

            with jax.named_scope("front"):
                lax.fori_loop(first, first + count, one, 0)

        @pl.when(phase == 1)
        def _():
            @pl.when(fresh)
            def _():
                wait_d(e)

            def one(t, c):
                back(t * tile, d_buf[e], expert)
                return c

            with jax.named_scope("back"):
                lax.fori_loop(first, first + count, one, 0)

    def own_id(e):
        return (plane * CORES + core) * 2 + e

    def load_pair(h):
        for way in range(2):
            with jax.named_scope("wait_final"):
                wait_final(way, h)
            load_slot(h, way)

    def stage(h, carry):
        def gates_and_ups(i, c):
            for way in range(2):
                with jax.named_scope("wait_z0"):
                    wait_ring(way, h, 0, i)

                @pl.when(h < last)
                def _():
                    next_gu(way, h, i).start()

                if way == 0:
                    @pl.when(h == last)
                    def _():
                        far_gu(0, i).start()
                transit_out(way, h, i).start()

            @pl.when((h == 2) & (i == 0))
            def _():
                with jax.named_scope("wait_fwd"):
                    for copy in forward():
                        copy.wait()
                dense_pair(CORES)

            @pl.when((h >= 3) | ((h == 1) & (i >= 2)))
            def _():
                mine = h == 1
                group(jnp.where(mine, 0, 1), jnp.where(mine, i - 2, i // 2), jnp.where(mine, 0, 2 * (i % 2)), 2,
                      jnp.where(mine, own_id(0), expert_id(h - 2, 1)), mine | (i % 2 == 0))

            @pl.when((h >= 2) & (i == CHUNKS - 1))
            def _():
                load_pair(h - 1)
            return c

        lax.fori_loop(0, CHUNKS, gates_and_ups, 0)

        def downs(i, c):
            for way in range(2):
                with jax.named_scope("wait_z1"):
                    wait_ring(way, h, 1, i)

                @pl.when(h < last)
                def _():
                    next_d(way, h, i).start()

                @pl.when((h == last) & ((i < mid) if way == 0 else (i == mid)))
                def _():
                    far_d(way, i).start()
            for way in range(2):
                with jax.named_scope("wait_t"):
                    transit_out(way, h, i).wait_recv()
                if way == 0:
                    transit_on(0, h, i, frecv.at[0, h - 1]).start()
                else:
                    @pl.when(h < last)
                    def _():
                        transit_on(1, h, i, frecv.at[1, h - 1]).start()

                    @pl.when(h == last)
                    def _():
                        transit_on(1, h, i, f3recv.at[i]).start()

            @pl.when((h == 1) & (i == 1))
            def _():
                with jax.named_scope("wait_near"):
                    for way in range(2):
                        wait_near(way)
                for copy in forward():
                    copy.start()

            @pl.when((h >= 2) | (i < 2))
            def _():
                mine = h == 1
                group(jnp.where(mine, 1, 0), jnp.where(mine, i, i // 2), jnp.where(mine, 0, 2 * (i % 2)), 2,
                      jnp.where(mine, own_id(1), expert_id(h - 1, 0)), mine | (i % 2 == 0))
            return c

        lax.fori_loop(0, CHUNKS, downs, 0)
        return carry

    lax.fori_loop(1, last + 1, stage, 0)

    load_early(0)

    def rest(n, c):
        group(1, n // 4, n % 4, 1, expert_id(last - 1, 1), n % 4 == 0)

        @pl.when((n == 0) | (n == 2) | (n == 5) | (n == 7))
        def _():
            i = (n + 1) // 2 - n // 5
            with jax.named_scope("wait_f3"):
                transit_on(1, last, i, f3recv.at[i]).wait_recv()
            far_gu(1, i).start()
        return c

    lax.fori_loop(0, 2 * CHUNKS, rest, 0)
    for i in range(mid + 1, CHUNKS):
        far_d(1, i).start()
    load_late(1)
    load_early(1)
    with jax.named_scope("wait_final"):
        wait_final(0, last)
    load_late(0)

    theirs, ours = CORES + 1 - core, CORES + core
    far_expert = expert_id(last + 1, 0)

    def far_front(row0):
        front(row0, gu_far)

    def far_back(row0):
        back(row0, d_far[...], far_expert)

    def both(fn, w):
        def one(n, c):
            fn((theirs + n * (ours - theirs)) * tok_n + w * part_n)
            return c

        lax.fori_loop(0, CORES, one, 0)

    def near_group(g, c):
        w = g // 4
        e, phase = (g % 4) // 2, g % 2

        @pl.when(phase == 0)
        def _():
            @pl.when(w == 0)
            def _():
                wait_gu(e)
            with jax.named_scope("near_front"):
                both(lambda row0: front(row0, gu_buf.at[e]), w)

        @pl.when(phase == 1)
        def _():
            @pl.when(w == 0)
            def _():
                wait_d(e)
            with jax.named_scope("near_back"):
                both(lambda row0: back(row0, d_buf[e], expert_id(last, e)), w)
        return c

    size = wave_n // BACK

    def to_peer(way, w, k):
        off = w * part_n + way * wave_n + k * size
        return remote(y_acc.at[pl.ds(theirs * tok_n + off, size)], b_peer.at[pl.ds(off, size)],
                      bsend, brecv.at[way, w, k], device_id=peer)

    def give_back(way, w, k):
        src = ours * tok_n + w * part_n + way * wave_n + k * size
        return remote(y_acc.at[pl.ds(src, size)], y_ret.at[pl.ds(way * part_n + w * wave_n + k * size, size)],
                      rsend.at[way], rrecv.at[way, w, k], device_id=side_dev[way])

    def wave(w, c):
        first = w == 0
        lax.fori_loop(jnp.where(first, 0, 5), jnp.where(first, 5, 8), near_group, 0)

        @pl.when(first)
        def _():
            with jax.named_scope("wait_far0"):
                for way in range(2):
                    m = cls if way == 0 else alt
                    remote(gu_far.at[m], gu_far.at[m], zsend.at[way, 0], farrecv.at[way, 0], device_id=ring[way]).wait_recv()
        with jax.named_scope("far_front"):
            both(far_front, w)

        @pl.when(first)
        def _():
            with jax.named_scope("wait_far1"):
                for way in range(2):
                    there = d_far.at[pl.ds(0, mid * d_rows)]
                    remote(there, there, zsend.at[way, 1], farrecv.at[way, 1], device_id=ring[way]).wait_recv()
        with jax.named_scope("far_back"):
            both(far_back, w)
        for k in range(BACK):
            for way in range(2):
                to_peer(way, w, k).start()

        def sums(k, c2):
            @pl.when(k < BACK)
            def _():
                for way in range(2):
                    with jax.named_scope("wait_b"):
                        to_peer(way, w, k).wait_recv()
                    off = w * part_n + way * wave_n + k * size
                    y_acc[pl.ds(ours * tok_n + off, size)] += b_peer[pl.ds(off, size)]

            @pl.when(k > 0)
            def _():
                for way in range(2):
                    give_back(way, w, k - 1).start()
            return c2

        lax.fori_loop(0, BACK + 1, sums, 0)
        return c

    lax.fori_loop(0, WAVES, wave, 0)
    with jax.named_scope("wait_bsend"):
        remote(b_peer, b_peer, bsend, brecv.at[0, 0, 0], device_id=peer).wait_send()
    pl.semaphore_signal(free_sem, inc=1, device_id=peer)

    def own_block(block):
        def one(g, c):
            group(g // 2, g % 2, block, 1, expert_id(last, g // 2), g < 0)
            return c

        lax.fori_loop(0, 4, one, 0)
        with jax.named_scope("far_own"):
            for fn in (far_front, far_back):
                def one(t, c, fn=fn):
                    fn((block * per_block + t) * tile)
                    return c

                lax.fori_loop(0, per_block, one, 0)

    def part_copy():
        return remote(y_acc.at[pl.ds((1 - core) * tok_n, tok_n)], y_acc.at[pl.ds(ours * tok_n, tok_n)], psend, precv, device_id=peer)

    def own_blocks(n, c):
        own_block(core + (1 - n) * (1 - 2 * core))

        @pl.when(n == 0)
        def _():
            pl.semaphore_wait(free_sem, 1)
            part_copy().start()
        return c

    lax.fori_loop(0, CORES, own_blocks, 0)
    with jax.named_scope("wait_part"):
        part_copy().wait()

    def finish(k, c):
        for way in range(2):
            with jax.named_scope("wait_r"):
                give_back(way, k // BACK, k % BACK).wait_recv()
            part = pl.ds(way * part_n + k * size, size)
            mine = pl.ds(core * tok_n + way * part_n + k * size, size)
            other = pl.ds(theirs * tok_n + way * part_n + k * size, size)
            y_ref[part] = (y_acc[mine] + y_acc[other] + y_ret[part]).astype(y_ref.dtype)
        return c

    lax.fori_loop(0, WAVES * BACK, finish, 0)

    with jax.named_scope("drain"):
        for way in range(2):
            whole = gu_ref.at[pl.ds(0, (last + 1) // 2)]
            remote(whole, whole, zsend.at[way, 0], farrecv.at[way, 0], device_id=ring[way]).wait_send()
            whole = gu_ref.at[pl.ds(0, 2), pl.ds(0, 2), pl.ds(0, (2 * last + 1) * gu_rows // 2)]
            remote(whole, whole, zsend.at[way, 1], farrecv.at[way, 1], device_id=ring[way]).wait_send()
            whole = tr_ref.at[pl.ds(0, last)]
            for hop in range(2):
                remote(whole, whole, tsend.at[way, hop], frecv.at[way, 0], device_id=side_dev[way]).wait_send()
            whole = y_ret.at[pl.ds(0, part_n)]
            remote(whole, whole, rsend.at[way], rrecv.at[way, 0, 0], device_id=side_dev[way]).wait_send()


def moe(side, planes, x, route, gate, wg, wu, wd):
    tok_n, d_model = x.shape
    d_ff = wg.shape[2]
    last = planes // 2 - 1
    bf = jnp.bfloat16
    f32 = jnp.float32
    any_spec = pl.BlockSpec(memory_space=pl.ANY)
    dma = pltpu.SemaphoreType.DMA
    blocks = 2 * CORES
    rows = blocks * tok_n
    top_k = route.shape[0]
    out = pl.pallas_call(
        functools.partial(kernel, side, planes),
        out_shape=(
            jax.ShapeDtypeStruct((tok_n, d_model), bf),
            jax.ShapeDtypeStruct((2 * last, 2, d_model, d_ff), bf),
            jax.ShapeDtypeStruct((2 * last, d_ff, d_model), bf),
            jax.ShapeDtypeStruct((2 * last, d_model, d_ff), bf),
        ),
        in_specs=[any_spec] * 6,
        out_specs=(pl.BlockSpec(memory_space=pltpu.VMEM),) + (any_spec,) * 3,
        scratch_shapes=[
            pltpu.VMEM((rows, d_model), bf),
            pltpu.VMEM((blocks, top_k, tok_n), jnp.int32),
            pltpu.VMEM((blocks, top_k, tok_n), f32),
            pltpu.VMEM((rows, LANES), f32),
            pltpu.VMEM((rows, d_model), f32),
            pltpu.VMEM((tok_n, d_model), f32),
            pltpu.VMEM((tok_n, d_model), f32),
            pltpu.VMEM((rows, d_ff), bf),
            pltpu.VMEM((2, 2, d_model, d_ff), bf),
            pltpu.VMEM((2, d_ff, d_model), bf),
            pltpu.VMEM((2, d_model, d_ff), bf),
            pltpu.VMEM((d_ff, d_model), bf),
            dma((2, 2)),
            dma((2, last, 2, CHUNKS)),
            dma((2, 2)),
            dma((2, last, CHUNKS)),
            dma((2, last)),
            dma((CHUNKS,)),
            dma((2, 2)),
            dma((2,)),
            dma((2,)),
            dma((3,)),
            dma((3,)),
            dma((3,)),
            dma((2, 3)),
            dma((2, 3)),
            dma((3,)),
            dma((3,)),
            dma(()),
            dma((2, WAVES, BACK)),
            dma((2,)),
            dma((2, WAVES, BACK)),
            dma(()),
            dma(()),
            pltpu.SemaphoreType.REGULAR,
        ],
        compiler_params=pltpu.CompilerParams(
            collective_id=0, has_side_effects=True, vmem_limit_bytes=50 * 1024 * 1024),
        name="stream_experts",
    )(x, route, gate, wg, wu, wd)
    return out[0]


def solution(mesh):
    planes = mesh.shape["ep"] // CORES
    side = math.isqrt(mesh.shape["dp"])
    row_spec = P(("dp", "ep"))
    expert_spec = P("ep")

    def local_step(tok_loc, route_loc, gate_loc, wg_loc, wu_loc, wd_loc):
        return moe(side, planes, tok_loc, route_loc.T, gate_loc.T, wg_loc, wu_loc, wd_loc)

    return jax.shard_map(local_step, mesh=mesh, in_specs=(row_spec, row_spec, row_spec, expert_spec, expert_spec, expert_spec), out_specs=row_spec, check_vma=False)
```

```python
import functools
import math

import jax
import jax.numpy as jnp
from jax import lax
from jax.experimental import pallas as pl
from jax.experimental.pallas import tpu as pltpu
from jax.sharding import PartitionSpec as P

CORES = 2
CHUNKS = 4
TILE = 512
BACK = 4
WAVES = 2
LANES = 128


def kernel(side, planes, x_ref, route_ref, gate_ref, wg_ref, wu_ref, wd_ref,
           y_ref, gu_ref, ds_ref, tr_ref,
           x_all, route_all, gate_all, gate_cols, y_acc, b_peer, y_ret, hidden,
           gu_buf, d_buf, gu_far, d_far,
           zsend, zrecv, tsend, trecv, frecv, f3recv, farrecv, gu_sem, d_sem, own_sem, own_send, own_recv,
           near_send, near_recv, fwd_send, fwd_recv, bsend, brecv, rsend, rrecv, psend, precv, free_sem):
    last = planes // 2 - 1
    tok_n, d_model = x_ref.shape
    part_n = tok_n // 2
    tile = min(TILE, tok_n // 2)
    per_block = tok_n // tile
    experts = planes * CORES * 2
    col = lax.axis_index("dp")
    pos = lax.axis_index("ep")
    core = pos % CORES
    plane = pos // CORES
    cx, cy = col // side, col % side
    parity = (cx + cy) % 2
    cls = cx % 2
    alt = 1 - cls
    col_x = col + side * (1 - 2 * (cx % 2))
    col_y = col + 1 - 2 * (cy % 2)
    up = (pos + CORES) % (planes * CORES)
    down = (pos + (planes - 1) * CORES) % (planes * CORES)
    peer = {"ep": pos + 1 - 2 * core}
    ring = ({"ep": up}, {"ep": down})
    side_dev = ({"dp": col_x}, {"dp": col_y})
    gu_rows = wg_ref.shape[1] // CHUNKS
    d_rows = wd_ref.shape[1] // CHUNKS
    mid = CHUNKS // 2
    remote = pltpu.make_async_remote_copy

    with jax.named_scope("entry"):
        barrier = pltpu.get_barrier_semaphore()
        for dev in (*ring, *side_dev, peer):
            pl.semaphore_signal(barrier, inc=1, device_id=dev)
        pl.semaphore_wait(barrier, 5)

    def gu_cut(i):
        return pl.ds(i * gu_rows, gu_rows)

    def d_cut(i):
        return pl.ds(i * d_rows, d_rows)

    def first_gu(way, i):
        for m, w in enumerate((wg_ref, wu_ref)):
            @pl.when(cls == m)
            def _(m=m, w=w):
                remote(w.at[parity, gu_cut(i)], gu_ref.at[way, m, gu_cut(i)],
                       zsend.at[way, 0], zrecv.at[way, 0, 0, i], device_id=ring[way]).start()

    def first_d(way, i):
        remote(wd_ref.at[parity, d_cut(i)], ds_ref.at[way, d_cut(i)],
               zsend.at[way, 1], zrecv.at[way, 0, 1, i], device_id=ring[way]).start()

    def next_gu(way, h, i):
        return remote(gu_ref.at[(h - 1) * 2 + way, cls, gu_cut(i)], gu_ref.at[h * 2 + way, cls, gu_cut(i)],
                      zsend.at[way, 0], zrecv.at[way, h, 0, i], device_id=ring[way])

    def next_d(way, h, i):
        return remote(ds_ref.at[(h - 1) * 2 + way, d_cut(i)], ds_ref.at[h * 2 + way, d_cut(i)],
                      zsend.at[way, 1], zrecv.at[way, h, 1, i], device_id=ring[way])

    def wait_ring(way, h, kind, i):
        there = ds_ref.at[(h - 1) * 2 + way, d_cut(i)] if kind else gu_ref.at[(h - 1) * 2 + way, cls, gu_cut(i)]
        remote(there, there, zsend.at[way, kind], zrecv.at[way, h - 1, kind, i], device_id=ring[way]).wait_recv()

    def far_gu(way, i):
        m = cls if way == 0 else alt
        return remote(gu_ref.at[(last - 1) * 2 + way, m, gu_cut(i)], gu_far.at[m, gu_cut(i)],
                      zsend.at[way, 0], farrecv.at[way, 0], device_id=ring[way])

    def far_rows(way, part):
        return remote(ds_ref.at[(last - 1) * 2 + way, part], d_far.at[part],
                      zsend.at[way, 1], farrecv.at[way, 1], device_id=ring[way])

    def far_d(way, i):
        return far_rows(way, d_cut(i))

    d_split = d_rows // 4
    d_last = (CHUNKS - 1) * d_rows
    d_up = mid * d_rows + d_split
    d_total = wd_ref.shape[1]

    def transit_out(way, h, i):
        slot = (h - 1) * 2 + way
        return remote(gu_ref.at[slot, cls, gu_cut(i)], tr_ref.at[slot, gu_cut(i)],
                      tsend.at[way, 0], trecv.at[way, h - 1, i], device_id=side_dev[way])

    def transit_on(way, h, i, sem):
        slot = (h - 1) * 2 + way
        m = alt if way == 0 else cls
        return remote(tr_ref.at[slot, gu_cut(i)], gu_ref.at[slot, m, gu_cut(i)],
                      tsend.at[way, 1], sem, device_id=side_dev[1 - way])

    def wait_final(way, h):
        there = gu_ref.at[(h - 1) * 2 + way, alt]
        remote(there, there, tsend.at[way, 1], frecv.at[way, h - 1], device_id=side_dev[1 - way]).wait_recv()

    for i in range(CHUNKS):
        for way in range(2):
            first_gu(way, i)
    for i in range(CHUNKS):
        for way in range(2):
            first_d(way, i)

    near_block = CORES + core

    wave_n = part_n // WAVES

    def near(way):
        copies = []
        for w in range(WAVES):
            src = pl.ds(way * part_n + w * wave_n, wave_n)
            off = w * part_n + way * wave_n
            dst = pl.ds(off, wave_n)
            copies += [
                remote(route_ref.at[:, src], route_all.at[near_block, :, dst], near_send.at[way, 0], near_recv.at[way, 0], device_id=side_dev[way]),
                remote(gate_ref.at[:, src], gate_all.at[near_block, :, dst], near_send.at[way, 1], near_recv.at[way, 1], device_id=side_dev[way]),
                remote(x_ref.at[src], x_all.at[pl.ds(near_block * tok_n + off, wave_n)], near_send.at[way, 2], near_recv.at[way, 2], device_id=side_dev[way])]
        return copies

    def wait_near(way):
        part = pl.ds(0, part_n)
        for k, ref in enumerate((route_all.at[near_block, :, part], gate_all.at[near_block, :, part], x_all.at[pl.ds(near_block * tok_n, part_n)])):
            remote(ref, ref, near_send.at[way, k], near_recv.at[way, k], device_id=side_dev[way]).wait()

    for way in range(2):
        for copy in near(way):
            copy.start()

    def load_own(e):
        for m, w in enumerate((wg_ref, wu_ref)):
            pltpu.make_async_copy(w.at[e], gu_buf.at[e, m], gu_sem.at[e]).start()
        pltpu.make_async_copy(wd_ref.at[e], d_buf.at[e], d_sem.at[e]).start()

    def load_slot(h, e):
        slot = (h - 1) * 2 + e
        pltpu.make_async_copy(gu_ref.at[slot], gu_buf.at[e], gu_sem.at[e]).start()
        pltpu.make_async_copy(ds_ref.at[slot], d_buf.at[e], d_sem.at[e]).start()

    def load_early(e):
        slot = (last - 1) * 2 + e
        pltpu.make_async_copy(gu_ref.at[slot, cls], gu_buf.at[e, cls], gu_sem.at[e]).start()
        pltpu.make_async_copy(ds_ref.at[slot], d_buf.at[e], d_sem.at[e]).start()

    def load_late(e):
        slot = (last - 1) * 2 + e
        pltpu.make_async_copy(gu_ref.at[slot, alt], gu_buf.at[e, alt], gu_sem.at[e]).start()

    def wait_gu(e):
        pltpu.make_async_copy(gu_ref.at[0], gu_buf.at[e], gu_sem.at[e]).wait()

    def wait_d(e):
        pltpu.make_async_copy(ds_ref.at[0], d_buf.at[e], d_sem.at[e]).wait()

    load_own(0)
    load_own(1)
    tok = ((route_ref, route_all.at[core]), (gate_ref, gate_all.at[core]), (x_ref, x_all.at[pl.ds(core * tok_n, tok_n)]))
    for k, (src, dst) in enumerate(tok):
        remote(src, dst, own_send.at[k], own_recv.at[k], device_id=peer).start()
        pltpu.make_async_copy(src, dst, own_sem.at[k]).start()
    y_acc[...] = jnp.zeros_like(y_acc)
    y_ret[pl.ds(0, LANES), :] = jnp.zeros((LANES, d_model), jnp.float32)
    for k, (src, dst) in enumerate(tok):
        pltpu.make_async_copy(src, dst, own_sem.at[k]).wait()
        remote(src, dst, own_send.at[k], own_recv.at[k], device_id=peer).wait()

    def dense(block):
        route, gate = route_all[block], gate_all[block]
        for e in range(experts):
            y_ret[e:e + 1, pl.ds(0, tok_n)] = jnp.sum(jnp.where(route == e, gate, 0.0), axis=0, keepdims=True)
        for b in range(tok_n // LANES):
            gate_cols[pl.ds(block * tok_n + b * LANES, LANES), :] = y_ret[pl.ds(0, LANES), b * LANES:(b + 1) * LANES].T

    def dense_pair(first):
        def one(c, carry):
            dense(first + c)
            return carry

        lax.fori_loop(0, CORES, one, 0)

    dense_pair(0)

    def forward():
        mine = pl.ds(near_block * tok_n, tok_n)
        return [remote(ref, ref, fwd_send.at[k], fwd_recv.at[k], device_id=peer) for k, ref in enumerate((
            route_all.at[near_block], gate_all.at[near_block], x_all.at[mine]))]

    def expert_id(h, way):
        src = (plane + planes + (2 * way - 1) * h) % planes
        return (src * CORES + core) * 2 + parity

    def front(row0, gu):
        x_tile = x_all[pl.ds(row0, tile)]
        a = jnp.dot(x_tile, gu[0], preferred_element_type=jnp.float32)
        b = jnp.dot(x_tile, gu[1], preferred_element_type=jnp.float32)
        hidden[pl.ds(row0, tile)] = (jax.nn.silu(a) * b).astype(jnp.bfloat16)

    def back(row0, d, expert):
        part = pl.ds(row0, tile)
        out = jnp.dot(hidden[part], d, preferred_element_type=jnp.float32).astype(jnp.bfloat16)
        gates = gate_cols[part]
        lane = lax.broadcasted_iota(jnp.int32, gates.shape, 1)
        gate = jnp.sum(jnp.where(lane == expert, gates, 0.0), axis=1, keepdims=True)
        y_acc[part] += jnp.where(gate > 0.0, gate * out.astype(jnp.float32), 0.0)

    def group(e, phase, block0, blocks, expert, fresh):
        first, count = block0 * per_block, blocks * per_block

        @pl.when(phase == 0)
        def _():
            @pl.when(fresh)
            def _():
                wait_gu(e)

            def one(t, c):
                front(t * tile, gu_buf.at[e])
                return c

            with jax.named_scope("front"):
                lax.fori_loop(first, first + count, one, 0)

        @pl.when(phase == 1)
        def _():
            @pl.when(fresh)
            def _():
                wait_d(e)

            def one(t, c):
                back(t * tile, d_buf[e], expert)
                return c

            with jax.named_scope("back"):
                lax.fori_loop(first, first + count, one, 0)

    def own_id(e):
        return (plane * CORES + core) * 2 + e

    def load_pair(h):
        for way in range(2):
            with jax.named_scope("wait_final"):
                wait_final(way, h)
            load_slot(h, way)

    def stage(h, carry):
        def gates_and_ups(i, c):
            for way in range(2):
                with jax.named_scope("wait_z0"):
                    wait_ring(way, h, 0, i)

                @pl.when(h < last)
                def _():
                    next_gu(way, h, i).start()

                if way == 0:
                    @pl.when(h == last)
                    def _():
                        far_gu(0, i).start()
                transit_out(way, h, i).start()

            @pl.when((h == 2) & (i == 0))
            def _():
                with jax.named_scope("wait_fwd"):
                    for copy in forward():
                        copy.wait()
                dense_pair(CORES)

            @pl.when((h >= 3) | ((h == 1) & (i >= 2)))
            def _():
                mine = h == 1
                group(jnp.where(mine, 0, 1), jnp.where(mine, i - 2, i // 2), jnp.where(mine, 0, 2 * (i % 2)), 2,
                      jnp.where(mine, own_id(0), expert_id(h - 2, 1)), mine | (i % 2 == 0))

            @pl.when((h >= 2) & (i == CHUNKS - 1))
            def _():
                load_pair(h - 1)
            return c

        lax.fori_loop(0, CHUNKS, gates_and_ups, 0)

        def downs(i, c):
            for way in range(2):
                with jax.named_scope("wait_z1"):
                    wait_ring(way, h, 1, i)

                @pl.when(h < last)
                def _():
                    next_d(way, h, i).start()

                @pl.when((h == last) & ((i < mid) if way == 0 else (i == mid)))
                def _():
                    far_d(way, i).start()
            for way in range(2):
                with jax.named_scope("wait_t"):
                    transit_out(way, h, i).wait_recv()
                if way == 0:
                    transit_on(0, h, i, frecv.at[0, h - 1]).start()
                else:
                    @pl.when(h < last)
                    def _():
                        transit_on(1, h, i, frecv.at[1, h - 1]).start()

                    @pl.when(h == last)
                    def _():
                        transit_on(1, h, i, f3recv.at[i]).start()

            @pl.when((h == 1) & (i == 1))
            def _():
                with jax.named_scope("wait_near"):
                    for way in range(2):
                        wait_near(way)
                for copy in forward():
                    copy.start()

            @pl.when((h >= 2) | (i < 2))
            def _():
                mine = h == 1
                group(jnp.where(mine, 1, 0), jnp.where(mine, i, i // 2), jnp.where(mine, 0, 2 * (i % 2)), 2,
                      jnp.where(mine, own_id(1), expert_id(h - 1, 0)), mine | (i % 2 == 0))
            return c

        lax.fori_loop(0, CHUNKS, downs, 0)
        return carry

    lax.fori_loop(1, last + 1, stage, 0)

    load_early(0)
    far_rows(0, pl.ds(d_last, d_split)).start()

    def rest(n, c):
        group(1, n // 4, n % 4, 1, expert_id(last - 1, 1), n % 4 == 0)

        @pl.when(n == 2 * CHUNKS - 1)
        def _():
            load_early(1)

        @pl.when((n == 0) | (n == 2) | (n == 5) | (n == 7))
        def _():
            i = (n + 1) // 2 - n // 5
            with jax.named_scope("wait_f3"):
                transit_on(1, last, i, f3recv.at[i]).wait_recv()
            far_gu(1, i).start()
        return c

    lax.fori_loop(0, 2 * CHUNKS, rest, 0)
    with jax.named_scope("wait_final"):
        wait_final(0, last)
    load_late(0)
    load_late(1)
    far_rows(1, pl.ds(d_last + d_split, d_rows - d_split)).start()

    theirs, ours = CORES + 1 - core, CORES + core
    far_expert = expert_id(last + 1, 0)

    def far_front(row0):
        front(row0, gu_far)

    def far_back(row0):
        back(row0, d_far[...], far_expert)

    def both(fn, w):
        def one(n, c):
            fn((theirs + n * (ours - theirs)) * tok_n + w * part_n)
            return c

        lax.fori_loop(0, CORES, one, 0)

    def near_group(g, c):
        w = g // 4
        e, phase = (g % 4) // 2, g % 2

        @pl.when(phase == 0)
        def _():
            @pl.when(w == 0)
            def _():
                wait_gu(e)
            with jax.named_scope("near_front"):
                both(lambda row0: front(row0, gu_buf.at[e]), w)

        @pl.when(phase == 1)
        def _():
            @pl.when(w == 0)
            def _():
                wait_d(e)
            with jax.named_scope("near_back"):
                both(lambda row0: back(row0, d_buf[e], expert_id(last, e)), w)
        return c

    size = wave_n // BACK

    def to_peer(way, w, k):
        off = w * part_n + way * wave_n + k * size
        return remote(y_acc.at[pl.ds(theirs * tok_n + off, size)], b_peer.at[pl.ds(off, size)],
                      bsend, brecv.at[way, w, k], device_id=peer)

    def give_back(way, w, k):
        src = ours * tok_n + w * part_n + way * wave_n + k * size
        return remote(y_acc.at[pl.ds(src, size)], y_ret.at[pl.ds(way * part_n + w * wave_n + k * size, size)],
                      rsend.at[way], rrecv.at[way, w, k], device_id=side_dev[way])

    def wave(w, c):
        first = w == 0
        lax.fori_loop(4 * w, 4 * w + 4, near_group, 0)

        @pl.when(first)
        def _():
            with jax.named_scope("wait_far0"):
                for way in range(2):
                    m = cls if way == 0 else alt
                    remote(gu_far.at[m], gu_far.at[m], zsend.at[way, 0], farrecv.at[way, 0], device_id=ring[way]).wait_recv()
        with jax.named_scope("far_front"):
            both(far_front, w)

        @pl.when(first)
        def _():
            with jax.named_scope("wait_far1"):
                for way in range(2):
                    there = d_far.at[pl.ds(0, d_up if way == 0 else d_total - d_up)]
                    remote(there, there, zsend.at[way, 1], farrecv.at[way, 1], device_id=ring[way]).wait_recv()
        with jax.named_scope("far_back"):
            far_back(theirs * tok_n + w * part_n)
        for k in range(BACK):
            for way in range(2):
                to_peer(way, w, k).start()
        with jax.named_scope("far_back"):
            far_back(ours * tok_n + w * part_n)

        def sums(k, c2):
            @pl.when(k < BACK)
            def _():
                for way in range(2):
                    with jax.named_scope("wait_b"):
                        to_peer(way, w, k).wait_recv()
                    off = w * part_n + way * wave_n + k * size
                    y_acc[pl.ds(ours * tok_n + off, size)] += b_peer[pl.ds(off, size)]

            @pl.when(k > 0)
            def _():
                for way in range(2):
                    give_back(way, w, k - 1).start()
            return c2

        lax.fori_loop(0, BACK + 1, sums, 0)
        return c

    lax.fori_loop(0, WAVES, wave, 0)
    with jax.named_scope("wait_bsend"):
        remote(b_peer, b_peer, bsend, brecv.at[0, 0, 0], device_id=peer).wait_send()
    pl.semaphore_signal(free_sem, inc=1, device_id=peer)

    def own_block(block):
        def one(g, c):
            group(g // 2, g % 2, block, 1, expert_id(last, g // 2), g < 0)
            return c

        lax.fori_loop(0, 4, one, 0)
        with jax.named_scope("far_own"):
            for fn in (far_front, far_back):
                def one(t, c, fn=fn):
                    fn((block * per_block + t) * tile)
                    return c

                lax.fori_loop(0, per_block, one, 0)

    def part_copy():
        return remote(y_acc.at[pl.ds((1 - core) * tok_n, tok_n)], y_acc.at[pl.ds(ours * tok_n, tok_n)], psend, precv, device_id=peer)

    def own_blocks(n, c):
        own_block(core + (1 - n) * (1 - 2 * core))

        @pl.when(n == 0)
        def _():
            pl.semaphore_wait(free_sem, 1)
            part_copy().start()
        return c

    lax.fori_loop(0, CORES, own_blocks, 0)
    with jax.named_scope("wait_part"):
        part_copy().wait()

    def finish(k, c):
        for way in range(2):
            with jax.named_scope("wait_r"):
                give_back(way, k // BACK, k % BACK).wait_recv()
            part = pl.ds(way * part_n + k * size, size)
            mine = pl.ds(core * tok_n + way * part_n + k * size, size)
            other = pl.ds(theirs * tok_n + way * part_n + k * size, size)
            y_ref[part] = (y_acc[mine] + y_acc[other] + y_ret[part]).astype(y_ref.dtype)
        return c

    lax.fori_loop(0, WAVES * BACK, finish, 0)

    with jax.named_scope("drain"):
        for way in range(2):
            whole = gu_ref.at[pl.ds(0, (last + 1) // 2)]
            remote(whole, whole, zsend.at[way, 0], farrecv.at[way, 0], device_id=ring[way]).wait_send()
            d_sent = last * d_total + (d_up if way == 0 else d_total - d_up)
            whole = gu_ref.at[pl.ds(0, 2), pl.ds(0, 2), pl.ds(0, d_sent * d_model // (4 * gu_ref.shape[3]))]
            remote(whole, whole, zsend.at[way, 1], farrecv.at[way, 1], device_id=ring[way]).wait_send()
            whole = tr_ref.at[pl.ds(0, last)]
            for hop in range(2):
                remote(whole, whole, tsend.at[way, hop], frecv.at[way, 0], device_id=side_dev[way]).wait_send()
            whole = y_ret.at[pl.ds(0, part_n)]
            remote(whole, whole, rsend.at[way], rrecv.at[way, 0, 0], device_id=side_dev[way]).wait_send()


def moe(side, planes, x, route, gate, wg, wu, wd):
    tok_n, d_model = x.shape
    d_ff = wg.shape[2]
    last = planes // 2 - 1
    bf = jnp.bfloat16
    f32 = jnp.float32
    any_spec = pl.BlockSpec(memory_space=pl.ANY)
    dma = pltpu.SemaphoreType.DMA
    blocks = 2 * CORES
    rows = blocks * tok_n
    top_k = route.shape[0]
    out = pl.pallas_call(
        functools.partial(kernel, side, planes),
        out_shape=(
            jax.ShapeDtypeStruct((tok_n, d_model), bf),
            jax.ShapeDtypeStruct((2 * last, 2, d_model, d_ff), bf),
            jax.ShapeDtypeStruct((2 * last, d_ff, d_model), bf),
            jax.ShapeDtypeStruct((2 * last, d_model, d_ff), bf),
        ),
        in_specs=[any_spec] * 6,
        out_specs=(pl.BlockSpec(memory_space=pltpu.VMEM),) + (any_spec,) * 3,
        scratch_shapes=[
            pltpu.VMEM((rows, d_model), bf),
            pltpu.VMEM((blocks, top_k, tok_n), jnp.int32),
            pltpu.VMEM((blocks, top_k, tok_n), f32),
            pltpu.VMEM((rows, LANES), f32),
            pltpu.VMEM((rows, d_model), f32),
            pltpu.VMEM((tok_n, d_model), f32),
            pltpu.VMEM((tok_n, d_model), f32),
            pltpu.VMEM((rows, d_ff), bf),
            pltpu.VMEM((2, 2, d_model, d_ff), bf),
            pltpu.VMEM((2, d_ff, d_model), bf),
            pltpu.VMEM((2, d_model, d_ff), bf),
            pltpu.VMEM((d_ff, d_model), bf),
            dma((2, 2)),
            dma((2, last, 2, CHUNKS)),
            dma((2, 2)),
            dma((2, last, CHUNKS)),
            dma((2, last)),
            dma((CHUNKS,)),
            dma((2, 2)),
            dma((2,)),
            dma((2,)),
            dma((3,)),
            dma((3,)),
            dma((3,)),
            dma((2, 3)),
            dma((2, 3)),
            dma((3,)),
            dma((3,)),
            dma(()),
            dma((2, WAVES, BACK)),
            dma((2,)),
            dma((2, WAVES, BACK)),
            dma(()),
            dma(()),
            pltpu.SemaphoreType.REGULAR,
        ],
        compiler_params=pltpu.CompilerParams(
            collective_id=0, has_side_effects=True, vmem_limit_bytes=103 * 512 * 1024),
        name="stream_experts",
    )(x, route, gate, wg, wu, wd)
    return out[0]


def solution(mesh):
    planes = mesh.shape["ep"] // CORES
    side = math.isqrt(mesh.shape["dp"])
    row_spec = P(("dp", "ep"))
    expert_spec = P("ep")

    def local_step(tok_loc, route_loc, gate_loc, wg_loc, wu_loc, wd_loc):
        tables = (pltpu.with_memory_space_constraint(table.T, pltpu.HBM) for table in (route_loc, gate_loc))
        return moe(side, planes, tok_loc, *tables, wg_loc, wu_loc, wd_loc)

    return jax.shard_map(local_step, mesh=mesh, in_specs=(row_spec, row_spec, row_spec, expert_spec, expert_spec, expert_spec), out_specs=row_spec, check_vma=False)
```

```python
import functools
import math

import jax
import jax.numpy as jnp
from jax import lax
from jax.experimental import pallas as pl
from jax.experimental.pallas import tpu as pltpu
from jax.sharding import PartitionSpec as P

CORES = 2
CHUNKS = 4
TILE = 512
BACK = 4
WAVES = 2
LANES = 128


def kernel(side, planes, x_ref, route_ref, gate_ref, wg_ref, wu_ref, wd_ref,
           y_ref, gu_ref, ds_ref, tr_ref,
           x_all, route_all, gate_all, gate_cols, y_acc, b_peer, y_ret, hidden,
           gu_buf, d_buf, gu_far, d_far,
           zsend, zrecv, tsend, trecv, frecv, f3recv, farrecv, gu_sem, d_sem, own_sem, own_send, own_recv,
           near_send, near_recv, fwd_send, fwd_recv, bsend, brecv, rsend, rrecv, psend, precv, free_sem):
    last = planes // 2 - 1
    tok_n, d_model = x_ref.shape
    part_n = tok_n // 2
    tile = min(TILE, tok_n // 2)
    per_block = tok_n // tile
    experts = planes * CORES * 2
    col = lax.axis_index("dp")
    pos = lax.axis_index("ep")
    core = pos % CORES
    plane = pos // CORES
    cx, cy = col // side, col % side
    parity = (cx + cy) % 2
    cls = cx % 2
    alt = 1 - cls
    col_x = col + side * (1 - 2 * (cx % 2))
    col_y = col + 1 - 2 * (cy % 2)
    up = (pos + CORES) % (planes * CORES)
    down = (pos + (planes - 1) * CORES) % (planes * CORES)
    peer = {"ep": pos + 1 - 2 * core}
    ring = ({"ep": up}, {"ep": down})
    side_dev = ({"dp": col_x}, {"dp": col_y})
    gu_rows = wg_ref.shape[1] // CHUNKS
    d_rows = wd_ref.shape[1] // CHUNKS
    mid = CHUNKS // 2
    remote = pltpu.make_async_remote_copy

    with jax.named_scope("entry"):
        barrier = pltpu.get_barrier_semaphore()
        for dev in (*ring, *side_dev, peer):
            pl.semaphore_signal(barrier, inc=1, device_id=dev)
        pl.semaphore_wait(barrier, 5)

    def gu_cut(i):
        return pl.ds(i * gu_rows, gu_rows)

    def d_cut(i):
        return pl.ds(i * d_rows, d_rows)

    def first_gu(way, i):
        for m, w in enumerate((wg_ref, wu_ref)):
            @pl.when(cls == m)
            def _(m=m, w=w):
                remote(w.at[parity, gu_cut(i)], gu_ref.at[way, m, gu_cut(i)],
                       zsend.at[way, 0], zrecv.at[way, 0, 0, i], device_id=ring[way]).start()

    def first_d(way, i):
        remote(wd_ref.at[parity, d_cut(i)], ds_ref.at[way, d_cut(i)],
               zsend.at[way, 1], zrecv.at[way, 0, 1, i], device_id=ring[way]).start()

    def next_gu(way, h, i):
        return remote(gu_ref.at[(h - 1) * 2 + way, cls, gu_cut(i)], gu_ref.at[h * 2 + way, cls, gu_cut(i)],
                      zsend.at[way, 0], zrecv.at[way, h, 0, i], device_id=ring[way])

    def next_d(way, h, i):
        return remote(ds_ref.at[(h - 1) * 2 + way, d_cut(i)], ds_ref.at[h * 2 + way, d_cut(i)],
                      zsend.at[way, 1], zrecv.at[way, h, 1, i], device_id=ring[way])

    def wait_ring(way, h, kind, i):
        there = ds_ref.at[(h - 1) * 2 + way, d_cut(i)] if kind else gu_ref.at[(h - 1) * 2 + way, cls, gu_cut(i)]
        remote(there, there, zsend.at[way, kind], zrecv.at[way, h - 1, kind, i], device_id=ring[way]).wait_recv()

    def far_gu(way, i):
        m = cls if way == 0 else alt
        return remote(gu_ref.at[(last - 1) * 2 + way, m, gu_cut(i)], gu_far.at[m, gu_cut(i)],
                      zsend.at[way, 0], farrecv.at[way, 0], device_id=ring[way])

    def far_rows(way, part):
        return remote(ds_ref.at[(last - 1) * 2 + way, part], d_far.at[part],
                      zsend.at[way, 1], farrecv.at[way, 1], device_id=ring[way])

    def far_d(way, i):
        return far_rows(way, d_cut(i))

    d_split = d_rows // 4
    d_last = (CHUNKS - 1) * d_rows
    d_up = mid * d_rows + d_split
    d_total = wd_ref.shape[1]

    def transit_out(way, h, i):
        slot = (h - 1) * 2 + way
        return remote(gu_ref.at[slot, cls, gu_cut(i)], tr_ref.at[slot, gu_cut(i)],
                      tsend.at[way, 0], trecv.at[way, h - 1, i], device_id=side_dev[way])

    def transit_on(way, h, i, sem):
        slot = (h - 1) * 2 + way
        m = alt if way == 0 else cls
        return remote(tr_ref.at[slot, gu_cut(i)], gu_ref.at[slot, m, gu_cut(i)],
                      tsend.at[way, 1], sem, device_id=side_dev[1 - way])

    def wait_final(way, h):
        there = gu_ref.at[(h - 1) * 2 + way, alt]
        remote(there, there, tsend.at[way, 1], frecv.at[way, h - 1], device_id=side_dev[1 - way]).wait_recv()


    wave_n = part_n // WAVES

    def near_row(w, k):
        return (CORES + w) * tok_n + k * part_n

    def near(way):
        copies = []
        for w in range(WAVES):
            src = pl.ds(way * part_n + w * wave_n, wave_n)
            dst = pl.ds(pl.multiple_of(core * part_n + way * wave_n, wave_n), wave_n)
            copies += [
                remote(route_ref.at[:, src], route_all.at[CORES + w, :, dst], near_send.at[way, 0], near_recv.at[way, 0], device_id=side_dev[way]),
                remote(gate_ref.at[:, src], gate_all.at[CORES + w, :, dst], near_send.at[way, 1], near_recv.at[way, 1], device_id=side_dev[way]),
                remote(x_ref.at[src], x_all.at[pl.ds(near_row(w, core) + way * wave_n, wave_n)], near_send.at[way, 2], near_recv.at[way, 2], device_id=side_dev[way])]
        return copies

    def wait_near(way):
        part = pl.ds(0, part_n)
        for k, ref in enumerate((route_all.at[CORES, :, part], gate_all.at[CORES, :, part], x_all.at[pl.ds(CORES * tok_n, part_n)])):
            remote(ref, ref, near_send.at[way, k], near_recv.at[way, k], device_id=side_dev[way]).wait()

    for way in range(2):
        for copy in near(way):
            copy.start()
    for i in range(CHUNKS):
        for way in range(2):
            first_gu(way, i)
    for i in range(CHUNKS):
        for way in range(2):
            first_d(way, i)

    def load_own(e):
        for m, w in enumerate((wg_ref, wu_ref)):
            pltpu.make_async_copy(w.at[e], gu_buf.at[e, m], gu_sem.at[e]).start()
        pltpu.make_async_copy(wd_ref.at[e], d_buf.at[e], d_sem.at[e]).start()

    def load_slot(h, e):
        slot = (h - 1) * 2 + e
        pltpu.make_async_copy(gu_ref.at[slot], gu_buf.at[e], gu_sem.at[e]).start()
        pltpu.make_async_copy(ds_ref.at[slot], d_buf.at[e], d_sem.at[e]).start()

    def load_early(e):
        slot = (last - 1) * 2 + e
        pltpu.make_async_copy(gu_ref.at[slot, cls], gu_buf.at[e, cls], gu_sem.at[e]).start()
        pltpu.make_async_copy(ds_ref.at[slot], d_buf.at[e], d_sem.at[e]).start()

    def load_late(e):
        slot = (last - 1) * 2 + e
        pltpu.make_async_copy(gu_ref.at[slot, alt], gu_buf.at[e, alt], gu_sem.at[e]).start()

    def wait_gu(e):
        pltpu.make_async_copy(gu_ref.at[0], gu_buf.at[e], gu_sem.at[e]).wait()

    def wait_d(e):
        pltpu.make_async_copy(ds_ref.at[0], d_buf.at[e], d_sem.at[e]).wait()

    load_own(0)
    load_own(1)
    tok = ((route_ref, route_all.at[core]), (gate_ref, gate_all.at[core]), (x_ref, x_all.at[pl.ds(core * tok_n, tok_n)]))
    for k, (src, dst) in enumerate(tok):
        remote(src, dst, own_send.at[k], own_recv.at[k], device_id=peer).start()
        pltpu.make_async_copy(src, dst, own_sem.at[k]).start()
    y_acc[...] = jnp.zeros_like(y_acc)
    y_ret[pl.ds(0, LANES), :] = jnp.zeros((LANES, d_model), jnp.float32)
    for k, (src, dst) in enumerate(tok):
        pltpu.make_async_copy(src, dst, own_sem.at[k]).wait()
        remote(src, dst, own_send.at[k], own_recv.at[k], device_id=peer).wait()

    def dense(block):
        route, gate = route_all[block], gate_all[block]
        for e in range(experts):
            y_ret[e:e + 1, pl.ds(0, tok_n)] = jnp.sum(jnp.where(route == e, gate, 0.0), axis=0, keepdims=True)
        for b in range(tok_n // LANES):
            gate_cols[pl.ds(block * tok_n + b * LANES, LANES), :] = y_ret[pl.ds(0, LANES), b * LANES:(b + 1) * LANES].T

    def dense_pair(first):
        def one(c, carry):
            dense(first + c)
            return carry

        lax.fori_loop(0, CORES, one, 0)

    dense_pair(0)

    def forward():
        lanes = pl.ds(pl.multiple_of(core * part_n, part_n), part_n)
        return [remote(ref, ref, fwd_send.at[k], fwd_recv.at[k], device_id=peer) for w in range(WAVES) for k, ref in enumerate((
            route_all.at[CORES + w, :, lanes], gate_all.at[CORES + w, :, lanes], x_all.at[pl.ds(near_row(w, core), part_n)]))]

    def wait_forward():
        for k, ref in enumerate((route_all.at[CORES], gate_all.at[CORES], x_all.at[pl.ds(CORES * tok_n, tok_n)])):
            remote(ref, ref, fwd_send.at[k], fwd_recv.at[k], device_id=peer).wait()

    def expert_id(h, way):
        src = (plane + planes + (2 * way - 1) * h) % planes
        return (src * CORES + core) * 2 + parity

    def front(row0, gu, n=tile):
        if n > 512:
            def piece(t, c):
                front(row0 + t * tile, gu)
                return c

            lax.fori_loop(0, n // tile, piece, 0)
            return
        part = pl.ds(row0, n)
        x_tile = x_all[part]
        a = jnp.dot(x_tile, gu[0], preferred_element_type=jnp.float32)
        b = jnp.dot(x_tile, gu[1], preferred_element_type=jnp.float32)
        hidden[part] = (jax.nn.silu(a) * b).astype(jnp.bfloat16)

    def back(row0, d, expert, n=tile):
        if n > 512:
            def piece(t, c):
                back(row0 + t * tile, d, expert)
                return c

            lax.fori_loop(0, n // tile, piece, 0)
            return
        part = pl.ds(row0, n)
        out = jnp.dot(hidden[part], d, preferred_element_type=jnp.float32).astype(jnp.bfloat16)
        gates = gate_cols[part]
        lane = lax.broadcasted_iota(jnp.int32, gates.shape, 1)
        gate = jnp.sum(jnp.where(lane == expert, gates, 0.0), axis=1, keepdims=True)
        y_acc[part] += jnp.where(gate > 0.0, gate * out.astype(jnp.float32), 0.0)

    def group(e, phase, block0, blocks, expert, fresh):
        first, count = block0 * per_block, blocks * per_block

        @pl.when(phase == 0)
        def _():
            @pl.when(fresh)
            def _():
                wait_gu(e)

            def one(t, c):
                front(t * tile, gu_buf.at[e])
                return c

            with jax.named_scope("front"):
                lax.fori_loop(first, first + count, one, 0)

        @pl.when(phase == 1)
        def _():
            @pl.when(fresh)
            def _():
                wait_d(e)

            def one(t, c):
                back(t * tile, d_buf[e], expert)
                return c

            with jax.named_scope("back"):
                lax.fori_loop(first, first + count, one, 0)

    def own_id(e):
        return (plane * CORES + core) * 2 + e

    def load_pair(h):
        for way in range(2):
            with jax.named_scope("wait_final"):
                wait_final(way, h)
            load_slot(h, way)

    def stage(h, carry):
        def gates_and_ups(i, c):
            for way in range(2):
                with jax.named_scope("wait_z0"):
                    wait_ring(way, h, 0, i)

                @pl.when(h < last)
                def _():
                    next_gu(way, h, i).start()

                if way == 0:
                    @pl.when(h == last)
                    def _():
                        far_gu(0, i).start()
                transit_out(way, h, i).start()

            @pl.when((h == 2) & (i == 0))
            def _():
                with jax.named_scope("wait_fwd"):
                    wait_forward()
                dense_pair(CORES)

            @pl.when((h >= 3) | ((h == 1) & (i >= 2)))
            def _():
                mine = h == 1
                group(jnp.where(mine, 0, 1), jnp.where(mine, i - 2, i // 2), jnp.where(mine, 0, 2 * (i % 2)), 2,
                      jnp.where(mine, own_id(0), expert_id(h - 2, 1)), mine | (i % 2 == 0))

            @pl.when((h >= 2) & (i == CHUNKS - 1))
            def _():
                load_pair(h - 1)
            return c

        lax.fori_loop(0, CHUNKS, gates_and_ups, 0)

        def downs(i, c):
            for way in range(2):
                with jax.named_scope("wait_z1"):
                    wait_ring(way, h, 1, i)

                @pl.when(h < last)
                def _():
                    next_d(way, h, i).start()

                @pl.when((h == last) & ((i < mid) if way == 0 else (i == mid)))
                def _():
                    far_d(way, i).start()
            for way in range(2):
                with jax.named_scope("wait_t"):
                    transit_out(way, h, i).wait_recv()
                if way == 0:
                    transit_on(0, h, i, frecv.at[0, h - 1]).start()
                else:
                    @pl.when(h < last)
                    def _():
                        transit_on(1, h, i, frecv.at[1, h - 1]).start()

                    @pl.when(h == last)
                    def _():
                        transit_on(1, h, i, f3recv.at[i]).start()

            @pl.when((h == 1) & (i == 1))
            def _():
                with jax.named_scope("wait_near"):
                    for way in range(2):
                        wait_near(way)
                for copy in forward():
                    copy.start()

            @pl.when((h >= 2) | (i < 2))
            def _():
                mine = h == 1
                group(jnp.where(mine, 1, 0), jnp.where(mine, i, i // 2), jnp.where(mine, 0, 2 * (i % 2)), 2,
                      jnp.where(mine, own_id(1), expert_id(h - 1, 0)), mine | (i % 2 == 0))
            return c

        lax.fori_loop(0, CHUNKS, downs, 0)
        return carry

    lax.fori_loop(1, last + 1, stage, 0)

    load_early(0)
    far_rows(0, pl.ds(d_last, d_split)).start()

    def rest(n, c):
        group(1, n // 4, n % 4, 1, expert_id(last - 1, 1), n % 4 == 0)

        @pl.when(n == 2 * CHUNKS - 1)
        def _():
            load_early(1)

        @pl.when((n == 0) | (n == 2) | (n == 5) | (n == 7))
        def _():
            i = (n + 1) // 2 - n // 5
            with jax.named_scope("wait_f3"):
                transit_on(1, last, i, f3recv.at[i]).wait_recv()
            far_gu(1, i).start()
        return c

    lax.fori_loop(0, 2 * CHUNKS, rest, 0)
    with jax.named_scope("wait_final"):
        wait_final(0, last)
    load_late(0)
    load_late(1)
    far_rows(1, pl.ds(d_last + d_split, d_rows - d_split)).start()

    def both(w):
        return (CORES + w) * tok_n

    far_expert = expert_id(last + 1, 0)

    def near_group(g, c):
        w = g // 4
        e, phase = (g % 4) // 2, g % 2

        @pl.when(phase == 0)
        def _():
            @pl.when(w == 0)
            def _():
                wait_gu(e)
            with jax.named_scope("near_front"):
                front(both(w), gu_buf.at[e], tok_n)

        @pl.when(phase == 1)
        def _():
            @pl.when(w == 0)
            def _():
                wait_d(e)
            with jax.named_scope("near_back"):
                back(both(w), d_buf[e], expert_id(last, e), tok_n)
        return c

    size = wave_n // BACK

    def to_peer(way, w, k):
        off = w * part_n + way * wave_n + k * size
        return remote(y_acc.at[pl.ds(near_row(w, 1 - core) + way * wave_n + k * size, size)], b_peer.at[pl.ds(off, size)],
                      bsend, brecv.at[way, w, k], device_id=peer)

    def give_back(way, w, k):
        src = near_row(w, core) + way * wave_n + k * size
        return remote(y_acc.at[pl.ds(src, size)], y_ret.at[pl.ds(way * part_n + w * wave_n + k * size, size)],
                      rsend.at[way], rrecv.at[way, w], device_id=side_dev[way])

    def wave(w, c):
        first = w == 0
        lax.fori_loop(4 * w, 4 * w + 4, near_group, 0)

        @pl.when(first)
        def _():
            with jax.named_scope("wait_far0"):
                for way in range(2):
                    m = cls if way == 0 else alt
                    remote(gu_far.at[m], gu_far.at[m], zsend.at[way, 0], farrecv.at[way, 0], device_id=ring[way]).wait_recv()
        with jax.named_scope("far_front"):
            front(both(w), gu_far, tok_n)

        @pl.when(first)
        def _():
            with jax.named_scope("wait_far1"):
                for way in range(2):
                    there = d_far.at[pl.ds(0, d_up if way == 0 else d_total - d_up)]
                    remote(there, there, zsend.at[way, 1], farrecv.at[way, 1], device_id=ring[way]).wait_recv()
        with jax.named_scope("far_back"):
            back(near_row(w, 1 - core), d_far[...], far_expert, part_n)
        for k in range(BACK):
            for way in range(2):
                to_peer(way, w, k).start()
        with jax.named_scope("far_back"):
            back(near_row(w, core), d_far[...], far_expert, part_n)

        def sums(k, c2):
            @pl.when(k < BACK)
            def _():
                for way in range(2):
                    with jax.named_scope("wait_b"):
                        to_peer(way, w, k).wait_recv()
                    off = w * part_n + way * wave_n + k * size
                    y_acc[pl.ds(near_row(w, core) + way * wave_n + k * size, size)] += b_peer[pl.ds(off, size)]

            @pl.when(k > 0)
            def _():
                for way in range(2):
                    give_back(way, w, k - 1).start()
            return c2

        lax.fori_loop(0, BACK + 1, sums, 0)
        return c

    lax.fori_loop(0, WAVES, wave, 0)
    with jax.named_scope("wait_bsend"):
        remote(b_peer, b_peer, bsend, brecv.at[0, 0, 0], device_id=peer).wait_send()
    pl.semaphore_signal(free_sem, inc=1, device_id=peer)

    def own_block(block):
        row0 = block * tok_n

        def one(e, c):
            with jax.named_scope("own"):
                front(row0, gu_buf.at[e], tok_n)
                back(row0, d_buf[e], expert_id(last, e), tok_n)
            return c

        lax.fori_loop(0, 2, one, 0)
        with jax.named_scope("far_own"):
            front(row0, gu_far, tok_n)
            back(row0, d_far[...], far_expert, tok_n)

    def part_copy(w):
        return remote(y_acc.at[pl.ds((1 - core) * tok_n + w * part_n, part_n)], y_acc.at[pl.ds(near_row(w, core), part_n)],
                      psend, precv, device_id=peer)

    def own_blocks(n, c):
        own_block(core + (1 - n) * (1 - 2 * core))

        @pl.when(n == 0)
        def _():
            pl.semaphore_wait(free_sem, 1)
            for w in range(WAVES):
                part_copy(w).start()
        return c

    lax.fori_loop(0, CORES, own_blocks, 0)
    with jax.named_scope("wait_part"):
        whole = y_acc.at[pl.ds(0, tok_n)]
        remote(whole, whole, psend, precv, device_id=peer).wait()

    def finish(w, c):
        for way in range(2):
            off = w * wave_n
            part = pl.ds(way * part_n + off, wave_n)
            with jax.named_scope("wait_r"):
                remote(y_ret.at[part], y_ret.at[part], rsend.at[way], rrecv.at[way, w], device_id=side_dev[way]).wait_recv()
            mine = pl.ds(core * tok_n + way * part_n + off, wave_n)
            other = pl.ds(near_row(way, 1 - core) + off, wave_n)
            y_ref[part] = (y_acc[mine] + y_acc[other] + y_ret[part]).astype(y_ref.dtype)
        return c

    lax.fori_loop(0, WAVES, finish, 0)

    with jax.named_scope("drain"):
        for way in range(2):
            whole = gu_ref.at[pl.ds(0, (last + 1) // 2)]
            remote(whole, whole, zsend.at[way, 0], farrecv.at[way, 0], device_id=ring[way]).wait_send()
            d_sent = last * d_total + (d_up if way == 0 else d_total - d_up)
            whole = gu_ref.at[pl.ds(0, 2), pl.ds(0, 2), pl.ds(0, d_sent * d_model // (4 * gu_ref.shape[3]))]
            remote(whole, whole, zsend.at[way, 1], farrecv.at[way, 1], device_id=ring[way]).wait_send()
            whole = tr_ref.at[pl.ds(0, last)]
            for hop in range(2):
                remote(whole, whole, tsend.at[way, hop], frecv.at[way, 0], device_id=side_dev[way]).wait_send()
            whole = y_ret.at[pl.ds(0, part_n)]
            remote(whole, whole, rsend.at[way], rrecv.at[way, 0], device_id=side_dev[way]).wait_send()


def moe(side, planes, x, route, gate, wg, wu, wd):
    tok_n, d_model = x.shape
    d_ff = wg.shape[2]
    last = planes // 2 - 1
    bf = jnp.bfloat16
    f32 = jnp.float32
    any_spec = pl.BlockSpec(memory_space=pl.ANY)
    dma = pltpu.SemaphoreType.DMA
    blocks = 2 * CORES
    rows = blocks * tok_n
    top_k = route.shape[0]
    out = pl.pallas_call(
        functools.partial(kernel, side, planes),
        out_shape=(
            jax.ShapeDtypeStruct((tok_n, d_model), bf),
            jax.ShapeDtypeStruct((2 * last, 2, d_model, d_ff), bf),
            jax.ShapeDtypeStruct((2 * last, d_ff, d_model), bf),
            jax.ShapeDtypeStruct((2 * last, d_model, d_ff), bf),
        ),
        in_specs=[any_spec] * 6,
        out_specs=(pl.BlockSpec(memory_space=pltpu.VMEM),) + (any_spec,) * 3,
        scratch_shapes=[
            pltpu.VMEM((rows, d_model), bf),
            pltpu.VMEM((blocks, top_k, tok_n), jnp.int32),
            pltpu.VMEM((blocks, top_k, tok_n), f32),
            pltpu.VMEM((rows, LANES), f32),
            pltpu.VMEM((rows, d_model), f32),
            pltpu.VMEM((tok_n, d_model), f32),
            pltpu.VMEM((tok_n, d_model), f32),
            pltpu.VMEM((rows, d_ff), bf),
            pltpu.VMEM((2, 2, d_model, d_ff), bf),
            pltpu.VMEM((2, d_ff, d_model), bf),
            pltpu.VMEM((2, d_model, d_ff), bf),
            pltpu.VMEM((d_ff, d_model), bf),
            dma((2, 2)),
            dma((2, last, 2, CHUNKS)),
            dma((2, 2)),
            dma((2, last, CHUNKS)),
            dma((2, last)),
            dma((CHUNKS,)),
            dma((2, 2)),
            dma((2,)),
            dma((2,)),
            dma((3,)),
            dma((3,)),
            dma((3,)),
            dma((2, 3)),
            dma((2, 3)),
            dma((3,)),
            dma((3,)),
            dma(()),
            dma((2, WAVES, BACK)),
            dma((2,)),
            dma((2, WAVES)),
            dma(()),
            dma(()),
            pltpu.SemaphoreType.REGULAR,
        ],
        compiler_params=pltpu.CompilerParams(
            collective_id=0, has_side_effects=True, vmem_limit_bytes=103 * 512 * 1024),
        name="stream_experts",
    )(x, route, gate, wg, wu, wd)
    return out[0]


def solution(mesh):
    planes = mesh.shape["ep"] // CORES
    side = math.isqrt(mesh.shape["dp"])
    row_spec = P(("dp", "ep"))
    expert_spec = P("ep")

    def local_step(tok_loc, route_loc, gate_loc, wg_loc, wu_loc, wd_loc):
        tables = (pltpu.with_memory_space_constraint(table.T, pltpu.HBM) for table in (route_loc, gate_loc))
        return moe(side, planes, tok_loc, *tables, wg_loc, wu_loc, wd_loc)

    return jax.shard_map(local_step, mesh=mesh, in_specs=(row_spec, row_spec, row_spec, expert_spec, expert_spec, expert_spec), out_specs=row_spec, check_vma=False)
```

```python
import functools
import math

import jax
import jax.numpy as jnp
from jax import lax
from jax.experimental import pallas as pl
from jax.experimental.pallas import tpu as pltpu
from jax.sharding import PartitionSpec as P

CORES = 2
CHUNKS = 4
TILE = 512
BACK = 2
WAVES = 2
LANES = 128


def kernel(side, planes, x_ref, route_ref, gate_ref, wg_ref, wu_ref, wd_ref,
           y_ref, gu_ref, ds_ref, tr_ref,
           x_all, route_all, gate_all, gate_cols, y_acc, b_peer, y_ret, hidden,
           gu_buf, d_buf, gu_far, d_far,
           zsend, zrecv, tsend, trecv, frecv, f3recv, farrecv, xrecv, f2recv, gu_sem, d_sem, own_sem, own_send, own_recv,
           near_send, near_recv, fwd_send, fwd_recv, bsend, brecv, rsend, rrecv, psend, precv, half_sem, free_sem):
    last = planes // 2 - 1
    tok_n, d_model = x_ref.shape
    part_n = tok_n // 2
    tile = min(TILE, tok_n // 2)
    per_block = tok_n // tile
    experts = planes * CORES * 2
    col = lax.axis_index("dp")
    pos = lax.axis_index("ep")
    core = pos % CORES
    plane = pos // CORES
    cx, cy = col // side, col % side
    parity = (cx + cy) % 2
    cls = cx % 2
    alt = 1 - cls
    col_x = col + side * (1 - 2 * (cx % 2))
    col_y = col + 1 - 2 * (cy % 2)
    up = (pos + CORES) % (planes * CORES)
    down = (pos + (planes - 1) * CORES) % (planes * CORES)
    peer = {"ep": pos + 1 - 2 * core}
    ring = ({"ep": up}, {"ep": down})
    side_dev = ({"dp": col_x}, {"dp": col_y})
    gu_rows = wg_ref.shape[1] // CHUNKS
    d_rows = wd_ref.shape[1] // CHUNKS
    remote = pltpu.make_async_remote_copy

    with jax.named_scope("entry"):
        barrier = pltpu.get_barrier_semaphore()
        for dev in (*ring, *side_dev, peer):
            pl.semaphore_signal(barrier, inc=1, device_id=dev)
        pl.semaphore_wait(barrier, 5)

    def gu_cut(i):
        return pl.ds(i * gu_rows, gu_rows)

    def d_cut(i):
        return pl.ds(i * d_rows, d_rows)

    def first_gu(way, i):
        for m, w in enumerate((wg_ref, wu_ref)):
            @pl.when(cls == m)
            def _(m=m, w=w):
                remote(w.at[parity, gu_cut(i)], gu_ref.at[way, m, gu_cut(i)],
                       zsend.at[way, 0], zrecv.at[way, 0, 0, i], device_id=ring[way]).start()

    def first_d(way, i):
        remote(wd_ref.at[parity, d_cut(i)], ds_ref.at[way, d_cut(i)],
               zsend.at[way, 1], zrecv.at[way, 0, 1, i], device_id=ring[way]).start()

    def next_gu(way, h, i):
        return remote(gu_ref.at[(h - 1) * 2 + way, cls, gu_cut(i)], gu_ref.at[h * 2 + way, cls, gu_cut(i)],
                      zsend.at[way, 0], zrecv.at[way, h, 0, i], device_id=ring[way])

    def next_d(way, h, i):
        return remote(ds_ref.at[(h - 1) * 2 + way, d_cut(i)], ds_ref.at[h * 2 + way, d_cut(i)],
                      zsend.at[way, 1], zrecv.at[way, h, 1, i], device_id=ring[way])

    def wait_ring(way, h, kind, i):
        there = ds_ref.at[(h - 1) * 2 + way, d_cut(i)] if kind else gu_ref.at[(h - 1) * 2 + way, cls, gu_cut(i)]
        remote(there, there, zsend.at[way, kind], zrecv.at[way, h - 1, kind, i], device_id=ring[way]).wait_recv()

    def far_gu(way, i):
        m = cls if way == 0 else alt
        return remote(gu_ref.at[(last - 1) * 2 + way, m, gu_cut(i)], gu_far.at[m, gu_cut(i)],
                      zsend.at[way, 0], farrecv.at[way, 0], device_id=ring[way])

    half_w = d_model // 2
    d_half = wd_ref.shape[1] // 2

    def cols(c):
        return pl.ds(c * half_w, half_w)

    def next_half(way, c, r):
        part = pl.ds(r * d_half, d_half)
        return remote(ds_ref.at[(last - 2) * 2 + way, part, cols(c)], ds_ref.at[(last - 1) * 2 + way, part, cols(c)],
                      zsend.at[way, 1], zrecv.at[way, last - 1, 1, 2 * c + r], device_id=ring[way])

    def far_half(way, c):
        part = pl.ds(way * d_half, d_half)
        return remote(ds_ref.at[(last - 1) * 2 + way, part, cols(c)], d_far.at[part, cols(c)],
                      zsend.at[way, 1], farrecv.at[way, 1 + c], device_id=ring[way])

    def extra(way):
        return remote(gu_ref.at[(last - 2) * 2 + way, alt, gu_cut(0)], gu_ref.at[(last - 1) * 2 + way, alt, gu_cut(0)],
                      zsend.at[way, 0], xrecv.at[way], device_id=ring[way])

    def transit_out(way, h, i):
        slot = (h - 1) * 2 + way
        return remote(gu_ref.at[slot, cls, gu_cut(i)], tr_ref.at[slot, gu_cut(i)],
                      tsend.at[way, 0], trecv.at[way, h - 1, i], device_id=side_dev[way])

    def transit_on(way, h, i, sem):
        slot = (h - 1) * 2 + way
        m = alt if way == 0 else cls
        return remote(tr_ref.at[slot, gu_cut(i)], gu_ref.at[slot, m, gu_cut(i)],
                      tsend.at[way, 1], sem, device_id=side_dev[1 - way])

    def wait_final(way, h):
        def wait(n):
            there = gu_ref.at[(h - 1) * 2 + way, alt, pl.ds(0, n * gu_rows)]
            remote(there, there, tsend.at[way, 1], frecv.at[way, h - 1], device_id=side_dev[1 - way]).wait_recv()

        pl.when(h < last - 1)(lambda: wait(CHUNKS))
        pl.when(h >= last - 1)(lambda: wait(CHUNKS - 1))


    wave_n = part_n // WAVES

    def near_row(w, k):
        return (CORES + w) * tok_n + k * part_n

    def near(way):
        copies = []
        for w in range(WAVES):
            src = pl.ds(way * part_n + w * wave_n, wave_n)
            dst = pl.ds(pl.multiple_of(core * part_n + way * wave_n, wave_n), wave_n)
            copies += [
                remote(route_ref.at[:, src], route_all.at[CORES + w, :, dst], near_send.at[way, 0], near_recv.at[way, 0], device_id=side_dev[way]),
                remote(gate_ref.at[:, src], gate_all.at[CORES + w, :, dst], near_send.at[way, 1], near_recv.at[way, 1], device_id=side_dev[way]),
                remote(x_ref.at[src], x_all.at[pl.ds(near_row(w, core) + way * wave_n, wave_n)], near_send.at[way, 2], near_recv.at[way, 2], device_id=side_dev[way])]
        return copies

    def wait_near(way):
        part = pl.ds(0, part_n)
        for k, ref in enumerate((route_all.at[CORES, :, part], gate_all.at[CORES, :, part], x_all.at[pl.ds(CORES * tok_n, part_n)])):
            remote(ref, ref, near_send.at[way, k], near_recv.at[way, k], device_id=side_dev[way]).wait()

    for way in range(2):
        for copy in near(way):
            copy.start()
    for i in range(CHUNKS):
        for way in range(2):
            first_gu(way, i)
    for i in range(CHUNKS):
        for way in range(2):
            first_d(way, i)

    def load_own(e):
        for m, w in enumerate((wg_ref, wu_ref)):
            pltpu.make_async_copy(w.at[e], gu_buf.at[e, m], gu_sem.at[e]).start()
        pltpu.make_async_copy(wd_ref.at[e], d_buf.at[e], d_sem.at[e]).start()

    def load_slot(h, e):
        slot = (h - 1) * 2 + e
        pltpu.make_async_copy(gu_ref.at[slot], gu_buf.at[e], gu_sem.at[e]).start()
        pltpu.make_async_copy(ds_ref.at[slot], d_buf.at[e], d_sem.at[e]).start()

    def load_half(e, c):
        slot = (last - 1) * 2 + e
        pltpu.make_async_copy(ds_ref.at[slot, :, cols(c)], d_buf.at[e, :, cols(c)], d_sem.at[e]).start()

    def wait_half(e):
        pltpu.make_async_copy(ds_ref.at[0, :, cols(0)], d_buf.at[e, :, cols(0)], d_sem.at[e]).wait()

    def load_early(e):
        slot = (last - 1) * 2 + e
        pltpu.make_async_copy(gu_ref.at[slot, cls], gu_buf.at[e, cls], gu_sem.at[e]).start()
        load_half(e, 0)

    def load_late(e):
        slot = (last - 1) * 2 + e
        pltpu.make_async_copy(gu_ref.at[slot, alt], gu_buf.at[e, alt], gu_sem.at[e]).start()

    def wait_gu(e):
        pltpu.make_async_copy(gu_ref.at[0], gu_buf.at[e], gu_sem.at[e]).wait()

    def wait_d(e):
        pltpu.make_async_copy(ds_ref.at[0], d_buf.at[e], d_sem.at[e]).wait()

    load_own(0)
    load_own(1)
    tok = ((route_ref, route_all.at[core]), (gate_ref, gate_all.at[core]), (x_ref, x_all.at[pl.ds(core * tok_n, tok_n)]))
    for k, (src, dst) in enumerate(tok):
        remote(src, dst, own_send.at[k], own_recv.at[k], device_id=peer).start()
        pltpu.make_async_copy(src, dst, own_sem.at[k]).start()
    y_acc[...] = jnp.zeros_like(y_acc)
    y_ret[pl.ds(0, LANES), :] = jnp.zeros((LANES, d_model), jnp.float32)
    for k, (src, dst) in enumerate(tok):
        pltpu.make_async_copy(src, dst, own_sem.at[k]).wait()
        remote(src, dst, own_send.at[k], own_recv.at[k], device_id=peer).wait()

    def dense(block):
        route, gate = route_all[block], gate_all[block]
        for e in range(experts):
            y_ret[e:e + 1, pl.ds(0, tok_n)] = jnp.sum(jnp.where(route == e, gate, 0.0), axis=0, keepdims=True)
        for b in range(tok_n // LANES):
            gate_cols[pl.ds(block * tok_n + b * LANES, LANES), :] = y_ret[pl.ds(0, LANES), b * LANES:(b + 1) * LANES].T

    def dense_pair(first):
        def one(c, carry):
            dense(first + c)
            return carry

        lax.fori_loop(0, CORES, one, 0)

    dense_pair(0)

    def forward():
        lanes = pl.ds(pl.multiple_of(core * part_n, part_n), part_n)
        return [remote(ref, ref, fwd_send.at[k], fwd_recv.at[k], device_id=peer) for w in range(WAVES) for k, ref in enumerate((
            route_all.at[CORES + w, :, lanes], gate_all.at[CORES + w, :, lanes], x_all.at[pl.ds(near_row(w, core), part_n)]))]

    def wait_forward():
        for k, ref in enumerate((route_all.at[CORES], gate_all.at[CORES], x_all.at[pl.ds(CORES * tok_n, tok_n)])):
            remote(ref, ref, fwd_send.at[k], fwd_recv.at[k], device_id=peer).wait()

    def expert_id(h, way):
        src = (plane + planes + (2 * way - 1) * h) % planes
        return (src * CORES + core) * 2 + parity

    def front(row0, gu, n=tile, shift=0):
        def piece(t, c):
            part = pl.ds(row0 + t * tile, tile)
            x_tile = x_all[part]
            a = jnp.dot(x_tile, gu[0], preferred_element_type=jnp.float32)
            b = jnp.dot(x_tile, gu[1], preferred_element_type=jnp.float32)
            hidden[pl.ds(row0 + t * tile + shift, tile)] = (jax.nn.silu(a) * b).astype(jnp.bfloat16)
            return c

        lax.fori_loop(0, n // tile, piece, 0)

    def back(row0, d, expert, n=tile, shift=0, at=None):
        at = pl.ds(0, d_model) if at is None else at

        def piece(t, c):
            part = pl.ds(row0 + t * tile, tile)
            out = jnp.dot(hidden[pl.ds(row0 + t * tile + shift, tile)], d(), preferred_element_type=jnp.float32).astype(jnp.bfloat16)
            gates = gate_cols[part]
            lane = lax.broadcasted_iota(jnp.int32, gates.shape, 1)
            gate = jnp.sum(jnp.where(lane == expert, gates, 0.0), axis=1, keepdims=True)
            y_acc[part, at] += jnp.where(gate > 0.0, gate * out.astype(jnp.float32), 0.0)
            return c

        lax.fori_loop(0, n // tile, piece, 0)

    def group(e, phase, block0, blocks, expert, fresh):
        first, count = block0 * per_block, blocks * per_block

        @pl.when(phase == 0)
        def _():
            @pl.when(fresh)
            def _():
                wait_gu(e)

            def one(t, c):
                front(t * tile, gu_buf.at[e])
                return c

            with jax.named_scope("front"):
                lax.fori_loop(first, first + count, one, 0)

        @pl.when(phase == 1)
        def _():
            @pl.when(fresh)
            def _():
                wait_d(e)

            def one(t, c):
                back(t * tile, lambda: d_buf[e], expert)
                return c

            with jax.named_scope("back"):
                lax.fori_loop(first, first + count, one, 0)

    def own_id(e):
        return (plane * CORES + core) * 2 + e

    def load_pair(h):
        for way in range(2):
            with jax.named_scope("wait_final"):
                wait_final(way, h)
            load_slot(h, way)

    def late_piece(i):
        with jax.named_scope("wait_f3"):
            transit_on(1, last, i, f3recv.at[i]).wait_recv()
        far_gu(1, i).start()

    def stage(h, carry):
        def gates_and_ups(i, c):
            for way in range(2):
                with jax.named_scope("wait_z0"):
                    wait_ring(way, h, 0, i)

                @pl.when(h < last)
                def _():
                    next_gu(way, h, i).start()

                if way == 0:
                    @pl.when(h == last)
                    def _():
                        far_gu(0, i).start()

                @pl.when((h < last) | (i > 0))
                def _():
                    transit_out(way, h, i).start()

            @pl.when((h == last) & (i == 1))
            def _():
                for way in range(2):
                    there = gu_ref.at[(last - 2) * 2 + way, alt, gu_cut(0)]
                    with jax.named_scope("wait_f2"):
                        remote(there, there, tsend.at[way, 1], f2recv.at[way], device_id=side_dev[1 - way]).wait_recv()
                    extra(way).start()

            @pl.when((h == 2) & (i == 0))
            def _():
                with jax.named_scope("wait_fwd"):
                    wait_forward()
                dense_pair(CORES)

            @pl.when((h >= 3) | ((h == 1) & (i >= 2)))
            def _():
                mine = h == 1
                group(jnp.where(mine, 0, 1), jnp.where(mine, i - 2, i // 2), jnp.where(mine, 0, 2 * (i % 2)), 2,
                      jnp.where(mine, own_id(0), expert_id(h - 2, 1)), mine | (i % 2 == 0))

            @pl.when((h >= 2) & (i == CHUNKS - 1))
            def _():
                load_pair(h - 1)
            return c

        lax.fori_loop(0, CHUNKS, gates_and_ups, 0)

        def downs(i, c):
            for way in range(2):
                @pl.when(h < last)
                def _():
                    with jax.named_scope("wait_z1"):
                        wait_ring(way, h, 1, i)

                @pl.when((h == last) & (i < 2))
                def _():
                    with jax.named_scope("wait_z2"):
                        next_half(way, 0, i).wait_recv()

                @pl.when(h < last - 1)
                def _():
                    next_d(way, h, i).start()

                @pl.when((h == last - 1) & (i % 2 == 1))
                def _():
                    next_half(way, 0, i // 2).start()

                @pl.when((h == last) & (i == way))
                def _():
                    far_half(way, 0).start()

            @pl.when((h < last) | (i > 0))
            def _():
                for way in range(2):
                    with jax.named_scope("wait_t"):
                        transit_out(way, h, i).wait_recv()
                    single = (h == last - 1) & (i == 0)

                    @pl.when(single)
                    def _():
                        transit_on(way, h, i, f2recv.at[way]).start()

                    @pl.when(((h < last) | (way == 0)) & jnp.logical_not(single))
                    def _():
                        transit_on(way, h, i, frecv.at[way, h - 1]).start()

                    if way == 1:
                        @pl.when(h == last)
                        def _():
                            transit_on(1, h, i, f3recv.at[i]).start()

            @pl.when((h == last) & (i == 2))
            def _():
                with jax.named_scope("wait_x1"):
                    extra(1).wait_recv()
                far_gu(1, 0).start()
                for r in range(2):
                    next_half(0, 1, r).start()

            @pl.when((h == last) & (i == CHUNKS - 1))
            def _():
                late_piece(1)

            @pl.when((h == 1) & (i == 1))
            def _():
                with jax.named_scope("wait_near"):
                    for way in range(2):
                        wait_near(way)
                for copy in forward():
                    copy.start()

            @pl.when((h >= 2) | (i < 2))
            def _():
                mine, end = h == 1, h == last
                second = end & (i == CHUNKS - 1)
                group(jnp.where(mine | second, 1, 0), jnp.where(mine, i, jnp.where(second, 0, i // 2)),
                      jnp.where(mine | (end & (i >= 2)), 0, 2 * (i % 2)), jnp.where(end & (i == 2), 4, 2),
                      jnp.where(mine, own_id(1), expert_id(h - 1, jnp.where(second, 1, 0))), mine | second | (i % 2 == 0))
            return c

        lax.fori_loop(0, CHUNKS, downs, 0)
        return carry

    lax.fori_loop(1, last + 1, stage, 0)

    load_early(0)

    def rest(n, c):
        @pl.when(n < 2)
        def _():
            late_piece(n + 2)

        @pl.when(n == 1)
        def _():
            for r in range(2):
                next_half(1, 1, r).start()

        @pl.when(n == 2)
        def _():
            with jax.named_scope("wait_final"):
                extra(0).wait_recv()
                wait_final(0, last)
            load_late(0)
        group(1, jnp.where(n == 0, 0, 1), jnp.where(n == 1, 0, 2), 2, expert_id(last - 1, 1), n == 1)
        return c

    lax.fori_loop(0, 3, rest, 0)
    load_late(1)
    load_early(1)

    def both(w):
        return (CORES + w) * tok_n

    far_expert = expert_id(last + 1, 0)

    def shift(e):
        return -e * CORES * tok_n

    far_shift = CORES * tok_n

    size = wave_n // BACK

    def to_peer(c, way, w, k):
        off = w * part_n + way * wave_n + k * size
        return remote(y_acc.at[pl.ds(near_row(w, 1 - core) + way * wave_n + k * size, size), cols(c)], b_peer.at[pl.ds(off, size)],
                      bsend, brecv.at[way, w, k], device_id=peer)

    def give_back(c, way, w, k):
        src = near_row(w, core) + way * wave_n + k * size
        return remote(y_acc.at[pl.ds(src, size), cols(c)], y_ret.at[pl.ds(way * part_n + w * wave_n + k * size, size), cols(c)],
                      rsend.at[way], rrecv.at[way, w], device_id=side_dev[way])

    def wave(c, w, carry):
        first = w == 0

        def pair(e, c2):
            if c == 0:
                pl.when(first)(lambda: wait_gu(e))
                with jax.named_scope("near_front"):
                    front(both(w), gu_buf.at[e], tok_n, shift(e))
            pl.when(first)(lambda: wait_half(e))
            with jax.named_scope("near_back"):
                back(both(w), lambda: d_buf[e, :, cols(c)], expert_id(last, e), tok_n, shift(e), cols(c))
            return c2

        lax.fori_loop(0, 2, pair, 0)
        if c == 0:
            @pl.when(first)
            def _():
                with jax.named_scope("wait_far0"):
                    for way in range(2):
                        m = cls if way == 0 else alt
                        remote(gu_far.at[m], gu_far.at[m], zsend.at[way, 0], farrecv.at[way, 0], device_id=ring[way]).wait_recv()
            with jax.named_scope("far_front"):
                front(both(w), gu_far, tok_n, far_shift)

        @pl.when(first)
        def _():
            with jax.named_scope("wait_far1"):
                for way in range(2):
                    far_half(way, c).wait_recv()

        def far_back(k):
            with jax.named_scope("far_back"):
                back(near_row(w, k), lambda: d_far[:, cols(c)], far_expert, part_n, far_shift, cols(c))

        far_back(1 - core)
        for k in range(BACK):
            for way in range(2):
                to_peer(c, way, w, k).start()
        far_back(core)

        def sums(k, c2):
            @pl.when(k < BACK)
            def _():
                for way in range(2):
                    with jax.named_scope("wait_b"):
                        to_peer(c, way, w, k).wait_recv()
                    off = w * part_n + way * wave_n + k * size
                    y_acc[pl.ds(near_row(w, core) + way * wave_n + k * size, size), cols(c)] += b_peer[pl.ds(off, size)]

            @pl.when(k > 0)
            def _():
                for way in range(2):
                    give_back(c, way, w, k - 1).start()
            return c2

        lax.fori_loop(0, BACK + 1, sums, 0)
        return carry

    lax.fori_loop(0, WAVES, functools.partial(wave, 0), 0)
    pl.semaphore_signal(half_sem, inc=1, device_id=peer)
    for r in range(2):
        for way in range(2):
            with jax.named_scope("wait_z3"):
                next_half(way, 1, r).wait_recv()
        far_half(r, 1).start()
    for e in range(2):
        load_half(e, 1)
    pl.semaphore_wait(half_sem, 1)
    lax.fori_loop(0, WAVES, functools.partial(wave, 1), 0)
    with jax.named_scope("wait_bsend"):
        whole = y_acc.at[pl.ds(0, tok_n)]
        remote(whole, whole, bsend, brecv.at[0, 0, 0], device_id=peer).wait_send()
    pl.semaphore_signal(free_sem, inc=1, device_id=peer)

    def own_block(block):
        row0 = block * tok_n

        def one(e, c):
            with jax.named_scope("own"):
                front(row0, gu_buf.at[e], tok_n)
                back(row0, lambda: d_buf[e], expert_id(last, e), tok_n)
            return c

        lax.fori_loop(0, 2, one, 0)
        with jax.named_scope("far_own"):
            front(row0, gu_far, tok_n)
            back(row0, lambda: d_far[...], far_expert, tok_n)

    def part_copy(w):
        return remote(y_acc.at[pl.ds((1 - core) * tok_n + w * part_n, part_n)], y_acc.at[pl.ds(near_row(w, core), part_n)],
                      psend, precv, device_id=peer)

    def own_blocks(n, c):
        own_block(core + (1 - n) * (1 - 2 * core))

        @pl.when(n == 0)
        def _():
            pl.semaphore_wait(free_sem, 1)
            for w in range(WAVES):
                part_copy(w).start()
        return c

    lax.fori_loop(0, CORES, own_blocks, 0)
    with jax.named_scope("wait_part"):
        whole = y_acc.at[pl.ds(0, tok_n)]
        remote(whole, whole, psend, precv, device_id=peer).wait()

    def finish(w, c):
        for way in range(2):
            off = w * wave_n
            part = pl.ds(way * part_n + off, wave_n)
            with jax.named_scope("wait_r"):
                remote(y_ret.at[part], y_ret.at[part], rsend.at[way], rrecv.at[way, w], device_id=side_dev[way]).wait_recv()
            mine = pl.ds(core * tok_n + way * part_n + off, wave_n)
            other = pl.ds(near_row(way, 1 - core) + off, wave_n)
            y_ref[part] = (y_acc[mine] + y_acc[other] + y_ret[part]).astype(y_ref.dtype)
        return c

    lax.fori_loop(0, WAVES, finish, 0)

    with jax.named_scope("drain"):
        for way in range(2):
            whole = gu_ref.at[pl.ds(0, 4), pl.ds(0, 2), pl.ds(0, (4 * last + 5) * gu_rows // 8)]
            remote(whole, whole, zsend.at[way, 0], farrecv.at[way, 0], device_id=ring[way]).wait_send()
            whole = gu_ref.at[pl.ds(0, 2), pl.ds(0, 2), pl.ds(0, (2 * last + 1) * gu_rows // 2)]
            remote(whole, whole, zsend.at[way, 1], farrecv.at[way, 1], device_id=ring[way]).wait_send()
            whole = tr_ref.at[pl.ds(0, 4), pl.ds(0, (4 * last - 1) * gu_rows // 4)]
            for hop in range(2):
                remote(whole, whole, tsend.at[way, hop], frecv.at[way, 0], device_id=side_dev[way]).wait_send()
            whole = y_ret.at[pl.ds(0, part_n)]
            remote(whole, whole, rsend.at[way], rrecv.at[way, 0], device_id=side_dev[way]).wait_send()


def moe(side, planes, x, route, gate, wg, wu, wd):
    tok_n, d_model = x.shape
    d_ff = wg.shape[2]
    last = planes // 2 - 1
    bf = jnp.bfloat16
    f32 = jnp.float32
    any_spec = pl.BlockSpec(memory_space=pl.ANY)
    dma = pltpu.SemaphoreType.DMA
    blocks = 2 * CORES
    rows = blocks * tok_n
    top_k = route.shape[0]
    out = pl.pallas_call(
        functools.partial(kernel, side, planes),
        out_shape=(
            jax.ShapeDtypeStruct((tok_n, d_model), bf),
            jax.ShapeDtypeStruct((2 * last, 2, d_model, d_ff), bf),
            jax.ShapeDtypeStruct((2 * last, d_ff, d_model), bf),
            jax.ShapeDtypeStruct((2 * last, d_model, d_ff), bf),
        ),
        in_specs=[any_spec] * 6,
        out_specs=(pl.BlockSpec(memory_space=pltpu.VMEM),) + (any_spec,) * 3,
        scratch_shapes=[
            pltpu.VMEM((rows, d_model), bf),
            pltpu.VMEM((blocks, top_k, tok_n), jnp.int32),
            pltpu.VMEM((blocks, top_k, tok_n), f32),
            pltpu.VMEM((rows, LANES), f32),
            pltpu.VMEM((rows, d_model), f32),
            pltpu.VMEM((tok_n, d_model // 2), f32),
            pltpu.VMEM((tok_n, d_model), f32),
            pltpu.VMEM((rows + CORES * tok_n, d_ff), bf),
            pltpu.VMEM((2, 2, d_model, d_ff), bf),
            pltpu.VMEM((2, d_ff, d_model), bf),
            pltpu.VMEM((2, d_model, d_ff), bf),
            pltpu.VMEM((d_ff, d_model), bf),
            dma((2, 2)),
            dma((2, last, 2, CHUNKS)),
            dma((2, 2)),
            dma((2, last, CHUNKS)),
            dma((2, last)),
            dma((CHUNKS,)),
            dma((2, 3)),
            dma((2,)),
            dma((2,)),
            dma((2,)),
            dma((2,)),
            dma((3,)),
            dma((3,)),
            dma((3,)),
            dma((2, 3)),
            dma((2, 3)),
            dma((3,)),
            dma((3,)),
            dma(()),
            dma((2, WAVES, BACK)),
            dma((2,)),
            dma((2, WAVES)),
            dma(()),
            dma(()),
            pltpu.SemaphoreType.REGULAR,
            pltpu.SemaphoreType.REGULAR,
        ],
        compiler_params=pltpu.CompilerParams(
            collective_id=0, has_side_effects=True, vmem_limit_bytes=103 * 512 * 1024),
        name="stream_experts",
    )(x, route, gate, wg, wu, wd)
    return out[0]


def solution(mesh):
    planes = mesh.shape["ep"] // CORES
    side = math.isqrt(mesh.shape["dp"])
    row_spec = P(("dp", "ep"))
    expert_spec = P("ep")

    def local_step(tok_loc, route_loc, gate_loc, wg_loc, wu_loc, wd_loc):
        tables = (pltpu.with_memory_space_constraint(table.T, pltpu.HBM) for table in (route_loc, gate_loc))
        return moe(side, planes, tok_loc, *tables, wg_loc, wu_loc, wd_loc)

    return jax.shard_map(local_step, mesh=mesh, in_specs=(row_spec, row_spec, row_spec, expert_spec, expert_spec, expert_spec), out_specs=row_spec, check_vma=False)
```

```python
import functools
import math

import jax
import jax.numpy as jnp
from jax import lax
from jax.experimental import pallas as pl
from jax.experimental.pallas import tpu as pltpu
from jax.sharding import PartitionSpec as P

CORES = 2
CHUNKS = 4
TILE = 512
BACK = 2
WAVES = 2
LANES = 128


def kernel(side, planes, x_ref, route_ref, gate_ref, wg_ref, wu_ref, wd_ref,
           y_ref, gu_ref, ds_ref, tr_ref,
           x_all, route_all, gate_all, gate_cols, y_acc, b_peer, y_ret, hidden,
           gu_buf, d_buf, gu_far, d_far,
           zsend, zrecv, tsend, trecv, frecv, f3recv, farrecv, xrecv, f2recv, gu_sem, d_sem, own_sem, own_send, own_recv,
           near_send, near_recv, fwd_send, fwd_recv, bsend, brecv, rsend, rrecv, psend, precv, half_sem, free_sem):
    last = planes // 2 - 1
    tok_n, d_model = x_ref.shape
    part_n = tok_n // 2
    tile = min(TILE, tok_n // 2)
    per_block = tok_n // tile
    experts = planes * CORES * 2
    col = lax.axis_index("dp")
    pos = lax.axis_index("ep")
    core = pos % CORES
    plane = pos // CORES
    cx, cy = col // side, col % side
    parity = (cx + cy) % 2
    cls = cx % 2
    alt = 1 - cls
    col_x = col + side * (1 - 2 * (cx % 2))
    col_y = col + 1 - 2 * (cy % 2)
    up = (pos + CORES) % (planes * CORES)
    down = (pos + (planes - 1) * CORES) % (planes * CORES)
    peer = {"ep": pos + 1 - 2 * core}
    ring = ({"ep": up}, {"ep": down})
    side_dev = ({"dp": col_x}, {"dp": col_y})
    gu_rows = wg_ref.shape[1] // CHUNKS
    d_rows = wd_ref.shape[1] // CHUNKS
    remote = pltpu.make_async_remote_copy

    with jax.named_scope("entry"):
        barrier = pltpu.get_barrier_semaphore()
        for dev in (*ring, *side_dev, peer):
            pl.semaphore_signal(barrier, inc=1, device_id=dev)
        pl.semaphore_wait(barrier, 5)

    def gu_cut(i):
        return pl.ds(i * gu_rows, gu_rows)

    def d_cut(i):
        return pl.ds(i * d_rows, d_rows)

    def first_gu(way, i):
        for m, w in enumerate((wg_ref, wu_ref)):
            @pl.when(cls == m)
            def _(m=m, w=w):
                remote(w.at[parity, gu_cut(i)], gu_ref.at[way, m, gu_cut(i)],
                       zsend.at[way, 0], zrecv.at[way, 0, 0, i], device_id=ring[way]).start()

    def first_d(way, i):
        remote(wd_ref.at[parity, d_cut(i)], ds_ref.at[way, d_cut(i)],
               zsend.at[way, 1], zrecv.at[way, 0, 1, i], device_id=ring[way]).start()

    def next_gu(way, h, i):
        return remote(gu_ref.at[(h - 1) * 2 + way, cls, gu_cut(i)], gu_ref.at[h * 2 + way, cls, gu_cut(i)],
                      zsend.at[way, 0], zrecv.at[way, h, 0, i], device_id=ring[way])

    def next_d(way, h, i):
        return remote(ds_ref.at[(h - 1) * 2 + way, d_cut(i)], ds_ref.at[h * 2 + way, d_cut(i)],
                      zsend.at[way, 1], zrecv.at[way, h, 1, i], device_id=ring[way])

    def wait_ring(way, h, kind, i):
        there = ds_ref.at[(h - 1) * 2 + way, d_cut(i)] if kind else gu_ref.at[(h - 1) * 2 + way, cls, gu_cut(i)]
        remote(there, there, zsend.at[way, kind], zrecv.at[way, h - 1, kind, i], device_id=ring[way]).wait_recv()

    def far_gu(way, i):
        m = cls if way == 0 else alt
        return remote(gu_ref.at[(last - 1) * 2 + way, m, gu_cut(i)], gu_far.at[m, gu_cut(i)],
                      zsend.at[way, 0], farrecv.at[way, 0], device_id=ring[way])

    half_w = d_model // 2
    d_half = wd_ref.shape[1] // 2

    def cols(c):
        return pl.ds(c * half_w, half_w)

    def next_half(way, c, r):
        part = pl.ds(r * d_half, d_half)
        return remote(ds_ref.at[(last - 2) * 2 + way, part, cols(c)], ds_ref.at[(last - 1) * 2 + way, part, cols(c)],
                      zsend.at[way, 1], zrecv.at[way, last - 1, 1, 2 * c + r], device_id=ring[way])

    def far_half(way, c):
        part = pl.ds(way * d_half, d_half)
        return remote(ds_ref.at[(last - 1) * 2 + way, part, cols(c)], d_far.at[part, cols(c)],
                      zsend.at[way, 1], farrecv.at[way, 1 + c], device_id=ring[way])

    def extra(way):
        return remote(gu_ref.at[(last - 2) * 2 + way, alt, gu_cut(0)], gu_ref.at[(last - 1) * 2 + way, alt, gu_cut(0)],
                      zsend.at[way, 0], xrecv.at[way], device_id=ring[way])

    def transit_out(way, h, i):
        slot = (h - 1) * 2 + way
        return remote(gu_ref.at[slot, cls, gu_cut(i)], tr_ref.at[slot, gu_cut(i)],
                      tsend.at[way, 0], trecv.at[way, h - 1, i], device_id=side_dev[way])

    def transit_on(way, h, i, sem):
        slot = (h - 1) * 2 + way
        m = alt if way == 0 else cls
        return remote(tr_ref.at[slot, gu_cut(i)], gu_ref.at[slot, m, gu_cut(i)],
                      tsend.at[way, 1], sem, device_id=side_dev[1 - way])

    def wait_final(way, h):
        def wait(n):
            there = gu_ref.at[(h - 1) * 2 + way, alt, pl.ds(0, n * gu_rows)]
            remote(there, there, tsend.at[way, 1], frecv.at[way, h - 1], device_id=side_dev[1 - way]).wait_recv()

        pl.when(h < last - 1)(lambda: wait(CHUNKS))
        pl.when(h >= last - 1)(lambda: wait(CHUNKS - 1))


    wave_n = part_n // WAVES

    def near_row(w, k):
        return (CORES + w) * tok_n + k * part_n

    def near(way):
        copies = []
        for w in range(WAVES):
            src = pl.ds(way * part_n + w * wave_n, wave_n)
            dst = pl.ds(pl.multiple_of(core * part_n + way * wave_n, wave_n), wave_n)
            copies += [
                remote(route_ref.at[:, src], route_all.at[CORES + w, :, dst], near_send.at[way, 0], near_recv.at[way, 0], device_id=side_dev[way]),
                remote(gate_ref.at[:, src], gate_all.at[CORES + w, :, dst], near_send.at[way, 1], near_recv.at[way, 1], device_id=side_dev[way]),
                remote(x_ref.at[src], x_all.at[pl.ds(near_row(w, core) + way * wave_n, wave_n)], near_send.at[way, 2], near_recv.at[way, 2], device_id=side_dev[way])]
        return copies

    def wait_near(way):
        part = pl.ds(0, part_n)
        for k, ref in enumerate((route_all.at[CORES, :, part], gate_all.at[CORES, :, part], x_all.at[pl.ds(CORES * tok_n, part_n)])):
            remote(ref, ref, near_send.at[way, k], near_recv.at[way, k], device_id=side_dev[way]).wait()

    for way in range(2):
        for copy in near(way):
            copy.start()
    for i in range(CHUNKS):
        for way in range(2):
            first_gu(way, i)
    for i in range(CHUNKS):
        for way in range(2):
            first_d(way, i)

    def load_own(e):
        for m, w in enumerate((wg_ref, wu_ref)):
            pltpu.make_async_copy(w.at[e], gu_buf.at[e, m], gu_sem.at[e]).start()
        pltpu.make_async_copy(wd_ref.at[e], d_buf.at[e], d_sem.at[e]).start()

    def load_slot(h, e):
        slot = (h - 1) * 2 + e
        pltpu.make_async_copy(gu_ref.at[slot], gu_buf.at[e], gu_sem.at[e]).start()
        pltpu.make_async_copy(ds_ref.at[slot], d_buf.at[e], d_sem.at[e]).start()

    def load_half(e, c):
        slot = (last - 1) * 2 + e
        pltpu.make_async_copy(ds_ref.at[slot, :, cols(c)], d_buf.at[e, :, cols(c)], d_sem.at[e]).start()

    def wait_half(e):
        pltpu.make_async_copy(ds_ref.at[0, :, cols(0)], d_buf.at[e, :, cols(0)], d_sem.at[e]).wait()

    def load_early(e):
        slot = (last - 1) * 2 + e
        pltpu.make_async_copy(gu_ref.at[slot, cls], gu_buf.at[e, cls], gu_sem.at[e]).start()
        load_half(e, 0)

    def load_late(e):
        slot = (last - 1) * 2 + e
        pltpu.make_async_copy(gu_ref.at[slot, alt], gu_buf.at[e, alt], gu_sem.at[e]).start()

    def wait_gu(e):
        pltpu.make_async_copy(gu_ref.at[0], gu_buf.at[e], gu_sem.at[e]).wait()

    def wait_d(e):
        pltpu.make_async_copy(ds_ref.at[0], d_buf.at[e], d_sem.at[e]).wait()

    load_own(0)
    load_own(1)
    tok = ((route_ref, route_all.at[core]), (gate_ref, gate_all.at[core]), (x_ref, x_all.at[pl.ds(core * tok_n, tok_n)]))
    for k, (src, dst) in enumerate(tok):
        remote(src, dst, own_send.at[k], own_recv.at[k], device_id=peer).start()
        pltpu.make_async_copy(src, dst, own_sem.at[k]).start()
    y_acc[...] = jnp.zeros_like(y_acc)
    y_ret[pl.ds(0, LANES), :] = jnp.zeros((LANES, d_model), jnp.float32)
    for k, (src, dst) in enumerate(tok):
        pltpu.make_async_copy(src, dst, own_sem.at[k]).wait()
        remote(src, dst, own_send.at[k], own_recv.at[k], device_id=peer).wait()

    def dense(block):
        route, gate = route_all[block], gate_all[block]
        for e in range(experts):
            y_ret[e:e + 1, pl.ds(0, tok_n)] = jnp.sum(jnp.where(route == e, gate, 0.0), axis=0, keepdims=True)
        for b in range(tok_n // LANES):
            gate_cols[pl.ds(block * tok_n + b * LANES, LANES), :] = y_ret[pl.ds(0, LANES), b * LANES:(b + 1) * LANES].T

    def dense_pair(first):
        def one(c, carry):
            dense(first + c)
            return carry

        lax.fori_loop(0, CORES, one, 0)

    dense_pair(0)

    def forward():
        lanes = pl.ds(pl.multiple_of(core * part_n, part_n), part_n)
        return [remote(ref, ref, fwd_send.at[k], fwd_recv.at[k], device_id=peer) for w in range(WAVES) for k, ref in enumerate((
            route_all.at[CORES + w, :, lanes], gate_all.at[CORES + w, :, lanes], x_all.at[pl.ds(near_row(w, core), part_n)]))]

    def wait_forward():
        for k, ref in enumerate((route_all.at[CORES], gate_all.at[CORES], x_all.at[pl.ds(CORES * tok_n, tok_n)])):
            remote(ref, ref, fwd_send.at[k], fwd_recv.at[k], device_id=peer).wait()

    def expert_id(h, way):
        src = (plane + planes + (2 * way - 1) * h) % planes
        return (src * CORES + core) * 2 + parity

    def front(row0, gu, n=tile, shift=0):
        def piece(t, c):
            part = pl.ds(row0 + t * tile, tile)
            x_tile = x_all[part]
            a = jnp.dot(x_tile, gu[0], preferred_element_type=jnp.float32)
            b = jnp.dot(x_tile, gu[1], preferred_element_type=jnp.float32)
            hidden[pl.ds(row0 + t * tile + shift, tile)] = (jax.nn.silu(a) * b).astype(jnp.bfloat16)
            return c

        lax.fori_loop(0, n // tile, piece, 0)

    def back(row0, d, expert, n=tile, shift=0, at=None):
        at = pl.ds(0, d_model) if at is None else at

        def piece(t, c):
            part = pl.ds(row0 + t * tile, tile)
            out = jnp.dot(hidden[pl.ds(row0 + t * tile + shift, tile)], d(), preferred_element_type=jnp.float32).astype(jnp.bfloat16)
            gates = gate_cols[part]
            lane = lax.broadcasted_iota(jnp.int32, gates.shape, 1)
            gate = jnp.sum(jnp.where(lane == expert, gates, 0.0), axis=1, keepdims=True)
            y_acc[part, at] += jnp.where(gate > 0.0, gate * out.astype(jnp.float32), 0.0)
            return c

        lax.fori_loop(0, n // tile, piece, 0)

    def group(e, phase, block0, blocks, expert, fresh):
        first, count = block0 * per_block, blocks * per_block

        @pl.when(phase == 0)
        def _():
            @pl.when(fresh)
            def _():
                wait_gu(e)

            def one(t, c):
                front(t * tile, gu_buf.at[e])
                return c

            with jax.named_scope("front"):
                lax.fori_loop(first, first + count, one, 0)

        @pl.when(phase == 1)
        def _():
            @pl.when(fresh)
            def _():
                wait_d(e)

            def one(t, c):
                back(t * tile, lambda: d_buf[e], expert)
                return c

            with jax.named_scope("back"):
                lax.fori_loop(first, first + count, one, 0)

    def own_id(e):
        return (plane * CORES + core) * 2 + e

    def load_pair(h):
        for way in range(2):
            with jax.named_scope("wait_final"):
                wait_final(way, h)
            load_slot(h, way)

    def late_piece(i):
        with jax.named_scope("wait_f3"):
            transit_on(1, last, i, f3recv.at[i]).wait_recv()
        far_gu(1, i).start()

    def stage(h, carry):
        def gates_and_ups(i, c):
            for way in range(2):
                with jax.named_scope("wait_z0"):
                    wait_ring(way, h, 0, i)

                @pl.when(h < last)
                def _():
                    next_gu(way, h, i).start()

                if way == 0:
                    @pl.when(h == last)
                    def _():
                        far_gu(0, i).start()

                @pl.when((h < last) | (i > 0))
                def _():
                    transit_out(way, h, i).start()

            @pl.when((h == last) & (i == 1))
            def _():
                for way in range(2):
                    there = gu_ref.at[(last - 2) * 2 + way, alt, gu_cut(0)]
                    with jax.named_scope("wait_f2"):
                        remote(there, there, tsend.at[way, 1], f2recv.at[way], device_id=side_dev[1 - way]).wait_recv()
                    extra(way).start()

            @pl.when((h == 2) & (i == 0))
            def _():
                with jax.named_scope("wait_fwd"):
                    wait_forward()
                dense_pair(CORES)

            @pl.when((h >= 3) | ((h == 1) & (i >= 2)))
            def _():
                mine = h == 1
                group(jnp.where(mine, 0, 1), jnp.where(mine, i - 2, i // 2), jnp.where(mine, 0, 2 * (i % 2)), 2,
                      jnp.where(mine, own_id(0), expert_id(h - 2, 1)), mine | (i % 2 == 0))

            @pl.when((h >= 2) & (i == CHUNKS - 1))
            def _():
                load_pair(h - 1)
            return c

        lax.fori_loop(0, CHUNKS, gates_and_ups, 0)

        def downs(i, c):
            for way in range(2):
                @pl.when(h < last)
                def _():
                    with jax.named_scope("wait_z1"):
                        wait_ring(way, h, 1, i)

                @pl.when((h == last) & (i < 2))
                def _():
                    with jax.named_scope("wait_z2"):
                        next_half(way, 0, i).wait_recv()

                @pl.when(h < last - 1)
                def _():
                    next_d(way, h, i).start()

                @pl.when((h == last - 1) & (i % 2 == 1))
                def _():
                    next_half(way, 0, i // 2).start()

                @pl.when((h == last) & (i == way))
                def _():
                    far_half(way, 0).start()

            @pl.when((h < last) | (i > 0))
            def _():
                for way in range(2):
                    with jax.named_scope("wait_t"):
                        transit_out(way, h, i).wait_recv()
                    single = (h == last - 1) & (i == 0)

                    @pl.when(single)
                    def _():
                        transit_on(way, h, i, f2recv.at[way]).start()

                    @pl.when(((h < last) | (way == 0)) & jnp.logical_not(single))
                    def _():
                        transit_on(way, h, i, frecv.at[way, h - 1]).start()

                    if way == 1:
                        @pl.when(h == last)
                        def _():
                            transit_on(1, h, i, f3recv.at[i]).start()

            @pl.when((h == last) & (i == 2))
            def _():
                with jax.named_scope("wait_x1"):
                    extra(1).wait_recv()
                far_gu(1, 0).start()
                for r in range(2):
                    next_half(0, 1, r).start()

            @pl.when((h == last) & (i == CHUNKS - 1))
            def _():
                late_piece(1)

            @pl.when((h == 1) & (i == 1))
            def _():
                with jax.named_scope("wait_near"):
                    for way in range(2):
                        wait_near(way)
                for copy in forward():
                    copy.start()

            @pl.when((h >= 2) | (i < 2))
            def _():
                mine, end = h == 1, h == last
                second = end & (i == CHUNKS - 1)
                group(jnp.where(mine | second, 1, 0), jnp.where(mine, i, jnp.where(second, 0, i // 2)),
                      jnp.where(mine | (end & (i >= 2)), 0, 2 * (i % 2)), jnp.where(end & (i == 2), 4, 2),
                      jnp.where(mine, own_id(1), expert_id(h - 1, jnp.where(second, 1, 0))), mine | second | (i % 2 == 0))
            return c

        lax.fori_loop(0, CHUNKS, downs, 0)
        return carry

    lax.fori_loop(1, last + 1, stage, 0)

    load_early(0)

    def rest(n, c):
        @pl.when(n < 2)
        def _():
            late_piece(n + 2)

        @pl.when(n == 1)
        def _():
            for r in range(2):
                next_half(1, 1, r).start()

        @pl.when(n == 2)
        def _():
            with jax.named_scope("wait_final"):
                extra(0).wait_recv()
                wait_final(0, last)
            load_late(0)
        group(1, jnp.where(n == 0, 0, 1), jnp.where(n == 1, 0, 2), 2, expert_id(last - 1, 1), n == 1)
        return c

    lax.fori_loop(0, 3, rest, 0)
    load_late(1)
    load_early(1)

    def both(w):
        return (CORES + w) * tok_n

    far_expert = expert_id(last + 1, 0)

    def shift(e):
        return -e * CORES * tok_n

    far_shift = CORES * tok_n

    size = wave_n // BACK

    def to_peer(c, way, w, k):
        off = w * part_n + way * wave_n + k * size
        return remote(y_acc.at[pl.ds(near_row(w, 1 - core) + way * wave_n + k * size, size), cols(c)], b_peer.at[pl.ds(off, size)],
                      bsend, brecv.at[way, w, k], device_id=peer)

    def give_back(c, way, w, k):
        src = near_row(w, core) + way * wave_n + k * size
        return remote(y_acc.at[pl.ds(src, size), cols(c)], y_ret.at[pl.ds(way * part_n + w * wave_n + k * size, size), cols(c)],
                      rsend.at[way], rrecv.at[way, w], device_id=side_dev[way])

    def right_half(r):
        for way in range(2):
            with jax.named_scope("wait_z3"):
                next_half(way, 1, r).wait_recv()
        far_half(r, 1).start()

    def own_expert(block, e):
        row0 = block * tok_n
        with jax.named_scope("own"):
            front(row0, gu_buf.at[e], tok_n)
            back(row0, lambda: d_buf[e], expert_id(last, e), tok_n)

    def near_back(c, w, e):
        pl.when(w == 0)(lambda: wait_half(e))
        with jax.named_scope("near_back"):
            back(both(w), lambda: d_buf[e, :, cols(c)], expert_id(last, e), tok_n, shift(e), cols(c))

    def right_pair(w):
        def one(e, carry):
            near_back(1, w, e)
            return carry

        lax.fori_loop(0, 2, one, 0)

    def wave(c, w, carry):
        first = w == 0
        if c == 0:
            pl.when(w == 1)(lambda: right_half(0))

        if c == 0:
            def pair(e, c2):
                pl.when(first)(lambda: wait_gu(e))
                with jax.named_scope("near_front"):
                    front(both(w), gu_buf.at[e], tok_n, shift(e))
                near_back(0, w, e)
                return c2

            lax.fori_loop(0, 2, pair, 0)
        else:
            pl.when(w == 1)(lambda: right_pair(1))
        if c == 0:
            @pl.when(first)
            def _():
                with jax.named_scope("wait_far0"):
                    for way in range(2):
                        m = cls if way == 0 else alt
                        remote(gu_far.at[m], gu_far.at[m], zsend.at[way, 0], farrecv.at[way, 0], device_id=ring[way]).wait_recv()
            @pl.when(w == 1)
            def _():
                right_half(1)
                for e in range(2):
                    load_half(e, 1)
            with jax.named_scope("far_front"):
                front(both(w), gu_far, tok_n, far_shift)

        @pl.when(first)
        def _():
            with jax.named_scope("wait_far1"):
                for way in range(2):
                    far_half(way, c).wait_recv()

        def far_back(k):
            with jax.named_scope("far_back"):
                back(near_row(w, k), lambda: d_far[:, cols(c)], far_expert, part_n, far_shift, cols(c))

        far_back(1 - core)
        for k in range(BACK):
            for way in range(2):
                to_peer(c, way, w, k).start()
        far_back(core)
        if c == 0:
            pl.when(w == 1)(lambda: right_pair(0))
        if c == 1:
            pl.when(w == 1)(lambda: own_expert(1 - core, 0))

        def sums(k, c2):
            @pl.when(k < BACK)
            def _():
                for way in range(2):
                    with jax.named_scope("wait_b"):
                        to_peer(c, way, w, k).wait_recv()
                    off = w * part_n + way * wave_n + k * size
                    y_acc[pl.ds(near_row(w, core) + way * wave_n + k * size, size), cols(c)] += b_peer[pl.ds(off, size)]

            @pl.when(k > 0)
            def _():
                for way in range(2):
                    give_back(c, way, w, k - 1).start()
            return c2

        lax.fori_loop(0, BACK + 1, sums, 0)
        return carry

    lax.fori_loop(0, WAVES, functools.partial(wave, 0), 0)
    pl.semaphore_signal(half_sem, inc=1, device_id=peer)
    pl.semaphore_wait(half_sem, 1)
    lax.fori_loop(0, WAVES, functools.partial(wave, 1), 0)
    with jax.named_scope("wait_bsend"):
        whole = y_acc.at[pl.ds(0, tok_n)]
        remote(whole, whole, bsend, brecv.at[0, 0, 0], device_id=peer).wait_send()
    pl.semaphore_signal(free_sem, inc=1, device_id=peer)

    def own_block(block, first):
        def one(e, c):
            own_expert(block, e)
            return c

        lax.fori_loop(first, 2, one, 0)
        with jax.named_scope("far_own"):
            front(block * tok_n, gu_far, tok_n)
            back(block * tok_n, lambda: d_far[...], far_expert, tok_n)

    def part_copy(w):
        return remote(y_acc.at[pl.ds((1 - core) * tok_n + w * part_n, part_n)], y_acc.at[pl.ds(near_row(w, core), part_n)],
                      psend, precv, device_id=peer)

    def own_blocks(n, c):
        own_block(core + (1 - n) * (1 - 2 * core), 1 - n)

        @pl.when(n == 0)
        def _():
            pl.semaphore_wait(free_sem, 1)
            for w in range(WAVES):
                part_copy(w).start()
        return c

    lax.fori_loop(0, CORES, own_blocks, 0)
    with jax.named_scope("wait_part"):
        whole = y_acc.at[pl.ds(0, tok_n)]
        remote(whole, whole, psend, precv, device_id=peer).wait()

    def finish(w, c):
        for way in range(2):
            off = w * wave_n
            part = pl.ds(way * part_n + off, wave_n)
            with jax.named_scope("wait_r"):
                remote(y_ret.at[part], y_ret.at[part], rsend.at[way], rrecv.at[way, w], device_id=side_dev[way]).wait_recv()
            mine = pl.ds(core * tok_n + way * part_n + off, wave_n)
            other = pl.ds(near_row(way, 1 - core) + off, wave_n)
            y_ref[part] = (y_acc[mine] + y_acc[other] + y_ret[part]).astype(y_ref.dtype)
        return c

    lax.fori_loop(0, WAVES, finish, 0)

    with jax.named_scope("drain"):
        for way in range(2):
            whole = gu_ref.at[pl.ds(0, 4), pl.ds(0, 2), pl.ds(0, (4 * last + 5) * gu_rows // 8)]
            remote(whole, whole, zsend.at[way, 0], farrecv.at[way, 0], device_id=ring[way]).wait_send()
            whole = gu_ref.at[pl.ds(0, 2), pl.ds(0, 2), pl.ds(0, (2 * last + 1) * gu_rows // 2)]
            remote(whole, whole, zsend.at[way, 1], farrecv.at[way, 1], device_id=ring[way]).wait_send()
            whole = tr_ref.at[pl.ds(0, 4), pl.ds(0, (4 * last - 1) * gu_rows // 4)]
            for hop in range(2):
                remote(whole, whole, tsend.at[way, hop], frecv.at[way, 0], device_id=side_dev[way]).wait_send()
            whole = y_ret.at[pl.ds(0, part_n)]
            remote(whole, whole, rsend.at[way], rrecv.at[way, 0], device_id=side_dev[way]).wait_send()


def moe(side, planes, x, route, gate, wg, wu, wd):
    tok_n, d_model = x.shape
    d_ff = wg.shape[2]
    last = planes // 2 - 1
    bf = jnp.bfloat16
    f32 = jnp.float32
    any_spec = pl.BlockSpec(memory_space=pl.ANY)
    dma = pltpu.SemaphoreType.DMA
    blocks = 2 * CORES
    rows = blocks * tok_n
    top_k = route.shape[0]
    out = pl.pallas_call(
        functools.partial(kernel, side, planes),
        out_shape=(
            jax.ShapeDtypeStruct((tok_n, d_model), bf),
            jax.ShapeDtypeStruct((2 * last, 2, d_model, d_ff), bf),
            jax.ShapeDtypeStruct((2 * last, d_ff, d_model), bf),
            jax.ShapeDtypeStruct((2 * last, d_model, d_ff), bf),
        ),
        in_specs=[any_spec] * 6,
        out_specs=(pl.BlockSpec(memory_space=pltpu.VMEM),) + (any_spec,) * 3,
        scratch_shapes=[
            pltpu.VMEM((rows, d_model), bf),
            pltpu.VMEM((blocks, top_k, tok_n), jnp.int32),
            pltpu.VMEM((blocks, top_k, tok_n), f32),
            pltpu.VMEM((rows, LANES), f32),
            pltpu.VMEM((rows, d_model), f32),
            pltpu.VMEM((tok_n, d_model // 2), f32),
            pltpu.VMEM((tok_n, d_model), f32),
            pltpu.VMEM((rows + CORES * tok_n, d_ff), bf),
            pltpu.VMEM((2, 2, d_model, d_ff), bf),
            pltpu.VMEM((2, d_ff, d_model), bf),
            pltpu.VMEM((2, d_model, d_ff), bf),
            pltpu.VMEM((d_ff, d_model), bf),
            dma((2, 2)),
            dma((2, last, 2, CHUNKS)),
            dma((2, 2)),
            dma((2, last, CHUNKS)),
            dma((2, last)),
            dma((CHUNKS,)),
            dma((2, 3)),
            dma((2,)),
            dma((2,)),
            dma((2,)),
            dma((2,)),
            dma((3,)),
            dma((3,)),
            dma((3,)),
            dma((2, 3)),
            dma((2, 3)),
            dma((3,)),
            dma((3,)),
            dma(()),
            dma((2, WAVES, BACK)),
            dma((2,)),
            dma((2, WAVES)),
            dma(()),
            dma(()),
            pltpu.SemaphoreType.REGULAR,
            pltpu.SemaphoreType.REGULAR,
        ],
        compiler_params=pltpu.CompilerParams(
            collective_id=0, has_side_effects=True, vmem_limit_bytes=103 * 512 * 1024),
        name="stream_experts",
    )(x, route, gate, wg, wu, wd)
    return out[0]


def solution(mesh):
    planes = mesh.shape["ep"] // CORES
    side = math.isqrt(mesh.shape["dp"])
    row_spec = P(("dp", "ep"))
    expert_spec = P("ep")

    def local_step(tok_loc, route_loc, gate_loc, wg_loc, wu_loc, wd_loc):
        tables = (pltpu.with_memory_space_constraint(table.T, pltpu.HBM) for table in (route_loc, gate_loc))
        return moe(side, planes, tok_loc, *tables, wg_loc, wu_loc, wd_loc)

    return jax.shard_map(local_step, mesh=mesh, in_specs=(row_spec, row_spec, row_spec, expert_spec, expert_spec, expert_spec), out_specs=row_spec, check_vma=False)
```

```python
import functools
import math

import jax
import jax.numpy as jnp
from jax import lax
from jax.experimental import pallas as pl
from jax.experimental.pallas import tpu as pltpu
from jax.sharding import PartitionSpec as P

CORES = 2
CHUNKS = 4
TILE = 512
BACK = 2
WAVES = 2
LANES = 128


def kernel(side, planes, x_ref, route_ref, gate_ref, wg_ref, wu_ref, wd_ref,
           y_ref, gu_ref, ds_ref, tr_ref,
           x_all, route_all, gate_all, gate_cols, y_acc, b_peer, y_ret, hidden,
           gu_buf, d_buf, gu_far, d_far,
           zsend, zrecv, tsend, trecv, frecv, f3recv, farrecv, xrecv, f2recv, gu_sem, d_sem, own_sem, own_send, own_recv,
           near_send, near_recv, fwd_send, fwd_recv, bsend, brecv, rsend, rrecv, psend, precv, half_sem, free_sem):
    last = planes // 2 - 1
    tok_n, d_model = x_ref.shape
    part_n = tok_n // 2
    tile = min(TILE, tok_n // 2)
    per_block = tok_n // tile
    experts = planes * CORES * 2
    col = lax.axis_index("dp")
    pos = lax.axis_index("ep")
    core = pos % CORES
    plane = pos // CORES
    cx, cy = col // side, col % side
    parity = (cx + cy) % 2
    cls = cx % 2
    alt = 1 - cls
    col_x = col + side * (1 - 2 * (cx % 2))
    col_y = col + 1 - 2 * (cy % 2)
    up = (pos + CORES) % (planes * CORES)
    down = (pos + (planes - 1) * CORES) % (planes * CORES)
    peer = {"ep": pos + 1 - 2 * core}
    ring = ({"ep": up}, {"ep": down})
    side_dev = ({"dp": col_x}, {"dp": col_y})
    gu_rows = wg_ref.shape[1] // CHUNKS
    d_rows = wd_ref.shape[1] // CHUNKS
    remote = pltpu.make_async_remote_copy

    with jax.named_scope("entry"):
        barrier = pltpu.get_barrier_semaphore()
        for dev in (*ring, *side_dev, peer):
            pl.semaphore_signal(barrier, inc=1, device_id=dev)
        pl.semaphore_wait(barrier, 5)

    def gu_cut(i):
        return pl.ds(i * gu_rows, gu_rows)

    def d_cut(i):
        return pl.ds(i * d_rows, d_rows)

    def first_gu(way, i):
        for m, w in enumerate((wg_ref, wu_ref)):
            @pl.when(cls == m)
            def _(m=m, w=w):
                remote(w.at[parity, gu_cut(i)], gu_ref.at[way, m, gu_cut(i)],
                       zsend.at[way, 0], zrecv.at[way, 0, 0, i], device_id=ring[way]).start()

    def first_d(way, i):
        remote(wd_ref.at[parity, d_cut(i)], ds_ref.at[way, d_cut(i)],
               zsend.at[way, 1], zrecv.at[way, 0, 1, i], device_id=ring[way]).start()

    def next_gu(way, h, i):
        return remote(gu_ref.at[(h - 1) * 2 + way, cls, gu_cut(i)], gu_ref.at[h * 2 + way, cls, gu_cut(i)],
                      zsend.at[way, 0], zrecv.at[way, h, 0, i], device_id=ring[way])

    def next_d(way, h, i):
        return remote(ds_ref.at[(h - 1) * 2 + way, d_cut(i)], ds_ref.at[h * 2 + way, d_cut(i)],
                      zsend.at[way, 1], zrecv.at[way, h, 1, i], device_id=ring[way])

    def wait_ring(way, h, kind, i):
        there = ds_ref.at[(h - 1) * 2 + way, d_cut(i)] if kind else gu_ref.at[(h - 1) * 2 + way, cls, gu_cut(i)]
        remote(there, there, zsend.at[way, kind], zrecv.at[way, h - 1, kind, i], device_id=ring[way]).wait_recv()

    def far_gu(way, i):
        m = cls if way == 0 else alt
        return remote(gu_ref.at[(last - 1) * 2 + way, m, gu_cut(i)], gu_far.at[m, gu_cut(i)],
                      zsend.at[way, 0], farrecv.at[way, 0], device_id=ring[way])

    half_w = d_model // 2
    d_half = wd_ref.shape[1] // 2

    def cols(c):
        return pl.ds(c * half_w, half_w)

    def next_half(way, c, r):
        part = pl.ds(r * d_half, d_half)
        return remote(ds_ref.at[(last - 2) * 2 + way, part, cols(c)], ds_ref.at[(last - 1) * 2 + way, part, cols(c)],
                      zsend.at[way, 1], zrecv.at[way, last - 1, 1, 2 * c + r], device_id=ring[way])

    def far_half(way, c):
        part = pl.ds(way * d_half, d_half)
        return remote(ds_ref.at[(last - 1) * 2 + way, part, cols(c)], d_far.at[part, cols(c)],
                      zsend.at[way, 1], farrecv.at[way, 1 + c], device_id=ring[way])

    def extra(way):
        return remote(gu_ref.at[(last - 2) * 2 + way, alt, gu_cut(0)], gu_ref.at[(last - 1) * 2 + way, alt, gu_cut(0)],
                      zsend.at[way, 0], xrecv.at[way], device_id=ring[way])

    def transit_out(way, h, i):
        slot = (h - 1) * 2 + way
        return remote(gu_ref.at[slot, cls, gu_cut(i)], tr_ref.at[slot, gu_cut(i)],
                      tsend.at[way, 0], trecv.at[way, h - 1, i], device_id=side_dev[way])

    def transit_on(way, h, i, sem):
        slot = (h - 1) * 2 + way
        m = alt if way == 0 else cls
        return remote(tr_ref.at[slot, gu_cut(i)], gu_ref.at[slot, m, gu_cut(i)],
                      tsend.at[way, 1], sem, device_id=side_dev[1 - way])

    def wait_final(way, h):
        def wait(n):
            there = gu_ref.at[(h - 1) * 2 + way, alt, pl.ds(0, n * gu_rows)]
            remote(there, there, tsend.at[way, 1], frecv.at[way, h - 1], device_id=side_dev[1 - way]).wait_recv()

        pl.when(h < last - 1)(lambda: wait(CHUNKS))
        pl.when(h >= last - 1)(lambda: wait(CHUNKS - 1))


    wave_n = part_n // WAVES

    def near_row(w, k):
        return (CORES + w) * tok_n + k * part_n

    def near(way):
        copies = []
        for w in range(WAVES):
            src = pl.ds(way * part_n + w * wave_n, wave_n)
            dst = pl.ds(pl.multiple_of(core * part_n + way * wave_n, wave_n), wave_n)
            copies += [
                remote(route_ref.at[:, src], route_all.at[CORES + w, :, dst], near_send.at[way, 0], near_recv.at[way, 0], device_id=side_dev[way]),
                remote(gate_ref.at[:, src], gate_all.at[CORES + w, :, dst], near_send.at[way, 1], near_recv.at[way, 1], device_id=side_dev[way]),
                remote(x_ref.at[src], x_all.at[pl.ds(near_row(w, core) + way * wave_n, wave_n)], near_send.at[way, 2], near_recv.at[way, 2], device_id=side_dev[way])]
        return copies

    def wait_near(way):
        part = pl.ds(0, part_n)
        for k, ref in enumerate((route_all.at[CORES, :, part], gate_all.at[CORES, :, part], x_all.at[pl.ds(CORES * tok_n, part_n)])):
            remote(ref, ref, near_send.at[way, k], near_recv.at[way, k], device_id=side_dev[way]).wait()

    for way in range(2):
        for copy in near(way):
            copy.start()
    for i in range(CHUNKS):
        for way in range(2):
            first_gu(way, i)
    for i in range(CHUNKS):
        for way in range(2):
            first_d(way, i)

    def load_own(e):
        for m, w in enumerate((wg_ref, wu_ref)):
            pltpu.make_async_copy(w.at[e], gu_buf.at[e, m], gu_sem.at[e]).start()
        pltpu.make_async_copy(wd_ref.at[e], d_buf.at[e], d_sem.at[e]).start()

    def load_slot(h, e):
        slot = (h - 1) * 2 + e
        pltpu.make_async_copy(gu_ref.at[slot], gu_buf.at[e], gu_sem.at[e]).start()
        pltpu.make_async_copy(ds_ref.at[slot], d_buf.at[e], d_sem.at[e]).start()

    def load_half(e, c):
        slot = (last - 1) * 2 + e
        pltpu.make_async_copy(ds_ref.at[slot, :, cols(c)], d_buf.at[e, :, cols(c)], d_sem.at[e]).start()

    def wait_half(e):
        pltpu.make_async_copy(ds_ref.at[0, :, cols(0)], d_buf.at[e, :, cols(0)], d_sem.at[e]).wait()

    def load_early(e):
        slot = (last - 1) * 2 + e
        pltpu.make_async_copy(gu_ref.at[slot, cls], gu_buf.at[e, cls], gu_sem.at[e]).start()
        load_half(e, 0)

    def load_late(e):
        slot = (last - 1) * 2 + e
        pltpu.make_async_copy(gu_ref.at[slot, alt], gu_buf.at[e, alt], gu_sem.at[e]).start()

    def wait_gu(e):
        pltpu.make_async_copy(gu_ref.at[0], gu_buf.at[e], gu_sem.at[e]).wait()

    def wait_d(e):
        pltpu.make_async_copy(ds_ref.at[0], d_buf.at[e], d_sem.at[e]).wait()

    load_own(0)
    load_own(1)
    tok = ((route_ref, route_all.at[core]), (gate_ref, gate_all.at[core]), (x_ref, x_all.at[pl.ds(core * tok_n, tok_n)]))
    for k, (src, dst) in enumerate(tok):
        remote(src, dst, own_send.at[k], own_recv.at[k], device_id=peer).start()
        pltpu.make_async_copy(src, dst, own_sem.at[k]).start()
    y_acc[...] = jnp.zeros_like(y_acc)
    y_ret[pl.ds(0, LANES), :] = jnp.zeros((LANES, d_model), jnp.float32)
    for k, (src, dst) in enumerate(tok):
        pltpu.make_async_copy(src, dst, own_sem.at[k]).wait()
        remote(src, dst, own_send.at[k], own_recv.at[k], device_id=peer).wait()

    def dense(block):
        route, gate = route_all[block], gate_all[block]
        for e in range(experts):
            y_ret[e:e + 1, pl.ds(0, tok_n)] = jnp.sum(jnp.where(route == e, gate, 0.0), axis=0, keepdims=True)
        for b in range(tok_n // LANES):
            gate_cols[pl.ds(block * tok_n + b * LANES, LANES), :] = y_ret[pl.ds(0, LANES), b * LANES:(b + 1) * LANES].T

    def dense_pair(first):
        def one(c, carry):
            dense(first + c)
            return carry

        lax.fori_loop(0, CORES, one, 0)

    dense_pair(0)

    def forward():
        lanes = pl.ds(pl.multiple_of(core * part_n, part_n), part_n)
        return [remote(ref, ref, fwd_send.at[k], fwd_recv.at[k], device_id=peer) for w in range(WAVES) for k, ref in enumerate((
            route_all.at[CORES + w, :, lanes], gate_all.at[CORES + w, :, lanes], x_all.at[pl.ds(near_row(w, core), part_n)]))]

    def wait_forward():
        for k, ref in enumerate((route_all.at[CORES], gate_all.at[CORES], x_all.at[pl.ds(CORES * tok_n, tok_n)])):
            remote(ref, ref, fwd_send.at[k], fwd_recv.at[k], device_id=peer).wait()

    def expert_id(h, way):
        src = (plane + planes + (2 * way - 1) * h) % planes
        return (src * CORES + core) * 2 + parity

    def front(row0, gu, n=tile, shift=0):
        def piece(t, c):
            part = pl.ds(row0 + t * tile, tile)
            x_tile = x_all[part]
            a = jnp.dot(x_tile, gu[0], preferred_element_type=jnp.float32)
            b = jnp.dot(x_tile, gu[1], preferred_element_type=jnp.float32)
            hidden[pl.ds(row0 + t * tile + shift, tile)] = (jax.nn.silu(a) * b).astype(jnp.bfloat16)
            return c

        lax.fori_loop(0, n // tile, piece, 0)

    def back(row0, d, expert, n=tile, shift=0, at=None):
        at = pl.ds(0, d_model) if at is None else at

        def piece(t, c):
            part = pl.ds(row0 + t * tile, tile)
            out = jnp.dot(hidden[pl.ds(row0 + t * tile + shift, tile)], d(), preferred_element_type=jnp.float32).astype(jnp.bfloat16)
            gates = gate_cols[part]
            lane = lax.broadcasted_iota(jnp.int32, gates.shape, 1)
            gate = jnp.sum(jnp.where(lane == expert, gates, 0.0), axis=1, keepdims=True)
            y_acc[part, at] += jnp.where(gate > 0.0, gate * out.astype(jnp.float32), 0.0)
            return c

        lax.fori_loop(0, n // tile, piece, 0)

    def group(e, phase, block0, blocks, expert, fresh):
        first, count = block0 * per_block, blocks * per_block

        @pl.when(phase == 0)
        def _():
            @pl.when(fresh)
            def _():
                wait_gu(e)

            def one(t, c):
                front(t * tile, gu_buf.at[e])
                return c

            with jax.named_scope("front"):
                lax.fori_loop(first, first + count, one, 0)

        @pl.when(phase == 1)
        def _():
            @pl.when(fresh)
            def _():
                wait_d(e)

            def one(t, c):
                back(t * tile, lambda: d_buf[e], expert)
                return c

            with jax.named_scope("back"):
                lax.fori_loop(first, first + count, one, 0)

    def own_id(e):
        return (plane * CORES + core) * 2 + e

    def load_next(h, way):
        with jax.named_scope("wait_final"):
            wait_final(way, h)
        load_slot(h, way)

    def late_piece(i):
        with jax.named_scope("wait_f3"):
            transit_on(1, last, i, f3recv.at[i]).wait_recv()
        far_gu(1, i).start()

    def stage(h, carry):
        def gates_and_ups(i, c):
            for way in range(2):
                with jax.named_scope("wait_z0"):
                    wait_ring(way, h, 0, i)

                @pl.when(h < last)
                def _():
                    next_gu(way, h, i).start()

                if way == 0:
                    @pl.when(h == last)
                    def _():
                        far_gu(0, i).start()

                @pl.when((h < last) | (i > 0))
                def _():
                    transit_out(way, h, i).start()

            @pl.when((h == last) & (i == 1))
            def _():
                for way in range(2):
                    there = gu_ref.at[(last - 2) * 2 + way, alt, gu_cut(0)]
                    with jax.named_scope("wait_f2"):
                        remote(there, there, tsend.at[way, 1], f2recv.at[way], device_id=side_dev[1 - way]).wait_recv()
                    extra(way).start()

            @pl.when((h == 2) & (i == 0))
            def _():
                with jax.named_scope("wait_fwd"):
                    wait_forward()
                dense_pair(CORES)

            @pl.when((h >= 2) & (i == CHUNKS - 1))
            def _():
                load_next(h - 1, 0)

            @pl.when((h >= 3) | ((h == 1) & (i >= 2)))
            def _():
                mine = h == 1
                group(jnp.where(mine, 0, 1), jnp.where(mine, i - 2, i // 2), jnp.where(mine, 0, 2 * (i % 2)), 2,
                      jnp.where(mine, own_id(0), expert_id(h - 2, 1)), mine | (i % 2 == 0))

            @pl.when((h >= 2) & (i == CHUNKS - 1))
            def _():
                load_next(h - 1, 1)
            return c

        lax.fori_loop(0, CHUNKS, gates_and_ups, 0)

        def downs(i, c):
            def products():
                mine, end = h == 1, h == last
                second = end & (i == CHUNKS - 1)
                group(jnp.where(mine | second, 1, 0), jnp.where(mine, i, jnp.where(second, 0, i // 2)),
                      jnp.where(mine | (end & (i >= 2)), 0, 2 * (i % 2)), jnp.where(end & (i == 2), 4, 2),
                      jnp.where(mine, own_id(1), expert_id(h - 1, jnp.where(second, 1, 0))), mine | second | (i % 2 == 0))

            pl.when(h == last)(products)
            for way in range(2):
                @pl.when(h < last)
                def _():
                    with jax.named_scope("wait_z1"):
                        wait_ring(way, h, 1, i)

                @pl.when((h == last) & (i < 2))
                def _():
                    with jax.named_scope("wait_z2"):
                        next_half(way, 0, i).wait_recv()

                @pl.when(h < last - 1)
                def _():
                    next_d(way, h, i).start()

                @pl.when((h == last - 1) & (i % 2 == 1))
                def _():
                    next_half(way, 0, i // 2).start()

                @pl.when((h == last) & (i == way))
                def _():
                    far_half(way, 0).start()

            @pl.when((h < last) | (i > 0))
            def _():
                for way in range(2):
                    with jax.named_scope("wait_t"):
                        transit_out(way, h, i).wait_recv()
                    single = (h == last - 1) & (i == 0)

                    @pl.when(single)
                    def _():
                        transit_on(way, h, i, f2recv.at[way]).start()

                    @pl.when(((h < last) | (way == 0)) & jnp.logical_not(single))
                    def _():
                        transit_on(way, h, i, frecv.at[way, h - 1]).start()

                    if way == 1:
                        @pl.when(h == last)
                        def _():
                            transit_on(1, h, i, f3recv.at[i]).start()

            @pl.when((h == last) & (i == 2))
            def _():
                with jax.named_scope("wait_x1"):
                    extra(1).wait_recv()
                far_gu(1, 0).start()
                for r in range(2):
                    next_half(0, 1, r).start()

            @pl.when((h == last) & (i == CHUNKS - 1))
            def _():
                late_piece(1)

            @pl.when((h == 1) & (i == 1))
            def _():
                with jax.named_scope("wait_near"):
                    for way in range(2):
                        wait_near(way)
                for copy in forward():
                    copy.start()

            pl.when((h < last) & ((h >= 2) | (i < 2)))(products)
            return c

        lax.fori_loop(0, CHUNKS, downs, 0)
        return carry

    lax.fori_loop(1, last + 1, stage, 0)

    load_early(0)

    def rest(n, c):
        @pl.when(n == 2)
        def _():
            with jax.named_scope("wait_final"):
                extra(0).wait_recv()
                wait_final(0, last)
            load_late(0)
        group(1, jnp.where(n == 0, 0, 1), jnp.where(n == 1, 0, 2), 2, expert_id(last - 1, 1), n == 1)

        @pl.when(n < 2)
        def _():
            late_piece(n + 2)

        @pl.when(n == 1)
        def _():
            for r in range(2):
                next_half(1, 1, r).start()
        return c

    lax.fori_loop(0, 3, rest, 0)
    load_late(1)
    load_early(1)

    def both(w):
        return (CORES + w) * tok_n

    far_expert = expert_id(last + 1, 0)

    def shift(e):
        return -e * CORES * tok_n

    far_shift = CORES * tok_n

    size = wave_n // BACK

    def to_peer(c, way, w, k):
        off = w * part_n + way * wave_n + k * size
        return remote(y_acc.at[pl.ds(near_row(w, 1 - core) + way * wave_n + k * size, size), cols(c)], b_peer.at[pl.ds(off, size)],
                      bsend, brecv.at[way, w, k], device_id=peer)

    def give_back(c, way, w, k):
        src = near_row(w, core) + way * wave_n + k * size
        return remote(y_acc.at[pl.ds(src, size), cols(c)], y_ret.at[pl.ds(way * part_n + w * wave_n + k * size, size), cols(c)],
                      rsend.at[way], rrecv.at[way, w], device_id=side_dev[way])

    def right_half(r):
        for way in range(2):
            with jax.named_scope("wait_z3"):
                next_half(way, 1, r).wait_recv()
        far_half(r, 1).start()

    def own_expert(block, e):
        row0 = block * tok_n
        with jax.named_scope("own"):
            front(row0, gu_buf.at[e], tok_n)
            back(row0, lambda: d_buf[e], expert_id(last, e), tok_n)

    def near_back(c, w, e):
        pl.when(w == 0)(lambda: wait_half(e))
        with jax.named_scope("near_back"):
            back(both(w), lambda: d_buf[e, :, cols(c)], expert_id(last, e), tok_n, shift(e), cols(c))

    def right_pair(w):
        def one(e, carry):
            near_back(1, w, e)
            return carry

        lax.fori_loop(0, 2, one, 0)

    def wave(c, w, carry):
        first = w == 0
        if c == 0:
            pl.when(w == 1)(lambda: right_half(0))

        if c == 0:
            def pair(e, c2):
                pl.when(first)(lambda: wait_gu(e))
                with jax.named_scope("near_front"):
                    front(both(w), gu_buf.at[e], tok_n, shift(e))
                near_back(0, w, e)
                return c2

            lax.fori_loop(0, 2, pair, 0)
        else:
            pl.when(w == 1)(lambda: right_pair(1))
        if c == 0:
            @pl.when(first)
            def _():
                with jax.named_scope("wait_far0"):
                    for way in range(2):
                        m = cls if way == 0 else alt
                        remote(gu_far.at[m], gu_far.at[m], zsend.at[way, 0], farrecv.at[way, 0], device_id=ring[way]).wait_recv()
            @pl.when(w == 1)
            def _():
                right_half(1)
                for e in range(2):
                    load_half(e, 1)
            with jax.named_scope("far_front"):
                front(both(w), gu_far, tok_n, far_shift)

        @pl.when(first)
        def _():
            with jax.named_scope("wait_far1"):
                for way in range(2):
                    far_half(way, c).wait_recv()

        def far_back(k):
            with jax.named_scope("far_back"):
                back(near_row(w, k), lambda: d_far[:, cols(c)], far_expert, part_n, far_shift, cols(c))

        far_back(1 - core)
        for k in range(BACK):
            for way in range(2):
                to_peer(c, way, w, k).start()
        far_back(core)
        if c == 0:
            pl.when(w == 1)(lambda: right_pair(0))
        if c == 1:
            pl.when(w == 1)(lambda: own_expert(1 - core, 0))

        def sums(k, c2):
            @pl.when(k < BACK)
            def _():
                for way in range(2):
                    with jax.named_scope("wait_b"):
                        to_peer(c, way, w, k).wait_recv()
                    off = w * part_n + way * wave_n + k * size
                    y_acc[pl.ds(near_row(w, core) + way * wave_n + k * size, size), cols(c)] += b_peer[pl.ds(off, size)]

            @pl.when(k > 0)
            def _():
                for way in range(2):
                    give_back(c, way, w, k - 1).start()
            return c2

        lax.fori_loop(0, BACK + 1, sums, 0)
        return carry

    lax.fori_loop(0, WAVES, functools.partial(wave, 0), 0)
    pl.semaphore_signal(half_sem, inc=1, device_id=peer)
    pl.semaphore_wait(half_sem, 1)
    lax.fori_loop(0, WAVES, functools.partial(wave, 1), 0)
    with jax.named_scope("wait_bsend"):
        whole = y_acc.at[pl.ds(0, tok_n)]
        remote(whole, whole, bsend, brecv.at[0, 0, 0], device_id=peer).wait_send()
    pl.semaphore_signal(free_sem, inc=1, device_id=peer)

    def own_block(block, first):
        def one(e, c):
            own_expert(block, e)
            return c

        lax.fori_loop(first, 2, one, 0)
        with jax.named_scope("far_own"):
            front(block * tok_n, gu_far, tok_n)
            back(block * tok_n, lambda: d_far[...], far_expert, tok_n)

    def part_copy(w):
        return remote(y_acc.at[pl.ds((1 - core) * tok_n + w * part_n, part_n)], y_acc.at[pl.ds(near_row(w, core), part_n)],
                      psend, precv, device_id=peer)

    def own_blocks(n, c):
        own_block(core + (1 - n) * (1 - 2 * core), 1 - n)

        @pl.when(n == 0)
        def _():
            pl.semaphore_wait(free_sem, 1)
            for w in range(WAVES):
                part_copy(w).start()
        return c

    lax.fori_loop(0, CORES, own_blocks, 0)
    with jax.named_scope("wait_part"):
        whole = y_acc.at[pl.ds(0, tok_n)]
        remote(whole, whole, psend, precv, device_id=peer).wait()

    def finish(w, c):
        for way in range(2):
            off = w * wave_n
            part = pl.ds(way * part_n + off, wave_n)
            with jax.named_scope("wait_r"):
                remote(y_ret.at[part], y_ret.at[part], rsend.at[way], rrecv.at[way, w], device_id=side_dev[way]).wait_recv()
            mine = pl.ds(core * tok_n + way * part_n + off, wave_n)
            other = pl.ds(near_row(way, 1 - core) + off, wave_n)
            y_ref[part] = (y_acc[mine] + y_acc[other] + y_ret[part]).astype(y_ref.dtype)
        return c

    lax.fori_loop(0, WAVES, finish, 0)

    with jax.named_scope("drain"):
        for way in range(2):
            whole = gu_ref.at[pl.ds(0, 4), pl.ds(0, 2), pl.ds(0, (4 * last + 5) * gu_rows // 8)]
            remote(whole, whole, zsend.at[way, 0], farrecv.at[way, 0], device_id=ring[way]).wait_send()
            whole = gu_ref.at[pl.ds(0, 2), pl.ds(0, 2), pl.ds(0, (2 * last + 1) * gu_rows // 2)]
            remote(whole, whole, zsend.at[way, 1], farrecv.at[way, 1], device_id=ring[way]).wait_send()
            whole = tr_ref.at[pl.ds(0, 4), pl.ds(0, (4 * last - 1) * gu_rows // 4)]
            for hop in range(2):
                remote(whole, whole, tsend.at[way, hop], frecv.at[way, 0], device_id=side_dev[way]).wait_send()
            whole = y_ret.at[pl.ds(0, part_n)]
            remote(whole, whole, rsend.at[way], rrecv.at[way, 0], device_id=side_dev[way]).wait_send()


def moe(side, planes, x, route, gate, wg, wu, wd):
    tok_n, d_model = x.shape
    d_ff = wg.shape[2]
    last = planes // 2 - 1
    bf = jnp.bfloat16
    f32 = jnp.float32
    any_spec = pl.BlockSpec(memory_space=pl.ANY)
    dma = pltpu.SemaphoreType.DMA
    blocks = 2 * CORES
    rows = blocks * tok_n
    top_k = route.shape[0]
    out = pl.pallas_call(
        functools.partial(kernel, side, planes),
        out_shape=(
            jax.ShapeDtypeStruct((tok_n, d_model), bf),
            jax.ShapeDtypeStruct((2 * last, 2, d_model, d_ff), bf),
            jax.ShapeDtypeStruct((2 * last, d_ff, d_model), bf),
            jax.ShapeDtypeStruct((2 * last, d_model, d_ff), bf),
        ),
        in_specs=[any_spec] * 6,
        out_specs=(pl.BlockSpec(memory_space=pltpu.VMEM),) + (any_spec,) * 3,
        scratch_shapes=[
            pltpu.VMEM((rows, d_model), bf),
            pltpu.VMEM((blocks, top_k, tok_n), jnp.int32),
            pltpu.VMEM((blocks, top_k, tok_n), f32),
            pltpu.VMEM((rows, LANES), f32),
            pltpu.VMEM((rows, d_model), f32),
            pltpu.VMEM((tok_n, d_model // 2), f32),
            pltpu.VMEM((tok_n, d_model), f32),
            pltpu.VMEM((rows + CORES * tok_n, d_ff), bf),
            pltpu.VMEM((2, 2, d_model, d_ff), bf),
            pltpu.VMEM((2, d_ff, d_model), bf),
            pltpu.VMEM((2, d_model, d_ff), bf),
            pltpu.VMEM((d_ff, d_model), bf),
            dma((2, 2)),
            dma((2, last, 2, CHUNKS)),
            dma((2, 2)),
            dma((2, last, CHUNKS)),
            dma((2, last)),
            dma((CHUNKS,)),
            dma((2, 3)),
            dma((2,)),
            dma((2,)),
            dma((2,)),
            dma((2,)),
            dma((3,)),
            dma((3,)),
            dma((3,)),
            dma((2, 3)),
            dma((2, 3)),
            dma((3,)),
            dma((3,)),
            dma(()),
            dma((2, WAVES, BACK)),
            dma((2,)),
            dma((2, WAVES)),
            dma(()),
            dma(()),
            pltpu.SemaphoreType.REGULAR,
            pltpu.SemaphoreType.REGULAR,
        ],
        compiler_params=pltpu.CompilerParams(
            collective_id=0, has_side_effects=True, vmem_limit_bytes=103 * 512 * 1024),
        name="stream_experts",
    )(x, route, gate, wg, wu, wd)
    return out[0]


def solution(mesh):
    planes = mesh.shape["ep"] // CORES
    side = math.isqrt(mesh.shape["dp"])
    row_spec = P(("dp", "ep"))
    expert_spec = P("ep")

    def local_step(tok_loc, route_loc, gate_loc, wg_loc, wu_loc, wd_loc):
        tables = (pltpu.with_memory_space_constraint(table.T, pltpu.HBM) for table in (route_loc, gate_loc))
        return moe(side, planes, tok_loc, *tables, wg_loc, wu_loc, wd_loc)

    return jax.shard_map(local_step, mesh=mesh, in_specs=(row_spec, row_spec, row_spec, expert_spec, expert_spec, expert_spec), out_specs=row_spec, check_vma=False)
```

```python
import functools
import math

import jax
import jax.numpy as jnp
from jax import lax
from jax.experimental import pallas as pl
from jax.experimental.pallas import tpu as pltpu
from jax.sharding import PartitionSpec as P

CORES = 2
CHUNKS = 4
TILE = 512
BACK = 2
WAVES = 2
LANES = 128


def kernel(side, planes, x_ref, route_ref, gate_ref, wg_ref, wu_ref, wd_ref,
           y_ref, gu_ref, ds_ref, tr_ref,
           x_all, route_all, gate_all, gate_cols, y_acc, b_peer, y_ret, hidden,
           gu_buf, d_buf, gu_far, d_far,
           zsend, zrecv, tsend, trecv, frecv, f3recv, farrecv, xrecv, f2recv, gu_sem, d_sem, own_sem, own_send, own_recv,
           near_send, near_recv, fwd_send, fwd_recv, bsend, brecv, rsend, rrecv, psend, precv, half_sem, free_sem):
    last = planes // 2 - 1
    tok_n, d_model = x_ref.shape
    part_n = tok_n // 2
    tile = min(TILE, tok_n // 2)
    per_block = tok_n // tile
    experts = planes * CORES * 2
    col = lax.axis_index("dp")
    pos = lax.axis_index("ep")
    core = pos % CORES
    plane = pos // CORES
    cx, cy = col // side, col % side
    parity = (cx + cy) % 2
    cls = cx % 2
    alt = 1 - cls
    col_x = col + side * (1 - 2 * (cx % 2))
    col_y = col + 1 - 2 * (cy % 2)
    up = (pos + CORES) % (planes * CORES)
    down = (pos + (planes - 1) * CORES) % (planes * CORES)
    peer = {"ep": pos + 1 - 2 * core}
    ring = ({"ep": up}, {"ep": down})
    side_dev = ({"dp": col_x}, {"dp": col_y})
    gu_rows = wg_ref.shape[1] // CHUNKS
    d_rows = wd_ref.shape[1] // CHUNKS
    remote = pltpu.make_async_remote_copy

    with jax.named_scope("entry"):
        barrier = pltpu.get_barrier_semaphore()
        for dev in (*ring, *side_dev, peer):
            pl.semaphore_signal(barrier, inc=1, device_id=dev)
        pl.semaphore_wait(barrier, 5)

    def gu_cut(i):
        return pl.ds(i * gu_rows, gu_rows)

    def d_cut(i):
        return pl.ds(i * d_rows, d_rows)

    def first_gu(way, i):
        for m, w in enumerate((wg_ref, wu_ref)):
            @pl.when(cls == m)
            def _(m=m, w=w):
                remote(w.at[parity, gu_cut(i)], gu_ref.at[way, m, gu_cut(i)],
                       zsend.at[way, 0], zrecv.at[way, 0, 0, i], device_id=ring[way]).start()

    def first_d(way, i):
        remote(wd_ref.at[parity, d_cut(i)], ds_ref.at[way, d_cut(i)],
               zsend.at[way, 1], zrecv.at[way, 0, 1, i], device_id=ring[way]).start()

    def next_gu(way, h, i):
        return remote(gu_ref.at[(h - 1) * 2 + way, cls, gu_cut(i)], gu_ref.at[h * 2 + way, cls, gu_cut(i)],
                      zsend.at[way, 0], zrecv.at[way, h, 0, i], device_id=ring[way])

    def next_d(way, h, i):
        return remote(ds_ref.at[(h - 1) * 2 + way, d_cut(i)], ds_ref.at[h * 2 + way, d_cut(i)],
                      zsend.at[way, 1], zrecv.at[way, h, 1, i], device_id=ring[way])

    def wait_ring(way, h, kind, i):
        there = ds_ref.at[(h - 1) * 2 + way, d_cut(i)] if kind else gu_ref.at[(h - 1) * 2 + way, cls, gu_cut(i)]
        remote(there, there, zsend.at[way, kind], zrecv.at[way, h - 1, kind, i], device_id=ring[way]).wait_recv()

    def far_gu(way, i):
        m = cls if way == 0 else alt
        return remote(gu_ref.at[(last - 1) * 2 + way, m, gu_cut(i)], gu_far.at[m, gu_cut(i)],
                      zsend.at[way, 0], farrecv.at[way, 0], device_id=ring[way])

    half_w = d_model // 2
    d_half = wd_ref.shape[1] // 2

    def cols(c):
        return pl.ds(c * half_w, half_w)

    def next_half(way, c, r):
        part = pl.ds(r * d_half, d_half)
        return remote(ds_ref.at[(last - 2) * 2 + way, part, cols(c)], ds_ref.at[(last - 1) * 2 + way, part, cols(c)],
                      zsend.at[way, 1], zrecv.at[way, last - 1, 1, 2 * c + r], device_id=ring[way])

    def far_half(way, c):
        part = pl.ds(way * d_half, d_half)
        return remote(ds_ref.at[(last - 1) * 2 + way, part, cols(c)], d_far.at[part, cols(c)],
                      zsend.at[way, 1], farrecv.at[way, 1 + c], device_id=ring[way])

    def extra(way):
        return remote(gu_ref.at[(last - 2) * 2 + way, alt, gu_cut(0)], gu_ref.at[(last - 1) * 2 + way, alt, gu_cut(0)],
                      zsend.at[way, 0], xrecv.at[way], device_id=ring[way])

    def transit_out(way, h, i):
        slot = (h - 1) * 2 + way
        return remote(gu_ref.at[slot, cls, gu_cut(i)], tr_ref.at[slot, gu_cut(i)],
                      tsend.at[way, 0], trecv.at[way, h - 1, i], device_id=side_dev[way])

    def transit_on(way, h, i, sem):
        slot = (h - 1) * 2 + way
        m = alt if way == 0 else cls
        return remote(tr_ref.at[slot, gu_cut(i)], gu_ref.at[slot, m, gu_cut(i)],
                      tsend.at[way, 1], sem, device_id=side_dev[1 - way])

    def wait_final(way, h):
        def wait(n):
            there = gu_ref.at[(h - 1) * 2 + way, alt, pl.ds(0, n * gu_rows)]
            remote(there, there, tsend.at[way, 1], frecv.at[way, h - 1], device_id=side_dev[1 - way]).wait_recv()

        pl.when(h < last - 1)(lambda: wait(CHUNKS))
        pl.when(h >= last - 1)(lambda: wait(CHUNKS - 1))


    wave_n = part_n // WAVES

    def near_row(w, k):
        return (CORES + w) * tok_n + k * part_n

    def near(way):
        copies = []
        for w in range(WAVES):
            src = pl.ds(way * part_n + w * wave_n, wave_n)
            dst = pl.ds(pl.multiple_of(core * part_n + way * wave_n, wave_n), wave_n)
            copies += [
                remote(route_ref.at[:, src], route_all.at[CORES + w, :, dst], near_send.at[way, 0], near_recv.at[way, 0], device_id=side_dev[way]),
                remote(gate_ref.at[:, src], gate_all.at[CORES + w, :, dst], near_send.at[way, 1], near_recv.at[way, 1], device_id=side_dev[way]),
                remote(x_ref.at[src], x_all.at[pl.ds(near_row(w, core) + way * wave_n, wave_n)], near_send.at[way, 2], near_recv.at[way, 2], device_id=side_dev[way])]
        return copies

    def wait_near(way):
        part = pl.ds(0, part_n)
        for k, ref in enumerate((route_all.at[CORES, :, part], gate_all.at[CORES, :, part], x_all.at[pl.ds(CORES * tok_n, part_n)])):
            remote(ref, ref, near_send.at[way, k], near_recv.at[way, k], device_id=side_dev[way]).wait()

    for way in range(2):
        for copy in near(way):
            copy.start()
    for i in range(CHUNKS):
        for way in range(2):
            first_gu(way, i)
    for i in range(CHUNKS):
        for way in range(2):
            first_d(way, i)

    def load_own(e):
        for m, w in enumerate((wg_ref, wu_ref)):
            pltpu.make_async_copy(w.at[e], gu_buf.at[e, m], gu_sem.at[e]).start()
        pltpu.make_async_copy(wd_ref.at[e], d_buf.at[e], d_sem.at[e]).start()

    def load_slot(h, e):
        slot = (h - 1) * 2 + e
        pltpu.make_async_copy(gu_ref.at[slot], gu_buf.at[e], gu_sem.at[e]).start()
        pltpu.make_async_copy(ds_ref.at[slot], d_buf.at[e], d_sem.at[e]).start()

    def load_half(e, c):
        slot = (last - 1) * 2 + e
        pltpu.make_async_copy(ds_ref.at[slot, :, cols(c)], d_buf.at[e, :, cols(c)], d_sem.at[e]).start()

    def wait_half(e):
        pltpu.make_async_copy(ds_ref.at[0, :, cols(0)], d_buf.at[e, :, cols(0)], d_sem.at[e]).wait()

    def load_early(e):
        slot = (last - 1) * 2 + e
        pltpu.make_async_copy(gu_ref.at[slot, cls], gu_buf.at[e, cls], gu_sem.at[e]).start()
        load_half(e, 0)

    def load_late(e):
        slot = (last - 1) * 2 + e
        pltpu.make_async_copy(gu_ref.at[slot, alt], gu_buf.at[e, alt], gu_sem.at[e]).start()

    def wait_gu(e):
        pltpu.make_async_copy(gu_ref.at[0], gu_buf.at[e], gu_sem.at[e]).wait()

    def wait_d(e):
        pltpu.make_async_copy(ds_ref.at[0], d_buf.at[e], d_sem.at[e]).wait()

    load_own(0)
    load_own(1)
    tok = ((route_ref, route_all.at[core]), (gate_ref, gate_all.at[core]), (x_ref, x_all.at[pl.ds(core * tok_n, tok_n)]))
    for k, (src, dst) in enumerate(tok):
        remote(src, dst, own_send.at[k], own_recv.at[k], device_id=peer).start()
        pltpu.make_async_copy(src, dst, own_sem.at[k]).start()
    y_acc[...] = jnp.zeros_like(y_acc)
    y_ret[pl.ds(0, LANES), :] = jnp.zeros((LANES, d_model), jnp.float32)
    for k, (src, dst) in enumerate(tok):
        pltpu.make_async_copy(src, dst, own_sem.at[k]).wait()
        remote(src, dst, own_send.at[k], own_recv.at[k], device_id=peer).wait()

    def dense(block):
        route, gate = route_all[block], gate_all[block]
        for e in range(experts):
            y_ret[e:e + 1, pl.ds(0, tok_n)] = jnp.sum(jnp.where(route == e, gate, 0.0), axis=0, keepdims=True)
        for b in range(tok_n // LANES):
            gate_cols[pl.ds(block * tok_n + b * LANES, LANES), :] = y_ret[pl.ds(0, LANES), b * LANES:(b + 1) * LANES].T

    def dense_pair(first):
        def one(c, carry):
            dense(first + c)
            return carry

        lax.fori_loop(0, CORES, one, 0)

    dense_pair(0)

    def forward():
        lanes = pl.ds(pl.multiple_of(core * part_n, part_n), part_n)
        return [remote(ref, ref, fwd_send.at[k], fwd_recv.at[k], device_id=peer) for w in range(WAVES) for k, ref in enumerate((
            route_all.at[CORES + w, :, lanes], gate_all.at[CORES + w, :, lanes], x_all.at[pl.ds(near_row(w, core), part_n)]))]

    def wait_forward():
        for k, ref in enumerate((route_all.at[CORES], gate_all.at[CORES], x_all.at[pl.ds(CORES * tok_n, tok_n)])):
            remote(ref, ref, fwd_send.at[k], fwd_recv.at[k], device_id=peer).wait()

    def expert_id(h, way):
        src = (plane + planes + (2 * way - 1) * h) % planes
        return (src * CORES + core) * 2 + parity

    def front(row0, gu, n=tile, shift=0):
        def piece(t, c):
            part = pl.ds(row0 + t * tile, tile)
            x_tile = x_all[part]
            a = jnp.dot(x_tile, gu[0], preferred_element_type=jnp.float32)
            b = jnp.dot(x_tile, gu[1], preferred_element_type=jnp.float32)
            hidden[pl.ds(row0 + t * tile + shift, tile)] = (jax.nn.silu(a) * b).astype(jnp.bfloat16)
            return c

        lax.fori_loop(0, n // tile, piece, 0)

    def back(row0, d, expert, n=tile, shift=0, at=None):
        at = pl.ds(0, d_model) if at is None else at

        def piece(t, c):
            part = pl.ds(row0 + t * tile, tile)
            out = jnp.dot(hidden[pl.ds(row0 + t * tile + shift, tile)], d(), preferred_element_type=jnp.float32).astype(jnp.bfloat16)
            gates = gate_cols[part]
            lane = lax.broadcasted_iota(jnp.int32, gates.shape, 1)
            gate = jnp.sum(jnp.where(lane == expert, gates, 0.0), axis=1, keepdims=True)
            y_acc[part, at] += jnp.where(gate > 0.0, gate * out.astype(jnp.float32), 0.0)
            return c

        lax.fori_loop(0, n // tile, piece, 0)

    def group(e, phase, block0, blocks, expert, fresh):
        first, count = block0 * per_block, blocks * per_block

        @pl.when(phase == 0)
        def _():
            @pl.when(fresh)
            def _():
                wait_gu(e)

            def one(t, c):
                front(t * tile, gu_buf.at[e])
                return c

            with jax.named_scope("front"):
                lax.fori_loop(first, first + count, one, 0)

        @pl.when(phase == 1)
        def _():
            @pl.when(fresh)
            def _():
                wait_d(e)

            def one(t, c):
                back(t * tile, lambda: d_buf[e], expert)
                return c

            with jax.named_scope("back"):
                lax.fori_loop(first, first + count, one, 0)

    def own_id(e):
        return (plane * CORES + core) * 2 + e

    def load_next(h, way):
        with jax.named_scope("wait_final"):
            wait_final(way, h)
        load_slot(h, way)

    def late_piece(i):
        with jax.named_scope("wait_f3"):
            transit_on(1, last, i, f3recv.at[i]).wait_recv()
        far_gu(1, i).start()

    def stage(h, carry):
        def gates_and_ups(i, c):
            for way in range(2):
                with jax.named_scope("wait_z0"):
                    wait_ring(way, h, 0, i)

                @pl.when(h < last)
                def _():
                    next_gu(way, h, i).start()

                if way == 0:
                    @pl.when(h == last)
                    def _():
                        far_gu(0, i).start()

                @pl.when((h < last) | (i > 0))
                def _():
                    transit_out(way, h, i).start()

            @pl.when((h == last) & (i == 1))
            def _():
                for way in range(2):
                    there = gu_ref.at[(last - 2) * 2 + way, alt, gu_cut(0)]
                    with jax.named_scope("wait_f2"):
                        remote(there, there, tsend.at[way, 1], f2recv.at[way], device_id=side_dev[1 - way]).wait_recv()
                    extra(way).start()

            @pl.when((h == 2) & (i == 0))
            def _():
                with jax.named_scope("wait_fwd"):
                    wait_forward()
                dense_pair(CORES)

            @pl.when((h >= 2) & (i == CHUNKS - 1))
            def _():
                load_next(h - 1, 0)

            @pl.when((h >= 3) | ((h == 1) & (i >= 2)))
            def _():
                mine = h == 1
                group(jnp.where(mine, 0, 1), jnp.where(mine, i - 2, i // 2), jnp.where(mine, 0, 2 * (i % 2)), 2,
                      jnp.where(mine, own_id(0), expert_id(h - 2, 1)), mine | (i % 2 == 0))

            @pl.when((h >= 2) & (i == CHUNKS - 1))
            def _():
                load_next(h - 1, 1)
            return c

        lax.fori_loop(0, CHUNKS, gates_and_ups, 0)

        def downs(i, c):
            def products():
                mine, end = h == 1, h == last
                second = end & (i == CHUNKS - 1)
                group(jnp.where(mine | second, 1, 0), jnp.where(mine, i, jnp.where(second, 0, i // 2)),
                      jnp.where(mine | (end & (i >= 2)), 0, 2 * (i % 2)), jnp.where(end & (i == 2), 4, 2),
                      jnp.where(mine, own_id(1), expert_id(h - 1, jnp.where(second, 1, 0))), mine | second | (i % 2 == 0))

            pl.when(h == last)(products)
            for way in range(2):
                @pl.when(h < last)
                def _():
                    with jax.named_scope("wait_z1"):
                        wait_ring(way, h, 1, i)

                @pl.when((h == last) & (i < 2))
                def _():
                    with jax.named_scope("wait_z2"):
                        next_half(way, 0, i).wait_recv()

                @pl.when(h < last - 1)
                def _():
                    next_d(way, h, i).start()

                @pl.when((h == last - 1) & (i % 2 == 1))
                def _():
                    next_half(way, 0, i // 2).start()

                @pl.when((h == last) & (i == way))
                def _():
                    far_half(way, 0).start()

            @pl.when((h < last) | (i > 0))
            def _():
                for way in range(2):
                    with jax.named_scope("wait_t"):
                        transit_out(way, h, i).wait_recv()
                    single = (h == last - 1) & (i == 0)

                    @pl.when(single)
                    def _():
                        transit_on(way, h, i, f2recv.at[way]).start()

                    @pl.when(((h < last) | (way == 0)) & jnp.logical_not(single))
                    def _():
                        transit_on(way, h, i, frecv.at[way, h - 1]).start()

                    if way == 1:
                        @pl.when(h == last)
                        def _():
                            transit_on(1, h, i, f3recv.at[i]).start()

            @pl.when((h == last) & (i == 2))
            def _():
                with jax.named_scope("wait_x1"):
                    extra(1).wait_recv()
                far_gu(1, 0).start()
                for r in range(2):
                    next_half(0, 1, r).start()

            @pl.when((h == last) & (i == CHUNKS - 1))
            def _():
                late_piece(1)

            @pl.when((h == 1) & (i == 1))
            def _():
                with jax.named_scope("wait_near"):
                    for way in range(2):
                        wait_near(way)
                for copy in forward():
                    copy.start()

            pl.when((h < last) & ((h >= 2) | (i < 2)))(products)
            return c

        lax.fori_loop(0, CHUNKS, downs, 0)
        return carry

    lax.fori_loop(1, last + 1, stage, 0)

    load_early(0)

    def rest(n, c):
        @pl.when(n == 2)
        def _():
            with jax.named_scope("wait_final"):
                extra(0).wait_recv()
                wait_final(0, last)
            load_late(0)
        group(1, jnp.where(n == 0, 0, 1), jnp.where(n == 1, 0, 2), 2, expert_id(last - 1, 1), n == 1)

        @pl.when(n < 2)
        def _():
            late_piece(n + 2)

        @pl.when(n == 1)
        def _():
            for r in range(2):
                next_half(1, 1, r).start()
        return c

    lax.fori_loop(0, 3, rest, 0)
    load_late(1)
    load_early(1)

    def both(w):
        return (CORES + w) * tok_n

    far_expert = expert_id(last + 1, 0)

    def shift(e):
        return -e * CORES * tok_n

    far_shift = CORES * tok_n

    size = wave_n // BACK

    def to_peer(c, way, w, k):
        off = w * part_n + way * wave_n + k * size
        return remote(y_acc.at[pl.ds(near_row(w, 1 - core) + way * wave_n + k * size, size), cols(c)], b_peer.at[pl.ds(off, size)],
                      bsend, brecv.at[way, w, k], device_id=peer)

    def give_back(c, way, w, k):
        src = near_row(w, core) + way * wave_n + k * size
        return remote(y_acc.at[pl.ds(src, size), cols(c)], y_ret.at[pl.ds(way * part_n + w * wave_n + k * size, size), cols(c)],
                      rsend.at[way], rrecv.at[way, w], device_id=side_dev[way])

    def right_half(r):
        for way in range(2):
            with jax.named_scope("wait_z3"):
                next_half(way, 1, r).wait_recv()
        far_half(r, 1).start()

    def own_expert(block, e):
        row0 = block * tok_n
        with jax.named_scope("own"):
            front(row0, gu_buf.at[e], tok_n, -row0)
            back(row0, lambda: d_buf[e], expert_id(last, e), tok_n, -row0)

    def near_back(c, w, e):
        pl.when(w == 0)(lambda: wait_half(e))
        with jax.named_scope("near_back"):
            back(both(w), lambda: d_buf[e, :, cols(c)], expert_id(last, e), tok_n, shift(e), cols(c))

    def right_pair(w):
        def one(e, carry):
            near_back(1, w, e)
            return carry

        lax.fori_loop(0, 2, one, 0)

    def wave(c, w, carry):
        first = w == 0

        if c == 0:
            def pair(e, c2):
                pl.when(first)(lambda: wait_gu(e))
                with jax.named_scope("near_front"):
                    front(both(w), gu_buf.at[e], tok_n, shift(e))
                near_back(0, w, e)
                return c2

            lax.fori_loop(0, 2, pair, 0)
            pl.when(w == 1)(lambda: right_half(0))
        else:
            right_pair(w)
            pl.when(first)(lambda: own_expert(1 - core, 0))
        if c == 0:
            @pl.when(first)
            def _():
                with jax.named_scope("wait_far0"):
                    for way in range(2):
                        m = cls if way == 0 else alt
                        remote(gu_far.at[m], gu_far.at[m], zsend.at[way, 0], farrecv.at[way, 0], device_id=ring[way]).wait_recv()
            @pl.when(w == 1)
            def _():
                right_half(1)
                for e in range(2):
                    load_half(e, 1)
            with jax.named_scope("far_front"):
                front(both(w), gu_far, tok_n, far_shift)

        @pl.when(first)
        def _():
            with jax.named_scope("wait_far1"):
                for way in range(2):
                    far_half(way, c).wait_recv()

        def far_back(k):
            with jax.named_scope("far_back"):
                back(near_row(w, k), lambda: d_far[:, cols(c)], far_expert, part_n, far_shift, cols(c))

        far_back(1 - core)
        for k in range(BACK):
            for way in range(2):
                to_peer(c, way, w, k).start()
        far_back(core)
        if c == 1:
            pl.when(w == 1)(lambda: own_expert(1 - core, 1))

        def sums(k, c2):
            @pl.when(k < BACK)
            def _():
                for way in range(2):
                    with jax.named_scope("wait_b"):
                        to_peer(c, way, w, k).wait_recv()
                    off = w * part_n + way * wave_n + k * size
                    y_acc[pl.ds(near_row(w, core) + way * wave_n + k * size, size), cols(c)] += b_peer[pl.ds(off, size)]

            @pl.when(k > 0)
            def _():
                for way in range(2):
                    give_back(c, way, w, k - 1).start()
            return c2

        lax.fori_loop(0, BACK + 1, sums, 0)
        return carry

    lax.fori_loop(0, WAVES, functools.partial(wave, 0), 0)
    pl.semaphore_signal(half_sem, inc=1, device_id=peer)
    pl.semaphore_wait(half_sem, 1)
    lax.fori_loop(0, WAVES, functools.partial(wave, 1), 0)
    with jax.named_scope("wait_bsend"):
        whole = y_acc.at[pl.ds(0, tok_n)]
        remote(whole, whole, bsend, brecv.at[0, 0, 0], device_id=peer).wait_send()
    pl.semaphore_signal(free_sem, inc=1, device_id=peer)

    def own_block(block, first):
        def one(e, c):
            own_expert(block, e)
            return c

        lax.fori_loop(first, 2, one, 0)
        with jax.named_scope("far_own"):
            front(block * tok_n, gu_far, tok_n)
            back(block * tok_n, lambda: d_far[...], far_expert, tok_n)

    def part_copy(w):
        return remote(y_acc.at[pl.ds((1 - core) * tok_n + w * part_n, part_n)], y_acc.at[pl.ds(near_row(w, core), part_n)],
                      psend, precv, device_id=peer)

    def own_blocks(n, c):
        own_block(core + (1 - n) * (1 - 2 * core), 2 * (1 - n))

        @pl.when(n == 0)
        def _():
            pl.semaphore_wait(free_sem, 1)
            for w in range(WAVES):
                part_copy(w).start()
        return c

    lax.fori_loop(0, CORES, own_blocks, 0)
    with jax.named_scope("wait_part"):
        whole = y_acc.at[pl.ds(0, tok_n)]
        remote(whole, whole, psend, precv, device_id=peer).wait()

    def finish(w, c):
        for way in range(2):
            off = w * wave_n
            part = pl.ds(way * part_n + off, wave_n)
            with jax.named_scope("wait_r"):
                remote(y_ret.at[part], y_ret.at[part], rsend.at[way], rrecv.at[way, w], device_id=side_dev[way]).wait_recv()
            mine = pl.ds(core * tok_n + way * part_n + off, wave_n)
            other = pl.ds(near_row(way, 1 - core) + off, wave_n)
            y_ref[part] = (y_acc[mine] + y_acc[other] + y_ret[part]).astype(y_ref.dtype)
        return c

    lax.fori_loop(0, WAVES, finish, 0)

    with jax.named_scope("drain"):
        for way in range(2):
            whole = gu_ref.at[pl.ds(0, 4), pl.ds(0, 2), pl.ds(0, (4 * last + 5) * gu_rows // 8)]
            remote(whole, whole, zsend.at[way, 0], farrecv.at[way, 0], device_id=ring[way]).wait_send()
            whole = gu_ref.at[pl.ds(0, 2), pl.ds(0, 2), pl.ds(0, (2 * last + 1) * gu_rows // 2)]
            remote(whole, whole, zsend.at[way, 1], farrecv.at[way, 1], device_id=ring[way]).wait_send()
            whole = tr_ref.at[pl.ds(0, 4), pl.ds(0, (4 * last - 1) * gu_rows // 4)]
            for hop in range(2):
                remote(whole, whole, tsend.at[way, hop], frecv.at[way, 0], device_id=side_dev[way]).wait_send()
            whole = y_ret.at[pl.ds(0, part_n)]
            remote(whole, whole, rsend.at[way], rrecv.at[way, 0], device_id=side_dev[way]).wait_send()


def moe(side, planes, x, route, gate, wg, wu, wd):
    tok_n, d_model = x.shape
    d_ff = wg.shape[2]
    last = planes // 2 - 1
    bf = jnp.bfloat16
    f32 = jnp.float32
    any_spec = pl.BlockSpec(memory_space=pl.ANY)
    dma = pltpu.SemaphoreType.DMA
    blocks = 2 * CORES
    rows = blocks * tok_n
    top_k = route.shape[0]
    out = pl.pallas_call(
        functools.partial(kernel, side, planes),
        out_shape=(
            jax.ShapeDtypeStruct((tok_n, d_model), bf),
            jax.ShapeDtypeStruct((2 * last, 2, d_model, d_ff), bf),
            jax.ShapeDtypeStruct((2 * last, d_ff, d_model), bf),
            jax.ShapeDtypeStruct((2 * last, d_model, d_ff), bf),
        ),
        in_specs=[any_spec] * 6,
        out_specs=(pl.BlockSpec(memory_space=pltpu.VMEM),) + (any_spec,) * 3,
        scratch_shapes=[
            pltpu.VMEM((rows, d_model), bf),
            pltpu.VMEM((blocks, top_k, tok_n), jnp.int32),
            pltpu.VMEM((blocks, top_k, tok_n), f32),
            pltpu.VMEM((rows, LANES), f32),
            pltpu.VMEM((rows, d_model), f32),
            pltpu.VMEM((tok_n, d_model // 2), f32),
            pltpu.VMEM((tok_n, d_model), f32),
            pltpu.VMEM((rows + CORES * tok_n, d_ff), bf),
            pltpu.VMEM((2, 2, d_model, d_ff), bf),
            pltpu.VMEM((2, d_ff, d_model), bf),
            pltpu.VMEM((2, d_model, d_ff), bf),
            pltpu.VMEM((d_ff, d_model), bf),
            dma((2, 2)),
            dma((2, last, 2, CHUNKS)),
            dma((2, 2)),
            dma((2, last, CHUNKS)),
            dma((2, last)),
            dma((CHUNKS,)),
            dma((2, 3)),
            dma((2,)),
            dma((2,)),
            dma((2,)),
            dma((2,)),
            dma((3,)),
            dma((3,)),
            dma((3,)),
            dma((2, 3)),
            dma((2, 3)),
            dma((3,)),
            dma((3,)),
            dma(()),
            dma((2, WAVES, BACK)),
            dma((2,)),
            dma((2, WAVES)),
            dma(()),
            dma(()),
            pltpu.SemaphoreType.REGULAR,
            pltpu.SemaphoreType.REGULAR,
        ],
        compiler_params=pltpu.CompilerParams(
            collective_id=0, has_side_effects=True, vmem_limit_bytes=103 * 512 * 1024),
        name="stream_experts",
    )(x, route, gate, wg, wu, wd)
    return out[0]


def solution(mesh):
    planes = mesh.shape["ep"] // CORES
    side = math.isqrt(mesh.shape["dp"])
    row_spec = P(("dp", "ep"))
    expert_spec = P("ep")

    def local_step(tok_loc, route_loc, gate_loc, wg_loc, wu_loc, wd_loc):
        tables = (pltpu.with_memory_space_constraint(table.T, pltpu.HBM) for table in (route_loc, gate_loc))
        return moe(side, planes, tok_loc, *tables, wg_loc, wu_loc, wd_loc)

    return jax.shard_map(local_step, mesh=mesh, in_specs=(row_spec, row_spec, row_spec, expert_spec, expert_spec, expert_spec), out_specs=row_spec, check_vma=False)
```
